512 devices in a mesh: views: 32 (over y, z_lo), rows: 16 (over z_hi, x, core).
Axes of the slice: x: 4, y: 8, z: 8 (z_hi: 2, z_lo: 4; z = z_hi * 4 + z_lo), core: 2. Of those that a mesh axis runs over, the one named last changes fastest.
Arguments:
- sinogram: bfloat16 [32, 256, 2048], P(None, 'views'), may hold values from -32 to 6176
- view_shift: int32 [256], P('views'), may hold values from -48 to 48
- conv_one: float32 [9, 32], replicated, may hold values from -2 to 2
- bias_one: float32 [32], replicated, may hold values from -3 to 3
- conv_two: bfloat16 [32, 288], replicated, may hold values from -0.375 to 0.375
- bias_two: float32 [32], replicated, may hold values from -3 to 3
Outputs:
- denoised: bfloat16 [32, 32, 64, 2048], P('views', None, 'rows')
The draws below stay inside these ranges and needn't reach their ends.
All inputs are finite; a program needn't handle non-finite values.
Results may differ from the reference program's by a relative error of at most 0.008.
Values may be sent and summed in bfloat16 or wider, within the bound.
No kernel may reach another device: no remote copies, remote signals or barrier semaphores. Data moves between devices by JAX's collectives and lax.ppermute only.
A program may use at most 64 MiB of HBM per device.

```python
import math
import jax
import jax.numpy as jnp
from jax import lax

BINS = 2048
WIDTH = 2048
CHAN = 32
MARGIN = 384
SHIFT_MAX = 48
VIEWS = 256
SLICES = 32
IMG_ROWS = 64


def draw_sinogram(key, part):
    radius = WIDTH / 2.0
    angle = jnp.arange(VIEWS, dtype=jnp.float32) * (math.pi / VIEWS)
    cosine = jnp.cos(angle)[None, :, None]
    sine = jnp.sin(angle)[None, :, None]
    detector = (jnp.arange(BINS, dtype=jnp.float32) - (BINS - 1) / 2.0)[None, None, :]
    count = 4
    dense_low = 0.2
    dense_high = 1.0
    axis_low = 0.15
    axis_high = 0.5
    keys = jax.random.split(key, 7)
    shape = (SLICES, count)
    centre_x = jax.random.uniform(keys[0], shape, jnp.float32, -0.5, 0.5) * radius
    centre_y = jax.random.uniform(keys[1], shape, jnp.float32, -0.3, 0.3) * radius
    semi_first = jax.random.uniform(keys[2], shape, jnp.float32, axis_low, axis_high) * radius
    semi_second = jax.random.uniform(keys[3], shape, jnp.float32, axis_low, axis_high) * radius
    tilt = jax.random.uniform(keys[4], shape, jnp.float32, 0.0, math.pi)
    density = jax.random.uniform(keys[5], shape, jnp.float32, dense_low, dense_high)
    total = jnp.zeros((SLICES, VIEWS, BINS), jnp.float32)
    for item in range(count):
        first = semi_first[:, item][:, None, None]
        second = semi_second[:, item][:, None, None]
        turned = angle[None, :, None] - tilt[:, item][:, None, None]
        reach_sq = (first * jnp.cos(turned)) ** 2 + (second * jnp.sin(turned)) ** 2
        offset = detector - (centre_x[:, item][:, None, None] * cosine + centre_y[:, item][:, None, None] * sine)
        chord = 2.0 * first * second / reach_sq * jnp.sqrt(jnp.maximum(reach_sq - offset * offset, 0.0))
        total = total + density[:, item][:, None, None] * chord
    noise = jnp.clip(6.0 * jax.random.normal(keys[6], (SLICES, VIEWS, BINS), jnp.float32), -30.0, 30.0)
    return (total + noise).astype(jnp.bfloat16)


def set_ends(drawn, stream_key, smallest, top_value):
    dims = drawn.shape
    place = [jax.random.randint(jax.random.fold_in(stream_key, axis), (), 0, dims[axis]) for axis in range(len(dims))]
    drawn = drawn.at[tuple(place)].set(smallest)
    longest = dims.index(max(dims))
    place[longest] = (place[longest] + 1) % dims[longest]
    return drawn.at[tuple(place)].set(top_value)


def centred(key, extent, deviation, most, held_as=jnp.bfloat16):
    entries = deviation * jax.random.normal(key, extent, jnp.float32)
    return jnp.clip(entries, min=-most, max=most).astype(held_as)


def setup_inputs(seed: int = 0) -> dict:
    seeds = jax.random.split(jax.random.key(seed), 7)
    return {
        "sinogram": draw_sinogram(jax.random.fold_in(seeds[6], 71), 0),
        "view_shift": set_ends(jax.random.randint(seeds[1], (VIEWS,), 0 - SHIFT_MAX, SHIFT_MAX + 1), jax.random.fold_in(seeds[1], 1), 0 - SHIFT_MAX, SHIFT_MAX).astype(jnp.int32),
        "conv_one": centred(seeds[2], (9, CHAN), 9 ** -0.5, 2.0, jnp.float32),
        "bias_one": centred(seeds[3], (CHAN,), 0.5, 3.0, jnp.float32),
        "conv_two": centred(seeds[4], (CHAN, 9 * CHAN), (9 * CHAN) ** -0.5, 0.375),
        "bias_two": centred(seeds[5], (CHAN,), 0.5, 3.0, jnp.float32),
    }


def ramp_table(detector):
    indices = jnp.arange(detector, dtype=jnp.int32)
    offset = indices[None, :] - indices[:, None]
    square = (offset * offset).astype(jnp.float32)
    guarded = jnp.maximum(square, 1.0)
    is_odd = (offset % 2) != 0
    values = jnp.where(offset == 0, 0.25, jnp.where(is_odd, -1.0 / ((math.pi * math.pi) * guarded), 0.0))
    return values.astype(jnp.float32)


def filter_views(sinogram):
    sheets, view_count, detector = sinogram.shape
    table = ramp_table(detector)
    flat = sinogram.reshape(sheets * view_count, detector).astype(jnp.float32)
    result = jnp.dot(flat, table, precision=lax.Precision.HIGHEST, preferred_element_type=jnp.float32)
    return result.astype(jnp.bfloat16).reshape(sheets, view_count, detector)


def first_layer(extended, conv_one, bias_one):
    row_count = extended.shape[1] - 2
    columns = extended.shape[2]
    padded = jnp.pad(extended.astype(jnp.float32), ((0, 0), (0, 0), (1, 1)))
    running = jnp.zeros((extended.shape[0], conv_one.shape[1], row_count, columns), jnp.float32)
    running = running + bias_one[None, :, None, None]
    for kernel_tap in range(9):
        row_off = kernel_tap // 3
        col_off = kernel_tap % 3
        window = padded[:, row_off:row_off + row_count, col_off:col_off + columns]
        running = running + conv_one[kernel_tap][None, :, None, None] * window[:, None]
    return jnp.maximum(running, 0.0).astype(jnp.bfloat16)


def second_layer(extended, conv_two, bias_two):
    sheets, channels, rows_ext, columns = extended.shape
    row_count = rows_ext - 2
    padded = jnp.pad(extended, ((0, 0), (0, 0), (0, 0), (1, 1)))
    windows = [padded[:, :, kernel_tap // 3:kernel_tap // 3 + row_count, kernel_tap % 3:kernel_tap % 3 + columns] for kernel_tap in range(9)]
    stacked = jnp.stack(windows, axis=1).reshape(sheets, 9 * channels, row_count * columns)
    mixed = jnp.einsum("ok,skn->son", conv_two.astype(jnp.float32), stacked.astype(jnp.float32), precision=lax.Precision.HIGHEST)
    mixed = mixed + bias_two[None, :, None]
    return jnp.maximum(mixed, 0.0).astype(jnp.bfloat16).reshape(sheets, channels, row_count, columns)


def reference(sinogram, view_shift, conv_one, bias_one, conv_two, bias_two):
    filtered = filter_views(sinogram)
    padded = jnp.pad(filtered, ((0, 0), (0, 0), (MARGIN, MARGIN)))
    sheets_by_view = jnp.swapaxes(padded, 0, 1)
    columns = jnp.arange(WIDTH, dtype=jnp.float32) - (WIDTH - 1) / 2.0
    rows_y = jnp.arange(IMG_ROWS, dtype=jnp.int32).astype(jnp.float32) - (IMG_ROWS - 1) / 2.0

    def one_view(running, inputs):
        view_index, shift, sheet = inputs
        angle = view_index.astype(jnp.float32) * (math.pi / VIEWS)
        cosine = jnp.cos(angle)
        sine = jnp.sin(angle)
        center = shift.astype(jnp.float32) + ((BINS - 1) / 2.0 + MARGIN)
        position = (columns[None, :] * cosine + rows_y[:, None] * sine) + center
        lower = jnp.floor(position)
        lower_index = lower.astype(jnp.int32)
        weight_low = jnp.maximum(0.0, 1.0 - jnp.abs(position - lower)).astype(jnp.bfloat16)
        weight_high = jnp.maximum(0.0, 1.0 - jnp.abs(position - (lower + 1.0))).astype(jnp.bfloat16)
        low_values = jnp.take(sheet, lower_index, axis=1).astype(jnp.float32)
        high_values = jnp.take(sheet, lower_index + 1, axis=1).astype(jnp.float32)
        term = low_values * weight_low.astype(jnp.float32)[None] + high_values * weight_high.astype(jnp.float32)[None]
        return running + term, 0

    start = jnp.zeros((SLICES, IMG_ROWS, WIDTH), jnp.float32)
    running = lax.scan(one_view, start, (jnp.arange(VIEWS, dtype=jnp.int32), view_shift, sheets_by_view))[0]
    image = (running * (math.pi / VIEWS)).astype(jnp.bfloat16)

    def one_slice(sheet):
        extended = jnp.pad(sheet[None], ((0, 0), (1, 1), (0, 0)))
        hidden = first_layer(extended, conv_one, bias_one)
        hidden = jnp.pad(hidden, ((0, 0), (0, 0), (1, 1), (0, 0)))
        return second_layer(hidden, conv_two, bias_two)[0]

    return lax.map(one_slice, image)
```

```python
import math

import jax
import jax.numpy as jnp
from jax import lax
from jax.experimental import pallas as pl
from jax.experimental.pallas import tpu as pltpu
from jax.sharding import PartitionSpec as P

BINS = 2048
WIDTH = 2048
MARGIN = 384
CHAN = 32
ROW_DEV = 4
GROUP = 4
BLOCK = 256
BLOCKS = BINS // BLOCK
CENTER = (BINS - 1) / 2.0 + MARGIN
FIRST_WIN = 4
WINDOWS = 38
TILES = WIDTH // 128
ROW_SETS = 3
VIEW_STEP = 8


def ramp_kernel(table_ref):
    def one_block(block, carry):
        row = lax.broadcasted_iota(jnp.int32, (BLOCK, BLOCK), 0)
        col = lax.broadcasted_iota(jnp.int32, (BLOCK, BLOCK), 1)
        offset = col - row + (block - (BLOCKS - 1)) * BLOCK
        place = offset.astype(jnp.float32)
        guarded = jnp.maximum(place * place, 1.0)
        odd = (offset & 1) == 1
        values = jnp.where(odd, -1.0 / (math.pi * math.pi * guarded), 0.0)
        values = jnp.where(offset == 0, 0.25, values)
        high = values.astype(jnp.bfloat16)
        low = (values - high.astype(jnp.float32)).astype(jnp.bfloat16)
        where = pl.ds(pl.multiple_of(block * BLOCK, BLOCK), BLOCK)
        table_ref[0:BLOCK, where] = high
        table_ref[BLOCK : 2 * BLOCK, where] = low
        return carry

    lax.fori_loop(0, 2 * BLOCKS - 1, one_block, 0)


def ramp_blocks():
    return pl.pallas_call(
        ramp_kernel,
        out_shape=jax.ShapeDtypeStruct((2 * BLOCK, (2 * BLOCKS - 1) * BLOCK), jnp.bfloat16),
        out_specs=pl.BlockSpec(memory_space=pltpu.VMEM),
        cost_estimate=pl.CostEstimate(flops=20_000_000, bytes_accessed=4_000_000, transcendentals=0),
        name="ramp",
    )()


def backproject_kernel(
    first_ref,
    x_ref,
    cos_ref,
    sin_ref,
    ramp_ref,
    out_ref,
    filt_ref,
    slope_ref,
    level_ref,
    bin_ref,
    center_ref,
    where_ref,
    acc_ref,
    where_smem,
    sem,
):
    views = x_ref.shape[0]
    first_y = first_ref[0]
    lane = lax.broadcasted_iota(jnp.int32, (views, 128), 1)
    lane_f = lane.astype(jnp.float32)

    cosine = cos_ref[...]
    sine = sin_ref[...]
    center = CENTER + x_ref[:, BINS : BINS + 128].astype(jnp.float32)
    center_ref[...] = center
    tile_x = (lane & 15).astype(jnp.float32) * 128.0 - (WIDTH - 1) / 2.0
    set_y = first_y + 8.0 * (lane >> 4).astype(jnp.float32)
    lowest = jnp.minimum(tile_x * cosine, (tile_x + 127.0) * cosine) + set_y * sine + center
    window = ((lowest - 0.25) * (1.0 / 64.0)).astype(jnp.int32) - FIRST_WIN
    window = jnp.clip(window, 0, WINDOWS - 3)
    view = lax.broadcasted_iota(jnp.int32, (views, 128), 0)
    where_ref[...] = window * views + view
    to_smem = pltpu.make_async_copy(where_ref, where_smem, sem)
    to_smem.start()

    for step in range(2 * BLOCKS - 1):
        delta = (step + 1) // 2 * (1 if step % 2 else -1)
        low, high = max(0, -delta), min(BLOCKS, BLOCKS - delta)
        left = jnp.concatenate(
            [x_ref[:, BLOCK * block : BLOCK * block + BLOCK] for block in range(low, high)], axis=0
        )
        left = jnp.concatenate([left, left], axis=1)
        right = ramp_ref[:, BLOCK * (delta + BLOCKS - 1) : BLOCK * (delta + BLOCKS)]
        part = jnp.dot(left, right, preferred_element_type=jnp.float32)
        rows = slice(views * (low + delta), views * (high + delta))
        if delta == 0:
            filt_ref[rows, :] = part
        else:
            filt_ref[rows, :] += part

    zero = jnp.zeros((views, 128), jnp.float32)
    margin = MARGIN // 128

    def filtered(block):
        place = block - margin
        if place < 0 or place >= BINS // 128:
            return zero
        half = 128 * (place % 2)
        piece = filt_ref[views * (place // 2) : views * (place // 2) + views, half : half + 128]
        return piece.astype(jnp.bfloat16).astype(jnp.float32)

    def turned(piece):
        return pltpu.roll(piece, 127, 1)

    def block_tables(block, piece, piece_turned, next_turned):
        after = jnp.where(lane < 127, piece_turned, next_turned)
        slope = after - piece
        bins = lane_f + 128.0 * block
        return slope, piece - bins * slope, bins + 1.0

    first_block = FIRST_WIN // 2
    piece = filtered(first_block)
    piece_turned = turned(piece)
    before = None
    for block in range(first_block, (FIRST_WIN + WINDOWS) // 2 + 1):
        following = filtered(block + 1)
        following_turned = turned(following)
        now = block_tables(block, piece, piece_turned, following_turned)
        for ref, value, old in zip((slope_ref, level_ref, bin_ref), now, before or now):
            row = (2 * block - FIRST_WIN) * views
            if before is not None:
                ref[row - views : row, :] = jnp.where(lane >= 64, old, value)
            if 2 * block < FIRST_WIN + WINDOWS:
                ref[row : row + views, :] = value
        before = now
        piece, piece_turned = following, following_turned

    acc_ref[...] = jnp.zeros_like(acc_ref)
    to_smem.wait()

    lane_one = lax.broadcasted_iota(jnp.int32, (8, 128), 1).astype(jnp.float32)
    sub_one = lax.broadcasted_iota(jnp.int32, (8, 128), 0).astype(jnp.float32)
    per_set = views // VIEW_STEP

    def steps(step, carry):
        row_set = step // per_set
        first_view = (step % per_set) * VIEW_STEP
        rows_y = sub_one + (first_y + 8.0 * row_set.astype(jnp.float32))
        totals = [acc_ref[row_set, :, 128 * tile : 128 * tile + 128] for tile in range(TILES)]
        for view_off in range(VIEW_STEP):
            view = first_view + view_off
            cos_v = jnp.broadcast_to(cos_ref[pl.ds(view, 1), :], (8, 128))
            sin_v = jnp.broadcast_to(sin_ref[pl.ds(view, 1), :], (8, 128))
            base = rows_y * sin_v + jnp.broadcast_to(center_ref[pl.ds(view, 1), :], (8, 128))
            stride = cos_v * 128.0
            middle = (lane_one + 0.5) * cos_v + base
            middle_low = jnp.minimum(0.5 * cos_v, 127.5 * cos_v) + base
            for direction in (1, -1):
                place, place_low = middle, middle_low
                tiles = range(TILES // 2, TILES) if direction == 1 else range(TILES // 2 - 1, -1, -1)
                for tile in tiles:
                    if direction == 1 and tile > TILES // 2:
                        place, place_low = place + stride, place_low + stride
                    elif direction == -1:
                        place, place_low = place - stride, place_low - stride
                    row = where_smem[view, row_set * TILES + tile]
                    near = pl.ds(row, 1)
                    far = pl.ds(row + 2 * views, 1)
                    pick = bin_ref[near, :] > place_low
                    slopes = jnp.where(pick, slope_ref[near, :], slope_ref[far, :])
                    levels = jnp.where(pick, level_ref[near, :], level_ref[far, :])
                    index = place.astype(jnp.int32) & 127
                    slope = jnp.take_along_axis(slopes, index, axis=1, mode="promise_in_bounds")
                    level = jnp.take_along_axis(levels, index, axis=1, mode="promise_in_bounds")
                    totals[tile] = totals[tile] + (level + place * slope)
        for tile in range(TILES):
            acc_ref[row_set, :, 128 * tile : 128 * tile + 128] = totals[tile]
        return carry

    lax.fori_loop(0, ROW_SETS * per_set, steps, 0)

    for member in range(GROUP):
        lower = acc_ref[member // 2]
        if member % 2:
            lower = jnp.concatenate([lower[4:8], acc_ref[member // 2 + 1][0:4]], axis=0)
        out_ref[member] = lower.astype(jnp.bfloat16)


def backproject(first_y, lines, cosine, sine, ramp):
    views = lines.shape[0]
    rows = WINDOWS * views
    vmem = pl.BlockSpec(memory_space=pltpu.VMEM)
    return pl.pallas_call(
        backproject_kernel,
        out_shape=jax.ShapeDtypeStruct((GROUP, 8, WIDTH), jnp.bfloat16),
        in_specs=[pl.BlockSpec(memory_space=pltpu.SMEM), vmem, vmem, vmem, vmem],
        out_specs=vmem,
        scratch_shapes=[
            pltpu.VMEM((BLOCKS * views, BLOCK), jnp.float32),
            pltpu.VMEM((rows, 128), jnp.float32),
            pltpu.VMEM((rows, 128), jnp.float32),
            pltpu.VMEM((rows, 128), jnp.float32),
            pltpu.VMEM((views, 128), jnp.float32),
            pltpu.VMEM((views, 128), jnp.int32),
            pltpu.VMEM((ROW_SETS, 8, WIDTH), jnp.float32),
            pltpu.SMEM((views, 128), jnp.int32),
            pltpu.SemaphoreType.DMA(()),
        ],
        cost_estimate=pl.CostEstimate(flops=1_000_000_000, bytes_accessed=6_000_000, transcendentals=0),
        name="backproject",
    )(first_y, lines, cosine, sine, ramp)


def layers_kernel(
    scale,
    image_rows,
    row_ref,
    parts_ref,
    first_ref,
    bias_one_ref,
    second_ref,
    bias_two_ref,
    out_ref,
    image_ref,
    stack_ref,
):
    row_base = row_ref[0]
    image = parts_ref[0].astype(jnp.float32)
    for member in range(1, GROUP):
        image = image + parts_ref[member].astype(jnp.float32)
    image = (image * scale).astype(jnp.bfloat16).astype(jnp.float32)
    row = lax.broadcasted_iota(jnp.int32, image.shape, 0) + (row_base - 2)
    image = jnp.where((row >= 0) & (row < image_rows), image, 0.0)
    column = lax.broadcasted_iota(jnp.int32, image.shape, 1)
    left = jnp.where(column == 0, 0.0, pltpu.roll(image, 1, 1))
    right = jnp.where(column == WIDTH - 1, 0.0, pltpu.roll(image, WIDTH - 1, 1))
    three = jnp.concatenate([left, image, right], axis=0).astype(jnp.bfloat16)
    image_ref[...] = jnp.concatenate([three, three, three], axis=0)

    weights = first_ref[...]
    high = weights.astype(jnp.bfloat16)
    rest = weights - high.astype(jnp.float32)
    middle = rest.astype(jnp.bfloat16)
    low = (rest - middle.astype(jnp.float32)).astype(jnp.bfloat16)
    weights = jnp.concatenate([high, middle, low], axis=1)

    count = CHAN * (ROW_DEV + 2)
    for tile in range(0, WIDTH, 256):
        hidden = jnp.dot(weights, image_ref[:, tile : tile + 256], preferred_element_type=jnp.float32)
        hidden = jnp.maximum(hidden + bias_one_ref[...], 0.0)
        top = jnp.where(row_base > 0, hidden[0:CHAN], 0.0)
        bottom = jnp.where(row_base + ROW_DEV < image_rows, hidden[count - CHAN : count], 0.0)
        hidden = jnp.concatenate([top, hidden[CHAN : count - CHAN], bottom], axis=0)
        stack_ref[:, tile : tile + 256] = hidden

    middle_rows = stack_ref[...]
    column = lax.broadcasted_iota(jnp.int32, middle_rows.shape, 1)
    before = jnp.where(column == 0, 0.0, pltpu.roll(middle_rows, 1, 1)).astype(jnp.bfloat16)
    after = jnp.where(column == WIDTH - 1, 0.0, pltpu.roll(middle_rows, WIDTH - 1, 1)).astype(jnp.bfloat16)
    stacked = jnp.concatenate([before, middle_rows.astype(jnp.bfloat16), after], axis=0)
    mixed = jnp.dot(second_ref[...], stacked, preferred_element_type=jnp.float32)
    mixed = jnp.maximum(mixed + bias_two_ref[...], 0.0)
    out_ref[...] = mixed.reshape(CHAN, ROW_DEV, WIDTH).astype(jnp.bfloat16)[None]


def layers(row_base, parts, first, bias_one, second, bias_two, scale, image_rows):
    vmem = pl.BlockSpec(memory_space=pltpu.VMEM)

    def body(*refs):
        layers_kernel(scale, image_rows, *refs)

    return pl.pallas_call(
        body,
        out_shape=jax.ShapeDtypeStruct((1, CHAN, ROW_DEV, WIDTH), jnp.bfloat16),
        in_specs=[pl.BlockSpec(memory_space=pltpu.SMEM)] + [vmem] * 5,
        out_specs=vmem,
        scratch_shapes=[
            pltpu.VMEM((72, WIDTH), jnp.bfloat16),
            pltpu.VMEM((CHAN * (ROW_DEV + 2), WIDTH), jnp.float32),
        ],
        cost_estimate=pl.CostEstimate(flops=500_000_000, bytes_accessed=1_000_000, transcendentals=0),
        name="layers",
    )(row_base, parts, first, bias_one, second, bias_two)


def first_matrix(conv_one):
    taps = conv_one.reshape(3, 3, CHAN)
    rows = []
    for row in range(ROW_DEV + 2):
        padded = jnp.pad(taps, ((row, ROW_DEV + 1 - row), (0, 0), (0, 0)))
        rows.append(jnp.transpose(padded, (2, 1, 0)))
    return jnp.stack(rows).reshape(CHAN * (ROW_DEV + 2), 24)


def second_matrix(conv_two):
    taps = conv_two.reshape(CHAN, 3, 3, CHAN)
    rows = []
    for row in range(ROW_DEV):
        padded = jnp.pad(taps, ((0, 0), (row, ROW_DEV - 1 - row), (0, 0), (0, 0)))
        rows.append(jnp.transpose(padded, (0, 2, 1, 3)))
    return jnp.stack(rows, axis=1).reshape(CHAN * ROW_DEV, 3 * (ROW_DEV + 2) * CHAN)


def local(sinogram, view_shift, conv_one, bias_one, conv_two, bias_two):
    sheets, view_count, detector = sinogram.shape
    row_groups = lax.axis_size("rows")
    view_groups = lax.axis_size("views")
    views_total = view_count * view_groups
    image_rows = ROW_DEV * row_groups
    share = view_count // GROUP
    row_index = lax.axis_index("rows")
    member = row_index % GROUP

    mine = lax.dynamic_slice_in_dim(sinogram, member * share, share, 1)
    shift = lax.dynamic_slice_in_dim(view_shift, member * share, share, 0).astype(jnp.bfloat16)
    shift = jnp.broadcast_to(shift[None, :, None], (sheets, share, 128))
    sent = jnp.concatenate([mine, shift], axis=2)
    lines = lax.all_to_all(sent, "views", 0, 0, tiled=True)
    lines = lines.reshape(view_groups * share, detector + 128)

    view = jnp.arange(view_groups * share, dtype=jnp.int32)
    view = view // share * view_count + member * share + view % share
    angle = view.astype(jnp.float32) * (math.pi / views_total)
    cosine = jnp.broadcast_to(jnp.cos(angle)[:, None], (view_groups * share, 128))
    sine = jnp.broadcast_to(jnp.sin(angle)[:, None], (view_groups * share, 128))
    first_row = (row_index - member) * ROW_DEV - 2
    first_y = first_row.astype(jnp.float32) - (image_rows - 1) / 2.0

    partial_rows = backproject(first_y.reshape(1), lines, cosine, sine, ramp_blocks())
    groups = [[GROUP * base + item for item in range(GROUP)] for base in range(row_groups // GROUP)]
    parts = lax.all_to_all(partial_rows, "rows", 0, 0, tiled=True, axis_index_groups=groups)

    row_base = (row_index * ROW_DEV).astype(jnp.int32).reshape(1)
    wide_one = jnp.tile(bias_one, ROW_DEV + 2)[:, None]
    wide_two = jnp.repeat(bias_two, ROW_DEV)[:, None]
    return layers(
        row_base,
        parts,
        first_matrix(conv_one),
        wide_one,
        second_matrix(conv_two),
        wide_two,
        math.pi / views_total,
        image_rows,
    )


def solution(mesh):
    return jax.shard_map(
        local,
        mesh=mesh,
        in_specs=(P(None, "views", None), P("views"), P(), P(), P(), P()),
        out_specs=P("views", None, "rows", None),
        check_vma=False,
    )
```

```python
import math

import jax
import jax.numpy as jnp
from jax import lax
from jax.experimental import pallas as pl
from jax.experimental.pallas import tpu as pltpu
from jax.sharding import PartitionSpec as P

BINS = 2048
WIDTH = 2048
MARGIN = 384
CHAN = 32
ROW_DEV = 4
GROUP = 4
BLOCK = 256
BLOCKS = BINS // BLOCK
CENTER = (BINS - 1) / 2.0 + MARGIN
FIRST_WIN = 4
WINDOWS = 38
TILES = WIDTH // 128
ROW_SETS = 3
VIEW_STEP = 8


def selection(shape, test):
    row = lax.broadcasted_iota(jnp.int32, shape, 0)
    col = lax.broadcasted_iota(jnp.int32, shape, 1)
    return jnp.where(test(row, col), 1.0, 0.0)


def exact_dot(left, right, contract=(1, 0)):
    return lax.dot_general(
        left,
        right,
        (((contract[0],), (contract[1],)), ((), ())),
        precision=lax.Precision.HIGHEST,
        preferred_element_type=jnp.float32,
    )


def column_of(picker, row):
    return jnp.sum(picker * row, axis=1, keepdims=True)


def prepare_kernel(
    views_total,
    share,
    view_count,
    member_ref,
    conv_one_ref,
    bias_one_ref,
    conv_two_ref,
    bias_two_ref,
    table_ref,
    cos_ref,
    sin_ref,
    first_ref,
    wide_one_ref,
    second_ref,
    wide_two_ref,
):
    width = (2 * BLOCKS - 1) * BLOCK

    for turn in range(8):
        row = lax.broadcasted_iota(jnp.int32, (16, width + 128), 0)
        col = lax.broadcasted_iota(jnp.int32, (16, width + 128), 1)
        offset = col - row - (128 + 16 * turn + (BLOCKS - 1) * BLOCK)
        place = offset.astype(jnp.float32)
        guarded = jnp.maximum(place * place, 1.0)
        odd = (offset & 1) == 1
        values = jnp.where(odd, (-1.0 / (math.pi * math.pi)) / guarded, 0.0)
        values = jnp.where(offset == 0, 0.25, values)
        high = values.astype(jnp.bfloat16)
        low = (values - high.astype(jnp.float32)).astype(jnp.bfloat16)
        for half in range(2):
            start = 16 * turn + 128 * half
            cols = slice(128 - 128 * half, 128 - 128 * half + width)
            table_ref[start : start + 16, :] = high[:, cols]
            table_ref[BLOCK + start : BLOCK + start + 16, :] = low[:, cols]

    view = lax.broadcasted_iota(jnp.int32, cos_ref.shape, 0)
    view = view // share * view_count + member_ref[0] * share + view % share
    angle = view.astype(jnp.float32) * (math.pi / views_total)
    cos_ref[...] = jnp.cos(angle)
    sin_ref[...] = jnp.sin(angle)

    rows_one = CHAN * (ROW_DEV + 2)
    picker = selection((rows_one, CHAN), lambda row, col: (row & (CHAN - 1)) == col)
    wide_one_ref[...] = column_of(picker, bias_one_ref[...])
    taps = exact_dot(picker, conv_one_ref[...], (1, 1))
    weights = jnp.zeros((rows_one, 24), jnp.float32)
    for item in range(3):
        moved = exact_dot(taps, selection((9, 24), lambda row, col: row == 3 * item + (col >> 3)))
        keep = selection((rows_one, 24), lambda row, col: (col & 7) == (row >> 5) + item)
        weights = weights + moved * keep
    high = weights.astype(jnp.bfloat16)
    rest = weights - high.astype(jnp.float32)
    middle = rest.astype(jnp.bfloat16)
    low = (rest - middle.astype(jnp.float32)).astype(jnp.bfloat16)
    first_ref[...] = jnp.concatenate([high, middle, low], axis=1)

    rows_two = CHAN * ROW_DEV
    picker = selection((rows_two, CHAN), lambda row, col: (row >> 2) == col)
    wide_two_ref[...] = column_of(picker, bias_two_ref[...])
    spread = jnp.dot(
        picker.astype(jnp.bfloat16), conv_two_ref[...], preferred_element_type=jnp.float32
    ).astype(jnp.bfloat16)
    cols_two = CHAN * (ROW_DEV + 2)
    for tap in range(3):
        block = jnp.zeros((rows_two, cols_two), jnp.float32)
        for item in range(3):
            source = spread[:, (3 * item + tap) * CHAN : (3 * item + tap + 1) * CHAN]
            place = selection((CHAN, cols_two), lambda row, col: (col & (CHAN - 1)) == row)
            moved = jnp.dot(source, place.astype(jnp.bfloat16), preferred_element_type=jnp.float32)
            keep = selection((rows_two, cols_two), lambda row, col: (col >> 5) == (row & 3) + item)
            block = block + moved * keep
        second_ref[tap] = block.astype(jnp.bfloat16)


def prepare(member, conv_one, bias_one, conv_two, bias_two, views, views_total, share, view_count):
    vmem = pl.BlockSpec(memory_space=pltpu.VMEM)

    def body(*refs):
        prepare_kernel(views_total, share, view_count, *refs)

    rows_one, rows_two = CHAN * (ROW_DEV + 2), CHAN * ROW_DEV
    return pl.pallas_call(
        body,
        out_shape=(
            jax.ShapeDtypeStruct((2 * BLOCK, (2 * BLOCKS - 1) * BLOCK), jnp.bfloat16),
            jax.ShapeDtypeStruct((views, 128), jnp.float32),
            jax.ShapeDtypeStruct((views, 128), jnp.float32),
            jax.ShapeDtypeStruct((rows_one, 72), jnp.bfloat16),
            jax.ShapeDtypeStruct((rows_one, 1), jnp.float32),
            jax.ShapeDtypeStruct((3, rows_two, rows_one), jnp.bfloat16),
            jax.ShapeDtypeStruct((rows_two, 1), jnp.float32),
        ),
        in_specs=[pl.BlockSpec(memory_space=pltpu.SMEM)] + [vmem] * 4,
        out_specs=(vmem,) * 7,
        compiler_params=pltpu.CompilerParams(vmem_limit_bytes=16 * 2**20),
        cost_estimate=pl.CostEstimate(flops=20_000_000, bytes_accessed=4_000_000, transcendentals=0),
        name="prepare",
    )(member, conv_one, bias_one, conv_two, bias_two)


def lane_gather(words, index):
    dims = lax.GatherDimensionNumbers(
        offset_dims=(),
        collapsed_slice_dims=(1,),
        start_index_map=(1,),
        operand_batching_dims=(0,),
        start_indices_batching_dims=(0,),
    )
    return lax.gather(
        words, index[:, :, None], dims, (1, 1), mode=lax.GatherScatterMode.PROMISE_IN_BOUNDS
    )


def backproject_kernel(
    first_ref,
    x_ref,
    cos_ref,
    sin_ref,
    ramp_ref,
    out_ref,
    filt_ref,
    word_ref,
    bin_ref,
    back_ref,
    center_ref,
    where_ref,
    acc_ref,
    where_smem,
    sem,
):
    views = x_ref.shape[0]
    first_y = first_ref[0]
    lane = lax.broadcasted_iota(jnp.int32, (views, 128), 1)
    lane_f = lane.astype(jnp.float32)

    cosine = cos_ref[...]
    sine = sin_ref[...]
    center = CENTER + x_ref[:, BINS : BINS + 128].astype(jnp.float32)
    center_ref[...] = center
    tile_x = (lane & 15).astype(jnp.float32) * 128.0 - (WIDTH - 1) / 2.0
    set_y = first_y + 8.0 * (lane >> 4).astype(jnp.float32)
    lowest = jnp.minimum(tile_x * cosine, (tile_x + 127.0) * cosine) + set_y * sine + center
    window = ((lowest - 0.25) * (1.0 / 64.0)).astype(jnp.int32) - FIRST_WIN
    window = jnp.clip(window, 0, WINDOWS - 3)
    view = lax.broadcasted_iota(jnp.int32, (views, 128), 0)
    where_ref[...] = window * views + view
    to_smem = pltpu.make_async_copy(where_ref, where_smem, sem)
    to_smem.start()

    for step in range(2 * BLOCKS - 1):
        delta = (step + 1) // 2 * (1 if step % 2 else -1)
        low, high = max(0, -delta), min(BLOCKS, BLOCKS - delta)
        left = jnp.concatenate(
            [x_ref[:, BLOCK * block : BLOCK * block + BLOCK] for block in range(low, high)], axis=0
        )
        left = jnp.concatenate([left, left], axis=1)
        right = ramp_ref[:, BLOCK * (delta + BLOCKS - 1) : BLOCK * (delta + BLOCKS)]
        part = jnp.dot(left, right, preferred_element_type=jnp.float32)
        rows = slice(views * (low + delta), views * (high + delta))
        if delta == 0:
            filt_ref[rows, :] = part
        else:
            filt_ref[rows, :] += part

    margin = MARGIN // 128
    inner = BINS // 128

    def raw(place):
        half = 128 * (place % 2)
        piece = filt_ref[views * (place // 2) : views * (place // 2) + views, half : half + 128]
        return piece.astype(jnp.bfloat16).astype(jnp.float32)

    largest = jnp.abs(raw(0))
    for place in range(1, inner):
        largest = jnp.maximum(largest, jnp.abs(raw(place)))
    largest = jnp.max(largest, axis=1, keepdims=True)
    largest = jnp.max(largest.reshape(views // VIEW_STEP, VIEW_STEP, 1), axis=1, keepdims=True)
    largest = jnp.maximum(jnp.broadcast_to(largest, (views // VIEW_STEP, VIEW_STEP, 128)), 1e-30)
    largest = largest.reshape(views, 128)
    back_ref[...] = largest * (1.0 / (16383.0 * 65536.0))
    scale = 16383.0 / largest
    zero = jnp.zeros((views, 128), jnp.int32)

    def filtered(block):
        place = block - margin
        if place < 0 or place >= inner:
            return zero
        return jnp.floor(raw(place) * scale + 0.5).astype(jnp.int32)

    def turned(piece):
        return pltpu.roll(piece, 127, 1)

    def block_tables(block, piece, piece_turned, next_turned):
        step = jnp.where(lane < 127, piece_turned, next_turned) - piece
        return piece * 65536 + step, lane_f + (128.0 * block + 1.0)

    first_block = FIRST_WIN // 2
    piece = filtered(first_block)
    piece_turned = turned(piece)
    before = None
    for block in range(first_block, (FIRST_WIN + WINDOWS) // 2 + 1):
        following = filtered(block + 1)
        following_turned = turned(following)
        now = block_tables(block, piece, piece_turned, following_turned)
        for ref, value, old in zip((word_ref, bin_ref), now, before or now):
            row = (2 * block - FIRST_WIN) * views
            if before is not None:
                ref[row - views : row, :] = jnp.where(lane >= 64, old, value)
            if 2 * block < FIRST_WIN + WINDOWS:
                ref[row : row + views, :] = value
        before = now
        piece, piece_turned = following, following_turned

    acc_ref[...] = jnp.zeros_like(acc_ref)
    to_smem.wait()

    lane_one = lax.broadcasted_iota(jnp.int32, (8, 128), 1).astype(jnp.float32)
    sub_one = lax.broadcasted_iota(jnp.int32, (8, 128), 0).astype(jnp.float32)
    per_set = views // VIEW_STEP

    def steps(step, carry):
        row_set = step // per_set
        first_view = (step % per_set) * VIEW_STEP
        rows_y = sub_one + (first_y + 8.0 * row_set.astype(jnp.float32))
        totals = [None] * TILES
        for view_off in range(VIEW_STEP):
            view = first_view + view_off
            cos_v = jnp.broadcast_to(cos_ref[pl.ds(view, 1), :], (8, 128))
            sin_v = jnp.broadcast_to(sin_ref[pl.ds(view, 1), :], (8, 128))
            base = rows_y * sin_v + jnp.broadcast_to(center_ref[pl.ds(view, 1), :], (8, 128))
            stride = cos_v * 128.0
            middle = (lane_one + 0.5) * cos_v + base
            middle_low = jnp.minimum(0.5 * cos_v, 127.5 * cos_v) + base
            for direction in (1, -1):
                place, place_low = middle, middle_low
                tiles = range(TILES // 2, TILES) if direction == 1 else range(TILES // 2 - 1, -1, -1)
                for tile in tiles:
                    if direction == 1 and tile > TILES // 2:
                        place, place_low = place + stride, place_low + stride
                    elif direction == -1:
                        place, place_low = place - stride, place_low - stride
                    row = where_smem[view, row_set * TILES + tile]
                    near = pl.ds(row, 1)
                    far = pl.ds(row + 2 * views, 1)
                    pick = bin_ref[near, :] > place_low
                    words = jnp.where(pick, word_ref[near, :], word_ref[far, :])
                    floor = jnp.floor(place)
                    word = lane_gather(words, floor.astype(jnp.int32) & 127)
                    value = word.astype(jnp.float32)
                    value = value + (place - floor) * (word << 16).astype(jnp.float32)
                    totals[tile] = value if totals[tile] is None else totals[tile] + value
        back = jnp.broadcast_to(back_ref[pl.ds(first_view, 1), :], (8, 128))
        for tile in range(TILES):
            acc_ref[row_set, :, 128 * tile : 128 * tile + 128] += totals[tile] * back
        return carry

    lax.fori_loop(0, ROW_SETS * per_set, steps, 0)

    for member in range(GROUP):
        lower = acc_ref[member // 2]
        if member % 2:
            lower = jnp.concatenate([lower[4:8], acc_ref[member // 2 + 1][0:4]], axis=0)
        out_ref[member] = lower.astype(jnp.bfloat16)


def backproject(first_y, lines, cosine, sine, ramp):
    views = lines.shape[0]
    rows = WINDOWS * views
    vmem = pl.BlockSpec(memory_space=pltpu.VMEM)
    return pl.pallas_call(
        backproject_kernel,
        out_shape=jax.ShapeDtypeStruct((GROUP, 8, WIDTH), jnp.bfloat16),
        in_specs=[pl.BlockSpec(memory_space=pltpu.SMEM), vmem, vmem, vmem, vmem],
        out_specs=vmem,
        scratch_shapes=[
            pltpu.VMEM((BLOCKS * views, BLOCK), jnp.float32),
            pltpu.VMEM((rows, 128), jnp.int32),
            pltpu.VMEM((rows, 128), jnp.float32),
            pltpu.VMEM((views, 128), jnp.float32),
            pltpu.VMEM((views, 128), jnp.float32),
            pltpu.VMEM((views, 128), jnp.int32),
            pltpu.VMEM((ROW_SETS, 8, WIDTH), jnp.float32),
            pltpu.SMEM((views, 128), jnp.int32),
            pltpu.SemaphoreType.DMA(()),
        ],
        compiler_params=pltpu.CompilerParams(vmem_limit_bytes=16 * 2**20),
        cost_estimate=pl.CostEstimate(flops=1_000_000_000, bytes_accessed=6_000_000, transcendentals=0),
        name="backproject",
    )(first_y, lines, cosine, sine, ramp)


def layers_kernel(
    scale,
    image_rows,
    row_ref,
    parts_ref,
    first_ref,
    bias_one_ref,
    second_ref,
    bias_two_ref,
    out_ref,
    image_ref,
    stack_ref,
):
    row_base = row_ref[0]
    image = parts_ref[0].astype(jnp.float32)
    for member in range(1, GROUP):
        image = image + parts_ref[member].astype(jnp.float32)
    image = (image * scale).astype(jnp.bfloat16).astype(jnp.float32)
    row = lax.broadcasted_iota(jnp.int32, image.shape, 0) + (row_base - 2)
    image = jnp.where((row >= 0) & (row < image_rows), image, 0.0)
    column = lax.broadcasted_iota(jnp.int32, image.shape, 1)
    left = jnp.where(column == 0, 0.0, pltpu.roll(image, 1, 1))
    right = jnp.where(column == WIDTH - 1, 0.0, pltpu.roll(image, WIDTH - 1, 1))
    three = jnp.concatenate([left, image, right], axis=0).astype(jnp.bfloat16)
    image_ref[...] = jnp.concatenate([three, three, three], axis=0)

    weights = first_ref[...]
    count = CHAN * (ROW_DEV + 2)
    for tile in range(0, WIDTH, 256):
        hidden = jnp.dot(weights, image_ref[:, tile : tile + 256], preferred_element_type=jnp.float32)
        hidden = jnp.maximum(hidden + bias_one_ref[...], 0.0)
        top = jnp.where(row_base > 0, hidden[0:CHAN], 0.0)
        bottom = jnp.where(row_base + ROW_DEV < image_rows, hidden[count - CHAN : count], 0.0)
        hidden = jnp.concatenate([top, hidden[CHAN : count - CHAN], bottom], axis=0)
        stack_ref[:, tile : tile + 256] = hidden

    middle_rows = stack_ref[...]
    column = lax.broadcasted_iota(jnp.int32, middle_rows.shape, 1)
    before = jnp.where(column == 0, 0.0, pltpu.roll(middle_rows, 1, 1)).astype(jnp.bfloat16)
    after = jnp.where(column == WIDTH - 1, 0.0, pltpu.roll(middle_rows, WIDTH - 1, 1)).astype(jnp.bfloat16)
    mixed = jnp.dot(second_ref[0], before, preferred_element_type=jnp.float32)
    mixed = mixed + jnp.dot(second_ref[1], middle_rows.astype(jnp.bfloat16), preferred_element_type=jnp.float32)
    mixed = mixed + jnp.dot(second_ref[2], after, preferred_element_type=jnp.float32)
    mixed = jnp.maximum(mixed + bias_two_ref[...], 0.0)
    out_ref[...] = mixed.reshape(CHAN, ROW_DEV, WIDTH).astype(jnp.bfloat16)[None]


def layers(row_base, parts, first, bias_one, second, bias_two, scale, image_rows):
    vmem = pl.BlockSpec(memory_space=pltpu.VMEM)

    def body(*refs):
        layers_kernel(scale, image_rows, *refs)

    return pl.pallas_call(
        body,
        out_shape=jax.ShapeDtypeStruct((1, CHAN, ROW_DEV, WIDTH), jnp.bfloat16),
        in_specs=[pl.BlockSpec(memory_space=pltpu.SMEM)] + [vmem] * 5,
        out_specs=vmem,
        scratch_shapes=[
            pltpu.VMEM((72, WIDTH), jnp.bfloat16),
            pltpu.VMEM((CHAN * (ROW_DEV + 2), WIDTH), jnp.float32),
        ],
        compiler_params=pltpu.CompilerParams(vmem_limit_bytes=16 * 2**20),
        cost_estimate=pl.CostEstimate(flops=500_000_000, bytes_accessed=1_000_000, transcendentals=0),
        name="layers",
    )(row_base, parts, first, bias_one, second, bias_two)


def local(sinogram, view_shift, conv_one, bias_one, conv_two, bias_two):
    sheets, view_count, detector = sinogram.shape
    row_groups = lax.axis_size("rows")
    view_groups = lax.axis_size("views")
    views_total = view_count * view_groups
    image_rows = ROW_DEV * row_groups
    share = view_count // GROUP
    row_index = lax.axis_index("rows")
    member = row_index % GROUP

    mine = lax.dynamic_slice_in_dim(sinogram, member * share, share, 1)
    shift = lax.dynamic_slice_in_dim(view_shift, member * share, share, 0).astype(jnp.bfloat16)
    shift = jnp.broadcast_to(shift[None, :, None], (sheets, share, 128))
    sent = jnp.concatenate([mine, shift], axis=2)
    lines = lax.all_to_all(sent, "views", 0, 0, tiled=True)
    lines = lines.reshape(view_groups * share, detector + 128)

    ramp, cosine, sine, first, wide_one, second, wide_two = prepare(
        member.astype(jnp.int32).reshape(1),
        conv_one,
        bias_one[None],
        conv_two,
        bias_two[None],
        view_groups * share,
        views_total,
        share,
        view_count,
    )
    first_row = (row_index - member) * ROW_DEV - 2
    first_y = first_row.astype(jnp.float32) - (image_rows - 1) / 2.0

    partial_rows = backproject(first_y.reshape(1), lines, cosine, sine, ramp)
    groups = [[GROUP * base + item for item in range(GROUP)] for base in range(row_groups // GROUP)]
    parts = lax.all_to_all(partial_rows, "rows", 0, 0, tiled=True, axis_index_groups=groups)

    row_base = (row_index * ROW_DEV).astype(jnp.int32).reshape(1)
    return layers(
        row_base,
        parts,
        first,
        wide_one,
        second,
        wide_two,
        math.pi / views_total,
        image_rows,
    )


def solution(mesh):
    return jax.shard_map(
        local,
        mesh=mesh,
        in_specs=(P(None, "views", None), P("views"), P(), P(), P(), P()),
        out_specs=P("views", None, "rows", None),
        check_vma=False,
    )
```

```python
import math

import jax
import jax.numpy as jnp
from jax import lax
from jax.experimental import pallas as pl
from jax.experimental.pallas import tpu as pltpu
from jax.sharding import PartitionSpec as P

BINS = 2048
WIDTH = 2048
MARGIN = 384
CHAN = 32
ROW_DEV = 4
GROUP = 4
BLOCK = 256
BLOCKS = BINS // BLOCK
CENTER = (BINS - 1) / 2.0 + MARGIN
FIRST_WIN = 4
WINDOWS = 38
TILES = WIDTH // 128
ROW_SETS = 3
RAMP_COLS = BLOCKS * BLOCK
VIEW_STEP = 64
SCALE_SET = 8
PARTS = 2


def selection(shape, test):
    row = lax.broadcasted_iota(jnp.int32, shape, 0)
    col = lax.broadcasted_iota(jnp.int32, shape, 1)
    return jnp.where(test(row, col), 1.0, 0.0)


def exact_dot(left, right, contract=(1, 0)):
    return lax.dot_general(
        left,
        right,
        (((contract[0],), (contract[1],)), ((), ())),
        precision=lax.Precision.HIGHEST,
        preferred_element_type=jnp.float32,
    )


def column_of(picker, row):
    return jnp.sum(picker * row, axis=1, keepdims=True)


def prepare_kernel(
    views_total,
    share,
    view_count,
    member_ref,
    conv_one_ref,
    bias_one_ref,
    conv_two_ref,
    bias_two_ref,
    table_ref,
    cos_ref,
    sin_ref,
    first_ref,
    wide_one_ref,
    second_ref,
    wide_two_ref,
):
    width = BLOCKS * BLOCK

    for turn in range(8):
        row = lax.broadcasted_iota(jnp.int32, (16, width + 128), 0)
        col = lax.broadcasted_iota(jnp.int32, (16, width + 128), 1)
        offset = col - row - (128 + 16 * turn)
        place = offset.astype(jnp.float32)
        guarded = jnp.maximum(place * place, 1.0)
        odd = (offset & 1) == 1
        values = jnp.where(odd, (-1.0 / (math.pi * math.pi)) / guarded, 0.0)
        values = jnp.where(offset == 0, 0.25, values)
        high = values.astype(jnp.bfloat16)
        low = (values - high.astype(jnp.float32)).astype(jnp.bfloat16)
        for half in range(2):
            start = 16 * turn + 128 * half
            cols = slice(128 - 128 * half, 128 - 128 * half + width)
            table_ref[start : start + 16, :] = high[:, cols]
            table_ref[BLOCK + start : BLOCK + start + 16, :] = low[:, cols]

    view = lax.broadcasted_iota(jnp.int32, cos_ref.shape, 0)
    view = view // share * view_count + member_ref[0] * share + view % share
    angle = view.astype(jnp.float32) * (math.pi / views_total)
    cos_ref[...] = jnp.cos(angle)
    sin_ref[...] = jnp.sin(angle)

    rows_one = CHAN * (ROW_DEV + 2)
    picker = selection((rows_one, CHAN), lambda row, col: (row & (CHAN - 1)) == col)
    wide_one_ref[...] = column_of(picker, bias_one_ref[...])
    taps = exact_dot(picker, conv_one_ref[...], (1, 1))
    weights = jnp.zeros((rows_one, 24), jnp.float32)
    for item in range(3):
        moved = exact_dot(taps, selection((9, 24), lambda row, col: row == 3 * item + (col >> 3)))
        keep = selection((rows_one, 24), lambda row, col: (col & 7) == (row >> 5) + item)
        weights = weights + moved * keep
    high = weights.astype(jnp.bfloat16)
    rest = weights - high.astype(jnp.float32)
    middle = rest.astype(jnp.bfloat16)
    low = (rest - middle.astype(jnp.float32)).astype(jnp.bfloat16)
    first_ref[...] = jnp.concatenate([high, middle, low], axis=1)

    rows_two = CHAN * ROW_DEV
    picker = selection((rows_two, CHAN), lambda row, col: (row >> 2) == col)
    wide_two_ref[...] = column_of(picker, bias_two_ref[...])
    spread = jnp.dot(
        picker.astype(jnp.bfloat16), conv_two_ref[...], preferred_element_type=jnp.float32
    ).astype(jnp.bfloat16)
    cols_two = CHAN * (ROW_DEV + 2)
    for tap in range(3):
        block = jnp.zeros((rows_two, cols_two), jnp.float32)
        for item in range(3):
            source = spread[:, (3 * item + tap) * CHAN : (3 * item + tap + 1) * CHAN]
            place = selection((CHAN, cols_two), lambda row, col: (col & (CHAN - 1)) == row)
            moved = jnp.dot(source, place.astype(jnp.bfloat16), preferred_element_type=jnp.float32)
            keep = selection((rows_two, cols_two), lambda row, col: (col >> 5) == (row & 3) + item)
            block = block + moved * keep
        second_ref[tap] = block.astype(jnp.bfloat16)


def prepare(member, conv_one, bias_one, conv_two, bias_two, views, views_total, share, view_count):
    vmem = pl.BlockSpec(memory_space=pltpu.VMEM)

    def body(*refs):
        prepare_kernel(views_total, share, view_count, *refs)

    rows_one, rows_two = CHAN * (ROW_DEV + 2), CHAN * ROW_DEV
    return pl.pallas_call(
        body,
        out_shape=(
            jax.ShapeDtypeStruct((2 * BLOCK, BLOCKS * BLOCK), jnp.bfloat16),
            jax.ShapeDtypeStruct((views, 128), jnp.float32),
            jax.ShapeDtypeStruct((views, 128), jnp.float32),
            jax.ShapeDtypeStruct((rows_one, 72), jnp.bfloat16),
            jax.ShapeDtypeStruct((rows_one, 1), jnp.float32),
            jax.ShapeDtypeStruct((3, rows_two, rows_one), jnp.bfloat16),
            jax.ShapeDtypeStruct((rows_two, 1), jnp.float32),
        ),
        in_specs=[pl.BlockSpec(memory_space=pltpu.SMEM)] + [vmem] * 4,
        out_specs=(vmem,) * 7,
        compiler_params=pltpu.CompilerParams(vmem_limit_bytes=16 * 2**20),
        cost_estimate=pl.CostEstimate(flops=20_000_000, bytes_accessed=4_000_000, transcendentals=0),
        name="prepare",
    )(member, conv_one, bias_one, conv_two, bias_two)


def dot_turned(left, right):
    return lax.dot_general(left, right, (((1,), (1,)), ((), ())), preferred_element_type=jnp.float32)


def lane_gather(words, index):
    dims = lax.GatherDimensionNumbers(
        offset_dims=(),
        collapsed_slice_dims=(1,),
        start_index_map=(1,),
        operand_batching_dims=(0,),
        start_indices_batching_dims=(0,),
    )
    return lax.gather(
        words, index[:, :, None], dims, (1, 1), mode=lax.GatherScatterMode.PROMISE_IN_BOUNDS
    )


def backproject_kernel(
    first_ref,
    x_ref,
    cos_ref,
    sin_ref,
    ramp_ref,
    out_ref,
    filt_ref,
    word_ref,
    bin_ref,
    back_ref,
    center_ref,
    where_ref,
    acc_ref,
    where_smem,
    sem,
):
    views = x_ref.shape[0]
    first_y = first_ref[0]
    lane = lax.broadcasted_iota(jnp.int32, (views, 128), 1)
    lane_f = lane.astype(jnp.float32)

    cosine = cos_ref[...]
    sine = sin_ref[...]
    center = CENTER + x_ref[:, BINS : BINS + 128].astype(jnp.float32)
    center_ref[...] = center
    tile_x = (lane & 15).astype(jnp.float32) * 128.0 - (WIDTH - 1) / 2.0
    set_y = first_y + 8.0 * (lane >> 4).astype(jnp.float32)
    lowest = jnp.minimum(tile_x * cosine, (tile_x + 127.0) * cosine) + set_y * sine + center
    window = ((lowest - 0.25) * (1.0 / 64.0)).astype(jnp.int32) - FIRST_WIN
    window = jnp.clip(window, 0, WINDOWS - 3)
    view = lax.broadcasted_iota(jnp.int32, (views, 128), 0)
    where_ref[...] = window * views + view
    to_smem = pltpu.make_async_copy(where_ref, where_smem, sem)
    to_smem.start()

    for step in range(2 * BLOCKS - 1):
        delta = (step + 1) // 2 * (1 if step % 2 else -1)
        low, high = max(0, -delta), min(BLOCKS, BLOCKS - delta)
        left = jnp.concatenate(
            [x_ref[:, BLOCK * block : BLOCK * block + BLOCK] for block in range(low, high)], axis=0
        )
        cols = slice(BLOCK * abs(delta), BLOCK * abs(delta) + BLOCK)
        if delta >= 0:
            left = jnp.concatenate([left, left], axis=1)
            part = jnp.dot(left, ramp_ref[:, cols], preferred_element_type=jnp.float32)
        else:
            part = dot_turned(left, ramp_ref[0:BLOCK, cols]) + dot_turned(left, ramp_ref[BLOCK:, cols])
        rows = slice(views * (low + delta), views * (high + delta))
        if delta == 0:
            filt_ref[rows, :] = part
        else:
            filt_ref[rows, :] += part

    margin = MARGIN // 128
    inner = BINS // 128

    def raw(place):
        half = 128 * (place % 2)
        piece = filt_ref[views * (place // 2) : views * (place // 2) + views, half : half + 128]
        return piece.astype(jnp.bfloat16).astype(jnp.float32)

    largest = jnp.abs(raw(0))
    for place in range(1, inner):
        largest = jnp.maximum(largest, jnp.abs(raw(place)))
    largest = jnp.max(largest, axis=1, keepdims=True)
    largest = jnp.max(largest.reshape(views // SCALE_SET, SCALE_SET, 1), axis=1, keepdims=True)
    largest = jnp.maximum(jnp.broadcast_to(largest, (views // SCALE_SET, SCALE_SET, 128)), 1e-30)
    largest = largest.reshape(views, 128)
    back_ref[...] = largest * (1.0 / (16383.0 * 65536.0))
    scale = 16383.0 / largest
    zero = jnp.zeros((views, 128), jnp.int32)

    def filtered(block):
        place = block - margin
        if place < 0 or place >= inner:
            return zero
        return jnp.floor(raw(place) * scale + 0.5).astype(jnp.int32)

    def turned(piece):
        return pltpu.roll(piece, 127, 1)

    def block_tables(block, piece, piece_turned, next_turned):
        step = jnp.where(lane < 127, piece_turned, next_turned) - piece
        return piece * 65536 + step, lane_f + (128.0 * block + 1.0)

    first_block = FIRST_WIN // 2
    piece = filtered(first_block)
    piece_turned = turned(piece)
    before = None
    for block in range(first_block, (FIRST_WIN + WINDOWS) // 2 + 1):
        following = filtered(block + 1)
        following_turned = turned(following)
        now = block_tables(block, piece, piece_turned, following_turned)
        for ref, value, old in zip((word_ref, bin_ref), now, before or now):
            row = (2 * block - FIRST_WIN) * views
            if before is not None:
                ref[row - views : row, :] = jnp.where(lane >= 64, old, value)
            if 2 * block < FIRST_WIN + WINDOWS:
                ref[row : row + views, :] = value
        before = now
        piece, piece_turned = following, following_turned

    acc_ref[...] = jnp.zeros_like(acc_ref)
    to_smem.wait()

    lane_one = lax.broadcasted_iota(jnp.int32, (8, 128), 1).astype(jnp.float32)
    sub_one = lax.broadcasted_iota(jnp.int32, (8, 128), 0).astype(jnp.float32)
    count = TILES // PARTS
    span = 128 * count
    top = lax.broadcasted_iota(jnp.int32, (8, 128), 0) < 4

    def spread(ref, row):
        return jnp.broadcast_to(ref[pl.ds(row, 1), :], (8, 128))

    def one_view(views_of, row_set, part, rows_y, totals):
        def both(ref, rows):
            if len(rows) == 1:
                return spread(ref, rows[0])
            return jnp.where(top, spread(ref, rows[0]), spread(ref, rows[1]))

        middle_x = part.astype(jnp.float32) * span + (span // 2 - WIDTH / 2.0 + 0.5)
        first_tile = row_set * TILES + part * count
        cos_v = both(cos_ref, views_of)
        base = rows_y * both(sin_ref, views_of) + both(center_ref, views_of)
        stride = cos_v * 128.0
        middle = (lane_one + middle_x) * cos_v + base
        middle_low = jnp.minimum(middle_x * cos_v, (middle_x + 127.0) * cos_v) + base
        for direction in (1, -1):
            place, place_low = middle, middle_low
            tiles = range(count // 2, count) if direction == 1 else range(count // 2 - 1, -1, -1)
            for tile in tiles:
                if direction == 1 and tile > count // 2:
                    place, place_low = place + stride, place_low + stride
                elif direction == -1:
                    place, place_low = place - stride, place_low - stride
                near = [where_smem[view, first_tile + tile] for view in views_of]
                far = [row + 2 * views for row in near]
                pick = both(bin_ref, near) > place_low
                words = jnp.where(pick, both(word_ref, near), both(word_ref, far))
                lower = place.astype(jnp.int32)
                word = lane_gather(words, lower & 127)
                value = word.astype(jnp.float32)
                along = place - lower.astype(jnp.float32)
                value = value + along * (word << 16).astype(jnp.float32)
                totals[tile] = value if totals[tile] is None else totals[tile] + value

    def add_up(block, first_view, totals):
        back = spread(back_ref, first_view)
        for tile in range(count):
            acc_ref[block, :, 128 * tile : 128 * tile + 128] += totals[tile] * back

    per_set = views // VIEW_STEP

    def steps(step, carry):
        block = step // per_set
        row_set = block // PARTS
        first_view = (step % per_set) * VIEW_STEP
        rows_y = sub_one + (first_y + 8.0 * row_set.astype(jnp.float32))
        for set_off in range(0, VIEW_STEP, SCALE_SET):
            totals = [None] * count
            for view_off in range(SCALE_SET):
                view = first_view + (set_off + view_off)
                one_view((view,), row_set, block % PARTS, rows_y, totals)
            add_up(block, first_view + set_off, totals)
        return carry

    lax.fori_loop(0, 2 * PARTS * per_set, steps, 0)

    def paired_steps(step, carry):
        part = step // per_set
        first_view = (step % per_set) * VIEW_STEP
        rows_y = jnp.where(top, sub_one, sub_one - 4.0) + (first_y + 16.0)
        for set_off in range(0, VIEW_STEP, SCALE_SET):
            totals = [None] * count
            for view_off in range(SCALE_SET // 2):
                view = first_view + (set_off + view_off)
                one_view((view, view + SCALE_SET // 2), 2, part, rows_y, totals)
            add_up(part + 2 * PARTS, first_view + set_off, totals)
        return carry

    lax.fori_loop(0, PARTS * per_set, paired_steps, 0)

    def rows_of(row_set, low, high):
        return jnp.concatenate(
            [acc_ref[row_set * PARTS + part, low:high, :] for part in range(PARTS)], axis=1
        )

    for member in range(GROUP):
        lower = rows_of(member // 2, 0, 8)
        if member == 1:
            lower = jnp.concatenate([rows_of(0, 4, 8), rows_of(1, 0, 4)], axis=0)
        elif member == 3:
            lower = jnp.concatenate([rows_of(1, 4, 8), rows_of(2, 0, 4) + rows_of(2, 4, 8)], axis=0)
        out_ref[member] = lower.astype(jnp.bfloat16)


def backproject(first_y, lines, cosine, sine, ramp):
    views = lines.shape[0]
    rows = WINDOWS * views
    vmem = pl.BlockSpec(memory_space=pltpu.VMEM)
    return pl.pallas_call(
        backproject_kernel,
        out_shape=jax.ShapeDtypeStruct((GROUP, 8, WIDTH), jnp.bfloat16),
        in_specs=[pl.BlockSpec(memory_space=pltpu.SMEM), vmem, vmem, vmem, vmem],
        out_specs=vmem,
        scratch_shapes=[
            pltpu.VMEM((BLOCKS * views, BLOCK), jnp.float32),
            pltpu.VMEM((rows, 128), jnp.int32),
            pltpu.VMEM((rows, 128), jnp.float32),
            pltpu.VMEM((views, 128), jnp.float32),
            pltpu.VMEM((views, 128), jnp.float32),
            pltpu.VMEM((views, 128), jnp.int32),
            pltpu.VMEM((ROW_SETS * PARTS, 8, WIDTH // PARTS), jnp.float32),
            pltpu.SMEM((views, 128), jnp.int32),
            pltpu.SemaphoreType.DMA(()),
        ],
        compiler_params=pltpu.CompilerParams(vmem_limit_bytes=16 * 2**20),
        cost_estimate=pl.CostEstimate(flops=1_000_000_000, bytes_accessed=6_000_000, transcendentals=0),
        name="backproject",
    )(first_y, lines, cosine, sine, ramp)


def layers_kernel(
    scale,
    image_rows,
    row_ref,
    parts_ref,
    first_ref,
    bias_one_ref,
    second_ref,
    bias_two_ref,
    out_ref,
    image_ref,
    stack_ref,
):
    row_base = row_ref[0]
    image = parts_ref[0].astype(jnp.float32)
    for member in range(1, GROUP):
        image = image + parts_ref[member].astype(jnp.float32)
    image = (image * scale).astype(jnp.bfloat16).astype(jnp.float32)
    row = lax.broadcasted_iota(jnp.int32, image.shape, 0) + (row_base - 2)
    image = jnp.where((row >= 0) & (row < image_rows), image, 0.0)
    column = lax.broadcasted_iota(jnp.int32, image.shape, 1)
    left = jnp.where(column == 0, 0.0, pltpu.roll(image, 1, 1))
    right = jnp.where(column == WIDTH - 1, 0.0, pltpu.roll(image, WIDTH - 1, 1))
    three = jnp.concatenate([left, image, right], axis=0).astype(jnp.bfloat16)
    image_ref[...] = jnp.concatenate([three, three, three], axis=0)

    weights = first_ref[...]
    count = CHAN * (ROW_DEV + 2)
    for tile in range(0, WIDTH, 256):
        hidden = jnp.dot(weights, image_ref[:, tile : tile + 256], preferred_element_type=jnp.float32)
        hidden = jnp.maximum(hidden + bias_one_ref[...], 0.0)
        top = jnp.where(row_base > 0, hidden[0:CHAN], 0.0)
        bottom = jnp.where(row_base + ROW_DEV < image_rows, hidden[count - CHAN : count], 0.0)
        hidden = jnp.concatenate([top, hidden[CHAN : count - CHAN], bottom], axis=0)
        stack_ref[:, tile : tile + 256] = hidden

    middle_rows = stack_ref[...]
    column = lax.broadcasted_iota(jnp.int32, middle_rows.shape, 1)
    before = jnp.where(column == 0, 0.0, pltpu.roll(middle_rows, 1, 1)).astype(jnp.bfloat16)
    after = jnp.where(column == WIDTH - 1, 0.0, pltpu.roll(middle_rows, WIDTH - 1, 1)).astype(jnp.bfloat16)
    mixed = jnp.dot(second_ref[0], before, preferred_element_type=jnp.float32)
    mixed = mixed + jnp.dot(second_ref[1], middle_rows.astype(jnp.bfloat16), preferred_element_type=jnp.float32)
    mixed = mixed + jnp.dot(second_ref[2], after, preferred_element_type=jnp.float32)
    mixed = jnp.maximum(mixed + bias_two_ref[...], 0.0)
    out_ref[...] = mixed.reshape(CHAN, ROW_DEV, WIDTH).astype(jnp.bfloat16)[None]


def layers(row_base, parts, first, bias_one, second, bias_two, scale, image_rows):
    vmem = pl.BlockSpec(memory_space=pltpu.VMEM)

    def body(*refs):
        layers_kernel(scale, image_rows, *refs)

    return pl.pallas_call(
        body,
        out_shape=jax.ShapeDtypeStruct((1, CHAN, ROW_DEV, WIDTH), jnp.bfloat16),
        in_specs=[pl.BlockSpec(memory_space=pltpu.SMEM)] + [vmem] * 5,
        out_specs=vmem,
        scratch_shapes=[
            pltpu.VMEM((72, WIDTH), jnp.bfloat16),
            pltpu.VMEM((CHAN * (ROW_DEV + 2), WIDTH), jnp.float32),
        ],
        compiler_params=pltpu.CompilerParams(vmem_limit_bytes=16 * 2**20),
        cost_estimate=pl.CostEstimate(flops=500_000_000, bytes_accessed=1_000_000, transcendentals=0),
        name="layers",
    )(row_base, parts, first, bias_one, second, bias_two)


def local(sinogram, view_shift, conv_one, bias_one, conv_two, bias_two):
    sheets, view_count, detector = sinogram.shape
    row_groups = lax.axis_size("rows")
    view_groups = lax.axis_size("views")
    views_total = view_count * view_groups
    image_rows = ROW_DEV * row_groups
    share = view_count // GROUP
    row_index = lax.axis_index("rows")
    member = row_index % GROUP

    mine = lax.dynamic_slice_in_dim(sinogram, member * share, share, 1)
    shift = lax.dynamic_slice_in_dim(view_shift, member * share, share, 0).astype(jnp.bfloat16)
    shift = jnp.broadcast_to(shift[None, :, None], (sheets, share, 128))
    sent = jnp.concatenate([mine, shift], axis=2)
    lines = lax.all_to_all(sent, "views", 0, 0, tiled=True)
    lines = lines.reshape(view_groups * share, detector + 128)

    ramp, cosine, sine, first, wide_one, second, wide_two = prepare(
        member.astype(jnp.int32).reshape(1),
        conv_one,
        bias_one[None],
        conv_two,
        bias_two[None],
        view_groups * share,
        views_total,
        share,
        view_count,
    )
    first_row = (row_index - member) * ROW_DEV - 2
    first_y = first_row.astype(jnp.float32) - (image_rows - 1) / 2.0

    partial_rows = backproject(first_y.reshape(1), lines, cosine, sine, ramp)
    groups = [[GROUP * base + item for item in range(GROUP)] for base in range(row_groups // GROUP)]
    parts = lax.all_to_all(partial_rows, "rows", 0, 0, tiled=True, axis_index_groups=groups)

    row_base = (row_index * ROW_DEV).astype(jnp.int32).reshape(1)
    return layers(
        row_base,
        parts,
        first,
        wide_one,
        second,
        wide_two,
        math.pi / views_total,
        image_rows,
    )


def solution(mesh):
    return jax.shard_map(
        local,
        mesh=mesh,
        in_specs=(P(None, "views", None), P("views"), P(), P(), P(), P()),
        out_specs=P("views", None, "rows", None),
        check_vma=False,
    )
```

```python
import math

import jax
import jax.numpy as jnp
from jax import lax
from jax.experimental import pallas as pl
from jax.experimental.pallas import tpu as pltpu
from jax.sharding import PartitionSpec as P

BINS = 2048
WIDTH = 2048
MARGIN = 384
CHAN = 32
ROW_DEV = 4
GROUP = 4
BLOCK = 256
BLOCKS = BINS // BLOCK
CENTER = (BINS - 1) / 2.0 + MARGIN
FIRST_WIN = 4
WINDOWS = 38
TILES = WIDTH // 128
ROW_SETS = 3
RAMP_COLS = BLOCKS * BLOCK
VIEW_STEP = 64
SCALE_SET = 8
PARTS = 2


def selection(shape, test):
    row = lax.broadcasted_iota(jnp.int32, shape, 0)
    col = lax.broadcasted_iota(jnp.int32, shape, 1)
    return jnp.where(test(row, col), 1.0, 0.0)


def exact_dot(left, right, contract=(1, 0)):
    return lax.dot_general(
        left,
        right,
        (((contract[0],), (contract[1],)), ((), ())),
        precision=lax.Precision.HIGHEST,
        preferred_element_type=jnp.float32,
    )


def column_of(picker, row):
    return jnp.sum(picker * row, axis=1, keepdims=True)


def pack_kernel(member_ref, shift_ref, x_ref, out_ref):
    sheets, views, bins = x_ref.shape
    share = out_ref.shape[1]
    for member in range(views // share):

        @pl.when(member_ref[0] == member)
        def copy_rows():
            out_ref[:, :, 0:bins] = x_ref[:, member * share : member * share + share, :]

    lane = lax.broadcasted_iota(jnp.int32, (1, share, 128), 2)
    shifts = jnp.zeros((1, share, 128), jnp.float32)
    for view in range(views):
        shifts = jnp.where(lane == view, shift_ref[view].astype(jnp.float32), shifts)
    shifts = jnp.broadcast_to(shifts.astype(jnp.bfloat16), (sheets, share, 128))
    out_ref[:, :, bins : bins + 128] = shifts


def pack(member, view_shift, sinogram, share):
    sheets, views, bins = sinogram.shape
    smem = pl.BlockSpec(memory_space=pltpu.SMEM)
    vmem = pl.BlockSpec(memory_space=pltpu.VMEM)
    return pl.pallas_call(
        pack_kernel,
        out_shape=jax.ShapeDtypeStruct((sheets, share, bins + 128), jnp.bfloat16),
        in_specs=[smem, smem, vmem],
        out_specs=vmem,
        compiler_params=pltpu.CompilerParams(vmem_limit_bytes=8 * 2**20),
        cost_estimate=pl.CostEstimate(flops=1_000_000, bytes_accessed=1_500_000, transcendentals=0),
        name="pack",
    )(member, view_shift, sinogram)


def prepare_kernel(
    views_total,
    share,
    view_count,
    member_ref,
    table_ref,
    trig_ref,
):
    width = BLOCKS * BLOCK

    for turn in range(8):
        row = lax.broadcasted_iota(jnp.int32, (16, width + 128), 0)
        col = lax.broadcasted_iota(jnp.int32, (16, width + 128), 1)
        offset = col - row - (128 + 16 * turn)
        place = offset.astype(jnp.float32)
        guarded = jnp.maximum(place * place, 1.0)
        odd = (offset & 1) == 1
        values = jnp.where(odd, (-1.0 / (math.pi * math.pi)) / guarded, 0.0)
        values = jnp.where(offset == 0, 0.25, values)
        high = values.astype(jnp.bfloat16)
        low = (values - high.astype(jnp.float32)).astype(jnp.bfloat16)
        for half in range(2):
            start = 16 * turn + 128 * half
            cols = slice(128 - 128 * half, 128 - 128 * half + width)
            table_ref[start : start + 16, :] = high[:, cols]
            table_ref[BLOCK + start : BLOCK + start + 16, :] = low[:, cols]

    views = trig_ref.shape[0] // 2
    view = lax.broadcasted_iota(jnp.int32, (views, 128), 0)
    view = view // share * view_count + member_ref[0] * share + view % share
    angle = view.astype(jnp.float32) * (math.pi / views_total)
    trig_ref[0:views, :] = jnp.cos(angle)
    trig_ref[views : 2 * views, :] = jnp.sin(angle)


def weights_kernel(
    after_ref,
    conv_one_ref,
    bias_one_ref,
    conv_two_ref,
    bias_two_ref,
    first_ref,
    wide_one_ref,
    second_ref,
    wide_two_ref,
):
    del after_ref
    rows_one = CHAN * (ROW_DEV + 2)
    picker = selection((rows_one, CHAN), lambda row, col: (row & (CHAN - 1)) == col)
    wide_one_ref[...] = column_of(picker, bias_one_ref[...])
    taps = exact_dot(picker, conv_one_ref[...], (1, 1))
    weights = jnp.zeros((rows_one, 24), jnp.float32)
    for item in range(3):
        moved = exact_dot(taps, selection((9, 24), lambda row, col: row == 3 * item + (col >> 3)))
        keep = selection((rows_one, 24), lambda row, col: (col & 7) == (row >> 5) + item)
        weights = weights + moved * keep
    high = weights.astype(jnp.bfloat16)
    rest = weights - high.astype(jnp.float32)
    middle = rest.astype(jnp.bfloat16)
    low = (rest - middle.astype(jnp.float32)).astype(jnp.bfloat16)
    first_ref[...] = jnp.concatenate([high, middle, low], axis=1)

    rows_two = CHAN * ROW_DEV
    picker = selection((rows_two, CHAN), lambda row, col: (row >> 2) == col)
    wide_two_ref[...] = column_of(picker, bias_two_ref[...])
    spread = jnp.dot(
        picker.astype(jnp.bfloat16), conv_two_ref[...], preferred_element_type=jnp.float32
    ).astype(jnp.bfloat16)
    cols_two = CHAN * (ROW_DEV + 2)
    for tap in range(3):
        block = jnp.zeros((rows_two, cols_two), jnp.float32)
        for item in range(3):
            source = spread[:, (3 * item + tap) * CHAN : (3 * item + tap + 1) * CHAN]
            place = selection((CHAN, cols_two), lambda row, col: (col & (CHAN - 1)) == row)
            moved = jnp.dot(source, place.astype(jnp.bfloat16), preferred_element_type=jnp.float32)
            keep = selection((rows_two, cols_two), lambda row, col: (col >> 5) == (row & 3) + item)
            block = block + moved * keep
        second_ref[tap] = block.astype(jnp.bfloat16)


def prepare(member, views, views_total, share, view_count):
    vmem = pl.BlockSpec(memory_space=pltpu.VMEM)

    def body(*refs):
        prepare_kernel(views_total, share, view_count, *refs)

    return pl.pallas_call(
        body,
        out_shape=(
            jax.ShapeDtypeStruct((2 * BLOCK, BLOCKS * BLOCK), jnp.bfloat16),
            jax.ShapeDtypeStruct((2 * views, 128), jnp.float32),
        ),
        in_specs=[pl.BlockSpec(memory_space=pltpu.SMEM)],
        out_specs=(vmem,) * 2,
        compiler_params=pltpu.CompilerParams(vmem_limit_bytes=8 * 2**20),
        cost_estimate=pl.CostEstimate(flops=20_000_000, bytes_accessed=4_000_000, transcendentals=0),
        name="prepare",
    )(member)


def spread_weights(after, conv_one, bias_one, conv_two, bias_two):
    vmem = pl.BlockSpec(memory_space=pltpu.VMEM)
    rows_one, rows_two = CHAN * (ROW_DEV + 2), CHAN * ROW_DEV
    return pl.pallas_call(
        weights_kernel,
        out_shape=(
            jax.ShapeDtypeStruct((rows_one, 72), jnp.bfloat16),
            jax.ShapeDtypeStruct((rows_one, 1), jnp.float32),
            jax.ShapeDtypeStruct((3, rows_two, rows_one), jnp.bfloat16),
            jax.ShapeDtypeStruct((rows_two, 1), jnp.float32),
        ),
        in_specs=[pl.BlockSpec(memory_space=pl.ANY)] + [vmem] * 4,
        out_specs=(vmem,) * 4,
        compiler_params=pltpu.CompilerParams(vmem_limit_bytes=8 * 2**20),
        cost_estimate=pl.CostEstimate(flops=20_000_000, bytes_accessed=1_000_000, transcendentals=0),
        name="weights",
    )(after, conv_one, bias_one, conv_two, bias_two)


def dot_turned(left, right):
    return lax.dot_general(left, right, (((1,), (1,)), ((), ())), preferred_element_type=jnp.float32)


def lane_gather(words, index):
    dims = lax.GatherDimensionNumbers(
        offset_dims=(),
        collapsed_slice_dims=(1,),
        start_index_map=(1,),
        operand_batching_dims=(0,),
        start_indices_batching_dims=(0,),
    )
    return lax.gather(
        words, index[:, :, None], dims, (1, 1), mode=lax.GatherScatterMode.PROMISE_IN_BOUNDS
    )


def backproject_kernel(
    first_ref,
    member_ref,
    x_ref,
    trig_ref,
    ramp_ref,
    out_ref,
    filt_ref,
    word_ref,
    bin_ref,
    back_ref,
    center_ref,
    where_ref,
    acc_ref,
    where_smem,
    sem,
):
    share = x_ref.shape[1]
    views = x_ref.shape[0] * share
    first_y = first_ref[0]
    lane = lax.broadcasted_iota(jnp.int32, (views, 128), 1)
    lane_f = lane.astype(jnp.float32)

    cosine = trig_ref[0:views, :]
    sine = trig_ref[views : 2 * views, :]
    view = lax.broadcasted_iota(jnp.int32, (views, 128), 0)
    shifts = x_ref[:, :, BINS : BINS + 128].reshape(views, 128).astype(jnp.float32)
    own = lane == member_ref[0] * 2 + (view & 1)
    center = CENTER + jnp.sum(jnp.where(own, shifts, 0.0), axis=1, keepdims=True)
    center = jnp.broadcast_to(center, (views, 128))
    center_ref[...] = center
    tile_x = (lane & 15).astype(jnp.float32) * 128.0 - (WIDTH - 1) / 2.0
    set_y = first_y + 8.0 * (lane >> 4).astype(jnp.float32)
    lowest = jnp.minimum(tile_x * cosine, (tile_x + 127.0) * cosine) + set_y * sine + center
    window = ((lowest - 0.25) * (1.0 / 64.0)).astype(jnp.int32) - FIRST_WIN
    window = jnp.clip(window, 0, WINDOWS - 3)
    where_ref[...] = window * views + view
    to_smem = pltpu.make_async_copy(where_ref, where_smem, sem)
    to_smem.start()

    @pl.when(member_ref[0] >= 0)
    def filter_and_tables():
        pieces = [
            x_ref[:, :, BLOCK * block : BLOCK * block + BLOCK].reshape(views, BLOCK)
            for block in range(BLOCKS)
        ]
        for step in range(2 * BLOCKS - 1):
            delta = (step + 1) // 2 * (1 if step % 2 else -1)
            low, high = max(0, -delta), min(BLOCKS, BLOCKS - delta)
            left = jnp.concatenate(
                [pieces[block] for block in range(low, high)], axis=0
            )
            cols = slice(BLOCK * abs(delta), BLOCK * abs(delta) + BLOCK)
            if delta >= 0:
                left = jnp.concatenate([left, left], axis=1)
                part = jnp.dot(left, ramp_ref[:, cols], preferred_element_type=jnp.float32)
            else:
                part = dot_turned(left, ramp_ref[0:BLOCK, cols]) + dot_turned(left, ramp_ref[BLOCK:, cols])
            rows = slice(views * (low + delta), views * (high + delta))
            if delta == 0:
                filt_ref[rows, :] = part
            else:
                filt_ref[rows, :] += part

        margin = MARGIN // 128
        inner = BINS // 128

        def raw(place):
            half = 128 * (place % 2)
            piece = filt_ref[views * (place // 2) : views * (place // 2) + views, half : half + 128]
            return piece.astype(jnp.bfloat16).astype(jnp.float32)

        largest = jnp.abs(raw(0))
        for place in range(1, inner):
            largest = jnp.maximum(largest, jnp.abs(raw(place)))
        largest = jnp.max(largest, axis=1, keepdims=True)
        largest = jnp.max(largest.reshape(views // SCALE_SET, SCALE_SET, 1), axis=1, keepdims=True)
        largest = jnp.maximum(jnp.broadcast_to(largest, (views // SCALE_SET, SCALE_SET, 128)), 1e-30)
        largest = largest.reshape(views, 128)
        back_ref[...] = largest * (1.0 / (16383.0 * 65536.0))
        scale = 16383.0 / largest
        zero = jnp.zeros((views, 128), jnp.int32)

        def filtered(block):
            place = block - margin
            if place < 0 or place >= inner:
                return zero
            return jnp.floor(raw(place) * scale + 0.5).astype(jnp.int32)

        def turned(piece):
            return pltpu.roll(piece, 127, 1)

        def block_tables(block, piece, piece_turned, next_turned):
            step = jnp.where(lane < 127, piece_turned, next_turned) - piece
            return piece * 65536 + step, lane_f + (128.0 * block + 1.0)

        first_block = FIRST_WIN // 2
        piece = filtered(first_block)
        piece_turned = turned(piece)
        before = None
        for block in range(first_block, (FIRST_WIN + WINDOWS) // 2 + 1):
            following = filtered(block + 1)
            following_turned = turned(following)
            now = block_tables(block, piece, piece_turned, following_turned)
            for ref, value, old in zip((word_ref, bin_ref), now, before or now):
                row = (2 * block - FIRST_WIN) * views
                if before is not None:
                    ref[row - views : row, :] = jnp.where(lane >= 64, old, value)
                if 2 * block < FIRST_WIN + WINDOWS:
                    ref[row : row + views, :] = value
            before = now
            piece, piece_turned = following, following_turned

    acc_ref[...] = jnp.zeros_like(acc_ref)
    to_smem.wait()

    lane_one = lax.broadcasted_iota(jnp.int32, (8, 128), 1).astype(jnp.float32)
    sub_one = lax.broadcasted_iota(jnp.int32, (8, 128), 0).astype(jnp.float32)
    count = TILES // PARTS
    span = 128 * count
    top = lax.broadcasted_iota(jnp.int32, (8, 128), 0) < 4

    def spread(ref, row):
        return jnp.broadcast_to(ref[pl.ds(row, 1), :], (8, 128))

    def one_view(views_of, row_set, part, rows_y, totals):
        def both(ref, rows):
            if len(rows) == 1:
                return spread(ref, rows[0])
            return jnp.where(top, spread(ref, rows[0]), spread(ref, rows[1]))

        middle_x = part.astype(jnp.float32) * span + (span // 2 - WIDTH / 2.0 + 0.5)
        first_tile = row_set * TILES + part * count
        cos_v = both(trig_ref, views_of)
        base = rows_y * both(trig_ref, [views + view for view in views_of]) + both(center_ref, views_of)
        stride = cos_v * 128.0
        middle = (lane_one + middle_x) * cos_v + base
        middle_low = jnp.minimum(middle_x * cos_v, (middle_x + 127.0) * cos_v) + base
        for direction in (1, -1):
            place, place_low = middle, middle_low
            tiles = range(count // 2, count) if direction == 1 else range(count // 2 - 1, -1, -1)
            for tile in tiles:
                if direction == 1 and tile > count // 2:
                    place, place_low = place + stride, place_low + stride
                elif direction == -1:
                    place, place_low = place - stride, place_low - stride
                near = [where_smem[view, first_tile + tile] for view in views_of]
                far = [row + 2 * views for row in near]
                pick = both(bin_ref, near) > place_low
                words = jnp.where(pick, both(word_ref, near), both(word_ref, far))
                lower = place.astype(jnp.int32)
                word = lane_gather(words, lower & 127)
                value = word.astype(jnp.float32)
                along = place - lower.astype(jnp.float32)
                value = value + along * (word << 16).astype(jnp.float32)
                totals[tile] = value if totals[tile] is None else totals[tile] + value

    def add_up(block, first_view, totals):
        back = spread(back_ref, first_view)
        for tile in range(count):
            acc_ref[block, :, 128 * tile : 128 * tile + 128] += totals[tile] * back

    per_set = views // VIEW_STEP

    def steps(step, carry):
        block = step // per_set
        row_set = block // PARTS
        first_view = (step % per_set) * VIEW_STEP
        rows_y = sub_one + (first_y + 8.0 * row_set.astype(jnp.float32))
        for set_off in range(0, VIEW_STEP, SCALE_SET):
            totals = [None] * count
            for view_off in range(SCALE_SET):
                view = first_view + (set_off + view_off)
                one_view((view,), row_set, block % PARTS, rows_y, totals)
            add_up(block, first_view + set_off, totals)
        return carry

    lax.fori_loop(0, 2 * PARTS * per_set, steps, 0)

    def paired_steps(step, carry):
        part = step // per_set
        first_view = (step % per_set) * VIEW_STEP
        rows_y = jnp.where(top, sub_one, sub_one - 4.0) + (first_y + 16.0)
        for set_off in range(0, VIEW_STEP, SCALE_SET):
            totals = [None] * count
            for view_off in range(SCALE_SET // 2):
                view = first_view + (set_off + view_off)
                one_view((view, view + SCALE_SET // 2), 2, part, rows_y, totals)
            add_up(part + 2 * PARTS, first_view + set_off, totals)
        return carry

    lax.fori_loop(0, PARTS * per_set, paired_steps, 0)

    def rows_of(row_set, low, high):
        return jnp.concatenate(
            [acc_ref[row_set * PARTS + part, low:high, :] for part in range(PARTS)], axis=1
        )

    for member in range(GROUP):
        lower = rows_of(member // 2, 0, 8)
        if member == 1:
            lower = jnp.concatenate([rows_of(0, 4, 8), rows_of(1, 0, 4)], axis=0)
        elif member == 3:
            lower = jnp.concatenate([rows_of(1, 4, 8), rows_of(2, 0, 4) + rows_of(2, 4, 8)], axis=0)
        out_ref[member] = lower.astype(jnp.bfloat16)


def backproject(first_y, member, lines, trig, ramp):
    views = lines.shape[0] * lines.shape[1]
    rows = WINDOWS * views
    vmem = pl.BlockSpec(memory_space=pltpu.VMEM)
    return pl.pallas_call(
        backproject_kernel,
        out_shape=jax.ShapeDtypeStruct((GROUP, 8, WIDTH), jnp.bfloat16),
        in_specs=[pl.BlockSpec(memory_space=pltpu.SMEM)] * 2 + [vmem] * 3,
        out_specs=vmem,
        scratch_shapes=[
            pltpu.VMEM((BLOCKS * views, BLOCK), jnp.float32),
            pltpu.VMEM((rows, 128), jnp.int32),
            pltpu.VMEM((rows, 128), jnp.float32),
            pltpu.VMEM((views, 128), jnp.float32),
            pltpu.VMEM((views, 128), jnp.float32),
            pltpu.VMEM((views, 128), jnp.int32),
            pltpu.VMEM((ROW_SETS * PARTS, 8, WIDTH // PARTS), jnp.float32),
            pltpu.SMEM((views, 128), jnp.int32),
            pltpu.SemaphoreType.DMA(()),
        ],
        compiler_params=pltpu.CompilerParams(vmem_limit_bytes=16 * 2**20),
        cost_estimate=pl.CostEstimate(flops=1_000_000_000, bytes_accessed=6_000_000, transcendentals=0),
        name="backproject",
    )(first_y, member, lines, trig, ramp)


def layers_kernel(
    scale,
    image_rows,
    row_ref,
    parts_ref,
    first_ref,
    bias_one_ref,
    second_ref,
    bias_two_ref,
    out_ref,
    image_ref,
    stack_ref,
):
    row_base = row_ref[0]
    image = parts_ref[0].astype(jnp.float32)
    for member in range(1, GROUP):
        image = image + parts_ref[member].astype(jnp.float32)
    image = (image * scale).astype(jnp.bfloat16).astype(jnp.float32)
    row = lax.broadcasted_iota(jnp.int32, image.shape, 0) + (row_base - 2)
    image = jnp.where((row >= 0) & (row < image_rows), image, 0.0)
    column = lax.broadcasted_iota(jnp.int32, image.shape, 1)
    left = jnp.where(column == 0, 0.0, pltpu.roll(image, 1, 1))
    right = jnp.where(column == WIDTH - 1, 0.0, pltpu.roll(image, WIDTH - 1, 1))
    three = jnp.concatenate([left, image, right], axis=0).astype(jnp.bfloat16)
    image_ref[...] = jnp.concatenate([three, three, three], axis=0)

    weights = first_ref[...]
    count = CHAN * (ROW_DEV + 2)
    for tile in range(0, WIDTH, 256):
        hidden = jnp.dot(weights, image_ref[:, tile : tile + 256], preferred_element_type=jnp.float32)
        hidden = jnp.maximum(hidden + bias_one_ref[...], 0.0)
        top = jnp.where(row_base > 0, hidden[0:CHAN], 0.0)
        bottom = jnp.where(row_base + ROW_DEV < image_rows, hidden[count - CHAN : count], 0.0)
        hidden = jnp.concatenate([top, hidden[CHAN : count - CHAN], bottom], axis=0)
        stack_ref[:, tile : tile + 256] = hidden

    middle_rows = stack_ref[...]
    column = lax.broadcasted_iota(jnp.int32, middle_rows.shape, 1)
    before = jnp.where(column == 0, 0.0, pltpu.roll(middle_rows, 1, 1)).astype(jnp.bfloat16)
    after = jnp.where(column == WIDTH - 1, 0.0, pltpu.roll(middle_rows, WIDTH - 1, 1)).astype(jnp.bfloat16)
    mixed = jnp.dot(second_ref[0], before, preferred_element_type=jnp.float32)
    mixed = mixed + jnp.dot(second_ref[1], middle_rows.astype(jnp.bfloat16), preferred_element_type=jnp.float32)
    mixed = mixed + jnp.dot(second_ref[2], after, preferred_element_type=jnp.float32)
    mixed = jnp.maximum(mixed + bias_two_ref[...], 0.0)
    out_ref[...] = mixed.reshape(CHAN, ROW_DEV, WIDTH).astype(jnp.bfloat16)[None]


def layers(row_base, parts, first, bias_one, second, bias_two, scale, image_rows):
    vmem = pl.BlockSpec(memory_space=pltpu.VMEM)

    def body(*refs):
        layers_kernel(scale, image_rows, *refs)

    return pl.pallas_call(
        body,
        out_shape=jax.ShapeDtypeStruct((1, CHAN, ROW_DEV, WIDTH), jnp.bfloat16),
        in_specs=[pl.BlockSpec(memory_space=pltpu.SMEM)] + [vmem] * 5,
        out_specs=vmem,
        scratch_shapes=[
            pltpu.VMEM((72, WIDTH), jnp.bfloat16),
            pltpu.VMEM((CHAN * (ROW_DEV + 2), WIDTH), jnp.float32),
        ],
        compiler_params=pltpu.CompilerParams(vmem_limit_bytes=16 * 2**20),
        cost_estimate=pl.CostEstimate(flops=500_000_000, bytes_accessed=1_000_000, transcendentals=0),
        name="layers",
    )(row_base, parts, first, bias_one, second, bias_two)


def local(sinogram, view_shift, conv_one, bias_one, conv_two, bias_two):
    sheets, view_count, detector = sinogram.shape
    row_groups = lax.axis_size("rows")
    view_groups = lax.axis_size("views")
    views_total = view_count * view_groups
    image_rows = ROW_DEV * row_groups
    share = view_count // GROUP
    row_index = lax.axis_index("rows")
    member = row_index % GROUP

    member_one = member.astype(jnp.int32).reshape(1)
    sent = pack(member_one, view_shift, sinogram, share)
    lines = lax.all_to_all(sent, "views", 0, 0, tiled=True)

    ramp, trig = prepare(member_one, view_groups * share, views_total, share, view_count)
    first_row = (row_index - member) * ROW_DEV - 2
    first_y = first_row.astype(jnp.float32) - (image_rows - 1) / 2.0

    partial_rows = backproject(first_y.reshape(1), member_one, lines, trig, ramp)
    groups = [[GROUP * base + item for item in range(GROUP)] for base in range(row_groups // GROUP)]
    parts = lax.all_to_all(partial_rows, "rows", 0, 0, tiled=True, axis_index_groups=groups)

    first, wide_one, second, wide_two = spread_weights(
        partial_rows, conv_one, bias_one[None], conv_two, bias_two[None]
    )
    row_base = (row_index * ROW_DEV).astype(jnp.int32).reshape(1)
    return layers(
        row_base,
        parts,
        first,
        wide_one,
        second,
        wide_two,
        math.pi / views_total,
        image_rows,
    )


def solution(mesh):
    return jax.shard_map(
        local,
        mesh=mesh,
        in_specs=(P(None, "views", None), P("views"), P(), P(), P(), P()),
        out_specs=P("views", None, "rows", None),
        check_vma=False,
    )
```

```python
import math

import jax
import jax.numpy as jnp
from jax import lax
from jax.experimental import pallas as pl
from jax.experimental.pallas import tpu as pltpu
from jax.sharding import PartitionSpec as P

BINS = 2048
WIDTH = 2048
MARGIN = 384
CHAN = 32
ROW_DEV = 4
GROUP = 4
BLOCK = 256
BLOCKS = BINS // BLOCK
CENTER = (BINS - 1) / 2.0 + MARGIN
FIRST_WIN = 4
WINDOWS = 38
TILES = WIDTH // 128
ROW_SETS = 3
RAMP_COLS = BLOCKS * BLOCK
VIEW_STEP = 64
SCALE_SET = 8
PARTS = 2


def selection(shape, test):
    row = lax.broadcasted_iota(jnp.int32, shape, 0)
    col = lax.broadcasted_iota(jnp.int32, shape, 1)
    return jnp.where(test(row, col), 1.0, 0.0)


def exact_dot(left, right, contract=(1, 0)):
    return lax.dot_general(
        left,
        right,
        (((contract[0],), (contract[1],)), ((), ())),
        precision=lax.Precision.HIGHEST,
        preferred_element_type=jnp.float32,
    )


def column_of(picker, row):
    return jnp.sum(picker * row, axis=1, keepdims=True)


def prepare_kernel(
    views_total,
    share,
    view_count,
    member_ref,
    table_ref,
    trig_ref,
):
    width = BLOCKS * BLOCK

    for turn in range(8):
        row = lax.broadcasted_iota(jnp.int32, (16, width + 128), 0)
        col = lax.broadcasted_iota(jnp.int32, (16, width + 128), 1)
        offset = col - row - (128 + 16 * turn)
        place = offset.astype(jnp.float32)
        guarded = jnp.maximum(place * place, 1.0)
        odd = (offset & 1) == 1
        values = jnp.where(odd, (-1.0 / (math.pi * math.pi)) / guarded, 0.0)
        values = jnp.where(offset == 0, 0.25, values)
        high = values.astype(jnp.bfloat16)
        low = (values - high.astype(jnp.float32)).astype(jnp.bfloat16)
        for half in range(2):
            start = 16 * turn + 128 * half
            cols = slice(128 - 128 * half, 128 - 128 * half + width)
            table_ref[start : start + 16, :] = high[:, cols]
            table_ref[BLOCK + start : BLOCK + start + 16, :] = low[:, cols]

    views = trig_ref.shape[0] // 2
    view = lax.broadcasted_iota(jnp.int32, (views, 128), 0)
    view = view // share * view_count + member_ref[0] * share + view % share
    angle = view.astype(jnp.float32) * (math.pi / views_total)
    trig_ref[0:views, :] = jnp.cos(angle)
    trig_ref[views : 2 * views, :] = jnp.sin(angle)


def weights_kernel(
    after_ref,
    conv_one_ref,
    bias_one_ref,
    conv_two_ref,
    bias_two_ref,
    first_ref,
    wide_one_ref,
    second_ref,
    wide_two_ref,
):
    del after_ref
    rows_one = CHAN * (ROW_DEV + 2)
    picker = selection((rows_one, CHAN), lambda row, col: (row & (CHAN - 1)) == col)
    wide_one_ref[...] = column_of(picker, bias_one_ref[...])
    taps = exact_dot(picker, conv_one_ref[...], (1, 1))
    weights = jnp.zeros((rows_one, 24), jnp.float32)
    for item in range(3):
        moved = exact_dot(taps, selection((9, 24), lambda row, col: row == 3 * item + (col >> 3)))
        keep = selection((rows_one, 24), lambda row, col: (col & 7) == (row >> 5) + item)
        weights = weights + moved * keep
    high = weights.astype(jnp.bfloat16)
    rest = weights - high.astype(jnp.float32)
    middle = rest.astype(jnp.bfloat16)
    low = (rest - middle.astype(jnp.float32)).astype(jnp.bfloat16)
    first_ref[...] = jnp.concatenate([high, middle, low], axis=1)

    rows_two = CHAN * ROW_DEV
    picker = selection((rows_two, CHAN), lambda row, col: (row >> 2) == col)
    wide_two_ref[...] = column_of(picker, bias_two_ref[...])
    spread = jnp.dot(
        picker.astype(jnp.bfloat16), conv_two_ref[...], preferred_element_type=jnp.float32
    ).astype(jnp.bfloat16)
    cols_two = CHAN * (ROW_DEV + 2)
    for tap in range(3):
        block = jnp.zeros((rows_two, cols_two), jnp.float32)
        for item in range(3):
            source = spread[:, (3 * item + tap) * CHAN : (3 * item + tap + 1) * CHAN]
            place = selection((CHAN, cols_two), lambda row, col: (col & (CHAN - 1)) == row)
            moved = jnp.dot(source, place.astype(jnp.bfloat16), preferred_element_type=jnp.float32)
            keep = selection((rows_two, cols_two), lambda row, col: (col >> 5) == (row & 3) + item)
            block = block + moved * keep
        second_ref[tap] = block.astype(jnp.bfloat16)


def prepare(member, views, views_total, share, view_count):
    vmem = pl.BlockSpec(memory_space=pltpu.VMEM)

    def body(*refs):
        prepare_kernel(views_total, share, view_count, *refs)

    return pl.pallas_call(
        body,
        out_shape=(
            jax.ShapeDtypeStruct((2 * BLOCK, BLOCKS * BLOCK), jnp.bfloat16),
            jax.ShapeDtypeStruct((2 * views, 128), jnp.float32),
        ),
        in_specs=[pl.BlockSpec(memory_space=pltpu.SMEM)],
        out_specs=(vmem,) * 2,
        compiler_params=pltpu.CompilerParams(vmem_limit_bytes=8 * 2**20),
        cost_estimate=pl.CostEstimate(flops=20_000_000, bytes_accessed=4_000_000, transcendentals=0),
        name="prepare",
    )(member)


def spread_weights(after, conv_one, bias_one, conv_two, bias_two):
    vmem = pl.BlockSpec(memory_space=pltpu.VMEM)
    rows_one, rows_two = CHAN * (ROW_DEV + 2), CHAN * ROW_DEV
    return pl.pallas_call(
        weights_kernel,
        out_shape=(
            jax.ShapeDtypeStruct((rows_one, 72), jnp.bfloat16),
            jax.ShapeDtypeStruct((rows_one, 1), jnp.float32),
            jax.ShapeDtypeStruct((3, rows_two, rows_one), jnp.bfloat16),
            jax.ShapeDtypeStruct((rows_two, 1), jnp.float32),
        ),
        in_specs=[pl.BlockSpec(memory_space=pl.ANY)] + [vmem] * 4,
        out_specs=(vmem,) * 4,
        compiler_params=pltpu.CompilerParams(vmem_limit_bytes=8 * 2**20),
        cost_estimate=pl.CostEstimate(flops=20_000_000, bytes_accessed=1_000_000, transcendentals=0),
        name="weights",
    )(after, conv_one, bias_one, conv_two, bias_two)


def dot_turned(left, right):
    return lax.dot_general(left, right, (((1,), (1,)), ((), ())), preferred_element_type=jnp.float32)


def lane_gather(words, index):
    dims = lax.GatherDimensionNumbers(
        offset_dims=(),
        collapsed_slice_dims=(1,),
        start_index_map=(1,),
        operand_batching_dims=(0,),
        start_indices_batching_dims=(0,),
    )
    return lax.gather(
        words, index[:, :, None], dims, (1, 1), mode=lax.GatherScatterMode.PROMISE_IN_BOUNDS
    )


def backproject_kernel(
    first_ref,
    member_ref,
    x_ref,
    trig_ref,
    ramp_ref,
    out_ref,
    filt_ref,
    word_ref,
    bin_ref,
    back_ref,
    center_ref,
    where_ref,
    acc_ref,
    where_smem,
    sem,
):
    share = x_ref.shape[1]
    views = x_ref.shape[0] * share
    first_y = first_ref[0]
    lane = lax.broadcasted_iota(jnp.int32, (views, 128), 1)
    lane_f = lane.astype(jnp.float32)

    cosine = trig_ref[0:views, :]
    sine = trig_ref[views : 2 * views, :]
    view = lax.broadcasted_iota(jnp.int32, (views, 128), 0)
    shifts = x_ref[:, :, BINS : BINS + 128].reshape(views, 128).astype(jnp.float32)
    own = lane == member_ref[0] * 2 + (view & 1)
    center = CENTER + jnp.sum(jnp.where(own, shifts, 0.0), axis=1, keepdims=True)
    center = jnp.broadcast_to(center, (views, 128))
    center_ref[...] = center
    tile_x = (lane & 15).astype(jnp.float32) * 128.0 - (WIDTH - 1) / 2.0
    set_y = first_y + 8.0 * (lane >> 4).astype(jnp.float32)
    lowest = jnp.minimum(tile_x * cosine, (tile_x + 127.0) * cosine) + set_y * sine + center
    window = ((lowest - 0.25) * (1.0 / 64.0)).astype(jnp.int32) - FIRST_WIN
    window = jnp.clip(window, 0, WINDOWS - 3)
    where_ref[...] = window * views + view
    to_smem = pltpu.make_async_copy(where_ref, where_smem, sem)
    to_smem.start()

    @pl.when(member_ref[0] >= 0)
    def filter_and_tables():
        pieces = [
            x_ref[:, :, BLOCK * block : BLOCK * block + BLOCK].reshape(views, BLOCK)
            for block in range(BLOCKS)
        ]
        for step in range(2 * BLOCKS - 1):
            delta = (step + 1) // 2 * (1 if step % 2 else -1)
            low, high = max(0, -delta), min(BLOCKS, BLOCKS - delta)
            left = jnp.concatenate(
                [pieces[block] for block in range(low, high)], axis=0
            )
            cols = slice(BLOCK * abs(delta), BLOCK * abs(delta) + BLOCK)
            if delta >= 0:
                left = jnp.concatenate([left, left], axis=1)
                part = jnp.dot(left, ramp_ref[:, cols], preferred_element_type=jnp.float32)
            else:
                part = dot_turned(left, ramp_ref[0:BLOCK, cols]) + dot_turned(left, ramp_ref[BLOCK:, cols])
            rows = slice(views * (low + delta), views * (high + delta))
            if delta == 0:
                filt_ref[rows, :] = part
            else:
                filt_ref[rows, :] += part

        margin = MARGIN // 128
        inner = BINS // 128

        def raw(place):
            half = 128 * (place % 2)
            piece = filt_ref[views * (place // 2) : views * (place // 2) + views, half : half + 128]
            return piece.astype(jnp.bfloat16).astype(jnp.float32)

        largest = jnp.abs(raw(0))
        for place in range(1, inner):
            largest = jnp.maximum(largest, jnp.abs(raw(place)))
        largest = jnp.max(largest, axis=1, keepdims=True)
        largest = jnp.max(largest.reshape(views // SCALE_SET, SCALE_SET, 1), axis=1, keepdims=True)
        largest = jnp.maximum(jnp.broadcast_to(largest, (views // SCALE_SET, SCALE_SET, 128)), 1e-30)
        largest = largest.reshape(views, 128)
        back_ref[...] = largest * (1.0 / (16383.0 * 65536.0))
        scale = 16383.0 / largest
        zero = jnp.zeros((views, 128), jnp.int32)

        def filtered(block):
            place = block - margin
            if place < 0 or place >= inner:
                return zero
            return jnp.floor(raw(place) * scale + 0.5).astype(jnp.int32)

        def turned(piece):
            return pltpu.roll(piece, 127, 1)

        def block_tables(block, piece, piece_turned, next_turned):
            step = jnp.where(lane < 127, piece_turned, next_turned) - piece
            return piece * 65536 + step, lane_f + (128.0 * block + 1.0)

        first_block = FIRST_WIN // 2
        piece = filtered(first_block)
        piece_turned = turned(piece)
        before = None
        for block in range(first_block, (FIRST_WIN + WINDOWS) // 2 + 1):
            following = filtered(block + 1)
            following_turned = turned(following)
            now = block_tables(block, piece, piece_turned, following_turned)
            for ref, value, old in zip((word_ref, bin_ref), now, before or now):
                row = (2 * block - FIRST_WIN) * views
                if before is not None:
                    ref[row - views : row, :] = jnp.where(lane >= 64, old, value)
                if 2 * block < FIRST_WIN + WINDOWS:
                    ref[row : row + views, :] = value
            before = now
            piece, piece_turned = following, following_turned

    acc_ref[...] = jnp.zeros_like(acc_ref)
    to_smem.wait()

    lane_one = lax.broadcasted_iota(jnp.int32, (8, 128), 1).astype(jnp.float32)
    sub_one = lax.broadcasted_iota(jnp.int32, (8, 128), 0).astype(jnp.float32)
    count = TILES // PARTS
    span = 128 * count
    top = lax.broadcasted_iota(jnp.int32, (8, 128), 0) < 4

    def spread(ref, row):
        return jnp.broadcast_to(ref[pl.ds(row, 1), :], (8, 128))

    def one_view(views_of, row_set, part, rows_y, totals):
        def both(ref, rows):
            if len(rows) == 1:
                return spread(ref, rows[0])
            return jnp.where(top, spread(ref, rows[0]), spread(ref, rows[1]))

        middle_x = part.astype(jnp.float32) * span + (span // 2 - WIDTH / 2.0 + 0.5)
        first_tile = row_set * TILES + part * count
        cos_v = both(trig_ref, views_of)
        base = rows_y * both(trig_ref, [views + view for view in views_of]) + both(center_ref, views_of)
        stride = cos_v * 128.0
        middle = (lane_one + middle_x) * cos_v + base
        middle_low = jnp.minimum(middle_x * cos_v, (middle_x + 127.0) * cos_v) + base
        for direction in (1, -1):
            place, place_low = middle, middle_low
            tiles = range(count // 2, count) if direction == 1 else range(count // 2 - 1, -1, -1)
            for tile in tiles:
                if direction == 1 and tile > count // 2:
                    place, place_low = place + stride, place_low + stride
                elif direction == -1:
                    place, place_low = place - stride, place_low - stride
                near = [where_smem[view, first_tile + tile] for view in views_of]
                far = [row + 2 * views for row in near]
                pick = both(bin_ref, near) > place_low
                words = jnp.where(pick, both(word_ref, near), both(word_ref, far))
                lower = place.astype(jnp.int32)
                word = lane_gather(words, lower & 127)
                value = word.astype(jnp.float32)
                along = place - lower.astype(jnp.float32)
                value = value + along * (word << 16).astype(jnp.float32)
                totals[tile] = value if totals[tile] is None else totals[tile] + value

    def add_up(block, first_view, totals):
        back = spread(back_ref, first_view)
        for tile in range(count):
            acc_ref[block, :, 128 * tile : 128 * tile + 128] += totals[tile] * back

    per_set = views // VIEW_STEP

    def steps(step, carry):
        block = step // per_set
        row_set = block // PARTS
        first_view = (step % per_set) * VIEW_STEP
        rows_y = sub_one + (first_y + 8.0 * row_set.astype(jnp.float32))
        for set_off in range(0, VIEW_STEP, SCALE_SET):
            totals = [None] * count
            for view_off in range(SCALE_SET):
                view = first_view + (set_off + view_off)
                one_view((view,), row_set, block % PARTS, rows_y, totals)
            add_up(block, first_view + set_off, totals)
        return carry

    lax.fori_loop(0, 2 * PARTS * per_set, steps, 0)

    def paired_steps(step, carry):
        part = step // per_set
        first_view = (step % per_set) * VIEW_STEP
        rows_y = jnp.where(top, sub_one, sub_one - 4.0) + (first_y + 16.0)
        for set_off in range(0, VIEW_STEP, SCALE_SET):
            totals = [None] * count
            for view_off in range(SCALE_SET // 2):
                view = first_view + (set_off + view_off)
                one_view((view, view + SCALE_SET // 2), 2, part, rows_y, totals)
            add_up(part + 2 * PARTS, first_view + set_off, totals)
        return carry

    lax.fori_loop(0, PARTS * per_set, paired_steps, 0)

    def rows_of(row_set, low, high):
        return jnp.concatenate(
            [acc_ref[row_set * PARTS + part, low:high, :] for part in range(PARTS)], axis=1
        )

    for member in range(GROUP):
        lower = rows_of(member // 2, 0, 8)
        if member == 1:
            lower = jnp.concatenate([rows_of(0, 4, 8), rows_of(1, 0, 4)], axis=0)
        elif member == 3:
            lower = jnp.concatenate([rows_of(1, 4, 8), rows_of(2, 0, 4) + rows_of(2, 4, 8)], axis=0)
        out_ref[member] = lower.astype(jnp.bfloat16)


def backproject(first_y, member, lines, trig, ramp):
    views = lines.shape[0] * lines.shape[1]
    rows = WINDOWS * views
    vmem = pl.BlockSpec(memory_space=pltpu.VMEM)
    return pl.pallas_call(
        backproject_kernel,
        out_shape=jax.ShapeDtypeStruct((GROUP, 8, WIDTH), jnp.bfloat16),
        in_specs=[pl.BlockSpec(memory_space=pltpu.SMEM)] * 2 + [vmem] * 3,
        out_specs=vmem,
        scratch_shapes=[
            pltpu.VMEM((BLOCKS * views, BLOCK), jnp.float32),
            pltpu.VMEM((rows, 128), jnp.int32),
            pltpu.VMEM((rows, 128), jnp.float32),
            pltpu.VMEM((views, 128), jnp.float32),
            pltpu.VMEM((views, 128), jnp.float32),
            pltpu.VMEM((views, 128), jnp.int32),
            pltpu.VMEM((ROW_SETS * PARTS, 8, WIDTH // PARTS), jnp.float32),
            pltpu.SMEM((views, 128), jnp.int32),
            pltpu.SemaphoreType.DMA(()),
        ],
        compiler_params=pltpu.CompilerParams(vmem_limit_bytes=16 * 2**20),
        cost_estimate=pl.CostEstimate(flops=1_000_000_000, bytes_accessed=6_000_000, transcendentals=0),
        name="backproject",
    )(first_y, member, lines, trig, ramp)


def layers_kernel(
    scale,
    image_rows,
    row_ref,
    parts_ref,
    first_ref,
    bias_one_ref,
    second_ref,
    bias_two_ref,
    out_ref,
    image_ref,
    stack_ref,
):
    row_base = row_ref[0]
    image = parts_ref[0].astype(jnp.float32)
    for member in range(1, GROUP):
        image = image + parts_ref[member].astype(jnp.float32)
    image = (image * scale).astype(jnp.bfloat16).astype(jnp.float32)
    row = lax.broadcasted_iota(jnp.int32, image.shape, 0) + (row_base - 2)
    image = jnp.where((row >= 0) & (row < image_rows), image, 0.0)
    column = lax.broadcasted_iota(jnp.int32, image.shape, 1)
    left = jnp.where(column == 0, 0.0, pltpu.roll(image, 1, 1))
    right = jnp.where(column == WIDTH - 1, 0.0, pltpu.roll(image, WIDTH - 1, 1))
    three = jnp.concatenate([left, image, right], axis=0).astype(jnp.bfloat16)
    image_ref[...] = jnp.concatenate([three, three, three], axis=0)

    weights = first_ref[...]
    count = CHAN * (ROW_DEV + 2)
    for tile in range(0, WIDTH, 256):
        hidden = jnp.dot(weights, image_ref[:, tile : tile + 256], preferred_element_type=jnp.float32)
        hidden = jnp.maximum(hidden + bias_one_ref[...], 0.0)
        top = jnp.where(row_base > 0, hidden[0:CHAN], 0.0)
        bottom = jnp.where(row_base + ROW_DEV < image_rows, hidden[count - CHAN : count], 0.0)
        hidden = jnp.concatenate([top, hidden[CHAN : count - CHAN], bottom], axis=0)
        stack_ref[:, tile : tile + 256] = hidden

    middle_rows = stack_ref[...]
    column = lax.broadcasted_iota(jnp.int32, middle_rows.shape, 1)
    before = jnp.where(column == 0, 0.0, pltpu.roll(middle_rows, 1, 1)).astype(jnp.bfloat16)
    after = jnp.where(column == WIDTH - 1, 0.0, pltpu.roll(middle_rows, WIDTH - 1, 1)).astype(jnp.bfloat16)
    mixed = jnp.dot(second_ref[0], before, preferred_element_type=jnp.float32)
    mixed = mixed + jnp.dot(second_ref[1], middle_rows.astype(jnp.bfloat16), preferred_element_type=jnp.float32)
    mixed = mixed + jnp.dot(second_ref[2], after, preferred_element_type=jnp.float32)
    mixed = jnp.maximum(mixed + bias_two_ref[...], 0.0)
    out_ref[...] = mixed.reshape(CHAN, ROW_DEV, WIDTH).astype(jnp.bfloat16)[None]


def layers(row_base, parts, first, bias_one, second, bias_two, scale, image_rows):
    vmem = pl.BlockSpec(memory_space=pltpu.VMEM)

    def body(*refs):
        layers_kernel(scale, image_rows, *refs)

    return pl.pallas_call(
        body,
        out_shape=jax.ShapeDtypeStruct((1, CHAN, ROW_DEV, WIDTH), jnp.bfloat16),
        in_specs=[pl.BlockSpec(memory_space=pltpu.SMEM)] + [vmem] * 5,
        out_specs=vmem,
        scratch_shapes=[
            pltpu.VMEM((72, WIDTH), jnp.bfloat16),
            pltpu.VMEM((CHAN * (ROW_DEV + 2), WIDTH), jnp.float32),
        ],
        compiler_params=pltpu.CompilerParams(vmem_limit_bytes=16 * 2**20),
        cost_estimate=pl.CostEstimate(flops=500_000_000, bytes_accessed=1_000_000, transcendentals=0),
        name="layers",
    )(row_base, parts, first, bias_one, second, bias_two)


def local(sinogram, view_shift, conv_one, bias_one, conv_two, bias_two):
    sheets, view_count, detector = sinogram.shape
    row_groups = lax.axis_size("rows")
    view_groups = lax.axis_size("views")
    views_total = view_count * view_groups
    image_rows = ROW_DEV * row_groups
    share = view_count // GROUP
    row_index = lax.axis_index("rows")
    member = row_index % GROUP

    mine = lax.dynamic_slice_in_dim(sinogram, member * share, share, 1)
    shift = jnp.pad(view_shift.astype(jnp.bfloat16), (0, 128 - view_count))
    sent = jnp.concatenate([mine, jnp.broadcast_to(shift, (sheets, share, 128))], axis=2)
    lines = lax.all_to_all(sent, "views", 0, 0, tiled=True)

    member_one = member.astype(jnp.int32).reshape(1)
    ramp, trig = prepare(member_one, view_groups * share, views_total, share, view_count)
    first_row = (row_index - member) * ROW_DEV - 2
    first_y = first_row.astype(jnp.float32) - (image_rows - 1) / 2.0

    partial_rows = backproject(first_y.reshape(1), member_one, lines, trig, ramp)
    groups = [[GROUP * base + item for item in range(GROUP)] for base in range(row_groups // GROUP)]
    parts = lax.all_to_all(partial_rows, "rows", 0, 0, tiled=True, axis_index_groups=groups)

    first, wide_one, second, wide_two = spread_weights(
        partial_rows, conv_one, bias_one[None], conv_two, bias_two[None]
    )
    row_base = (row_index * ROW_DEV).astype(jnp.int32).reshape(1)
    return layers(
        row_base,
        parts,
        first,
        wide_one,
        second,
        wide_two,
        math.pi / views_total,
        image_rows,
    )


def solution(mesh):
    return jax.shard_map(
        local,
        mesh=mesh,
        in_specs=(P(None, "views", None), P("views"), P(), P(), P(), P()),
        out_specs=P("views", None, "rows", None),
        check_vma=False,
    )
```

```python
import math

import jax
import jax.numpy as jnp
from jax import lax
from jax.experimental import pallas as pl
from jax.experimental.pallas import tpu as pltpu
from jax.sharding import PartitionSpec as P

BINS = 2048
WIDTH = 2048
MARGIN = 384
CHAN = 32
ROW_DEV = 4
GROUP = 4
BLOCK = 256
BLOCKS = BINS // BLOCK
FIRST_WIN = 4
WINDOWS = 36
HALF_TURN = 64
PAIRS = 32
SLOTS = 40
CENTER = (BINS - 1) / 2.0 + MARGIN - HALF_TURN
TILES = WIDTH // 128
ROW_SETS = 3
RAMP_COLS = BLOCKS * BLOCK
SCALE_SET = 8
PARTS = 2


def selection(shape, test):
    row = lax.broadcasted_iota(jnp.int32, shape, 0)
    col = lax.broadcasted_iota(jnp.int32, shape, 1)
    return jnp.where(test(row, col), 1.0, 0.0)


def exact_dot(left, right, contract=(1, 0)):
    return lax.dot_general(
        left,
        right,
        (((contract[0],), (contract[1],)), ((), ())),
        precision=lax.Precision.HIGHEST,
        preferred_element_type=jnp.float32,
    )


def column_of(picker, row):
    return jnp.sum(picker * row, axis=1, keepdims=True)


def source_of(row, member):
    slot = row & (PAIRS - 1)
    mirror = row >> 5
    turned = jnp.where(mirror == 1, PAIRS - 1 - slot, slot)
    zero_even = jnp.where(mirror == 1, PAIRS + 15 - slot, slot - 15)
    zero_last = jnp.where(mirror == 1, PAIRS // 2, 0)
    zero_group = jnp.where(slot == PAIRS - 1, zero_last, zero_even)
    zero_group = jnp.where(slot < PAIRS // 2, turned, zero_group)
    zero_which = jnp.where(slot < PAIRS // 2, 1, 0)
    group = jnp.where(member == 0, zero_group, turned)
    which = jnp.where(member == 0, zero_which, mirror)
    return group, which


def residue_of(which, member, view_count):
    return jnp.where(
        which == 0, member, jnp.where(member == 0, view_count // 2, view_count - member)
    )


def prepare_kernel(
    views_total,
    view_count,
    member_ref,
    table_ref,
    trig_ref,
):
    width = BLOCKS * BLOCK

    for turn in range(8):
        row = lax.broadcasted_iota(jnp.int32, (16, width + 128), 0)
        col = lax.broadcasted_iota(jnp.int32, (16, width + 128), 1)
        offset = col - row - (128 + 16 * turn)
        place = offset.astype(jnp.float32)
        guarded = jnp.maximum(place * place, 1.0)
        odd = (offset & 1) == 1
        values = jnp.where(odd, (-1.0 / (math.pi * math.pi)) / guarded, 0.0)
        values = jnp.where(offset == 0, 0.25, values)
        high = values.astype(jnp.bfloat16)
        low = (values - high.astype(jnp.float32)).astype(jnp.bfloat16)
        for half in range(2):
            start = 16 * turn + 128 * half
            cols = slice(128 - 128 * half, 128 - 128 * half + width)
            table_ref[start : start + 16, :] = high[:, cols]
            table_ref[BLOCK + start : BLOCK + start + 16, :] = low[:, cols]

    slot = lax.broadcasted_iota(jnp.int32, (SLOTS, 128), 0)
    member = jnp.full((SLOTS, 128), member_ref[0], jnp.int32)
    group, which = source_of(slot & (PAIRS - 1), member)
    view = group * view_count + residue_of(which, member, view_count)
    view = jnp.where(slot < PAIRS, view, views_total // 2)
    angle = view.astype(jnp.float32) * (math.pi / views_total)
    trig_ref[0:SLOTS, :] = jnp.cos(angle)
    trig_ref[SLOTS : 2 * SLOTS, :] = jnp.sin(angle)


def weights_kernel(
    after_ref,
    conv_one_ref,
    bias_one_ref,
    conv_two_ref,
    bias_two_ref,
    first_ref,
    wide_one_ref,
    second_ref,
    wide_two_ref,
):
    del after_ref
    rows_one = CHAN * (ROW_DEV + 2)
    picker = selection((rows_one, CHAN), lambda row, col: (row & (CHAN - 1)) == col)
    wide_one_ref[...] = column_of(picker, bias_one_ref[...])
    taps = exact_dot(picker, conv_one_ref[...], (1, 1))
    weights = jnp.zeros((rows_one, 24), jnp.float32)
    for item in range(3):
        moved = exact_dot(taps, selection((9, 24), lambda row, col: row == 3 * item + (col >> 3)))
        keep = selection((rows_one, 24), lambda row, col: (col & 7) == (row >> 5) + item)
        weights = weights + moved * keep
    high = weights.astype(jnp.bfloat16)
    rest = weights - high.astype(jnp.float32)
    middle = rest.astype(jnp.bfloat16)
    low = (rest - middle.astype(jnp.float32)).astype(jnp.bfloat16)
    first_ref[...] = jnp.concatenate([high, middle, low], axis=1)

    rows_two = CHAN * ROW_DEV
    picker = selection((rows_two, CHAN), lambda row, col: (row >> 2) == col)
    wide_two_ref[...] = column_of(picker, bias_two_ref[...])
    spread = jnp.dot(
        picker.astype(jnp.bfloat16), conv_two_ref[...], preferred_element_type=jnp.float32
    ).astype(jnp.bfloat16)
    cols_two = CHAN * (ROW_DEV + 2)
    for tap in range(3):
        block = jnp.zeros((rows_two, cols_two), jnp.float32)
        for item in range(3):
            source = spread[:, (3 * item + tap) * CHAN : (3 * item + tap + 1) * CHAN]
            place = selection((CHAN, cols_two), lambda row, col: (col & (CHAN - 1)) == row)
            moved = jnp.dot(source, place.astype(jnp.bfloat16), preferred_element_type=jnp.float32)
            keep = selection((rows_two, cols_two), lambda row, col: (col >> 5) == (row & 3) + item)
            block = block + moved * keep
        second_ref[tap] = block.astype(jnp.bfloat16)


def prepare(member, views_total, view_count):
    vmem = pl.BlockSpec(memory_space=pltpu.VMEM)

    def body(*refs):
        prepare_kernel(views_total, view_count, *refs)

    return pl.pallas_call(
        body,
        out_shape=(
            jax.ShapeDtypeStruct((2 * BLOCK, BLOCKS * BLOCK), jnp.bfloat16),
            jax.ShapeDtypeStruct((2 * SLOTS, 128), jnp.float32),
        ),
        in_specs=[pl.BlockSpec(memory_space=pltpu.SMEM)],
        out_specs=(vmem,) * 2,
        compiler_params=pltpu.CompilerParams(vmem_limit_bytes=8 * 2**20),
        cost_estimate=pl.CostEstimate(flops=20_000_000, bytes_accessed=4_000_000, transcendentals=0),
        name="prepare",
    )(member)


def spread_weights(after, conv_one, bias_one, conv_two, bias_two):
    vmem = pl.BlockSpec(memory_space=pltpu.VMEM)
    rows_one, rows_two = CHAN * (ROW_DEV + 2), CHAN * ROW_DEV
    return pl.pallas_call(
        weights_kernel,
        out_shape=(
            jax.ShapeDtypeStruct((rows_one, 72), jnp.bfloat16),
            jax.ShapeDtypeStruct((rows_one, 1), jnp.float32),
            jax.ShapeDtypeStruct((3, rows_two, rows_one), jnp.bfloat16),
            jax.ShapeDtypeStruct((rows_two, 1), jnp.float32),
        ),
        in_specs=[pl.BlockSpec(memory_space=pl.ANY)] + [vmem] * 4,
        out_specs=(vmem,) * 4,
        compiler_params=pltpu.CompilerParams(vmem_limit_bytes=8 * 2**20),
        cost_estimate=pl.CostEstimate(flops=20_000_000, bytes_accessed=1_000_000, transcendentals=0),
        name="weights",
    )(after, conv_one, bias_one, conv_two, bias_two)


def dot_turned(left, right):
    return lax.dot_general(left, right, (((1,), (1,)), ((), ())), preferred_element_type=jnp.float32)


def lane_gather(words, index):
    dims = lax.GatherDimensionNumbers(
        offset_dims=(),
        collapsed_slice_dims=(1,),
        start_index_map=(1,),
        operand_batching_dims=(0,),
        start_indices_batching_dims=(0,),
    )
    return lax.gather(
        words, index[:, :, None], dims, (1, 1), mode=lax.GatherScatterMode.PROMISE_IN_BOUNDS
    )


def backproject_kernel(
    first_ref,
    member_ref,
    x_ref,
    trig_ref,
    ramp_ref,
    out_ref,
    filt_ref,
    word_ref,
    bin_ref,
    back_ref,
    where_ref,
    acc_ref,
    where_smem,
    sem,
):
    share = x_ref.shape[1]
    views = x_ref.shape[0] * share
    first_y = first_ref[0]
    member = member_ref[0]
    lane = lax.broadcasted_iota(jnp.int32, (views, 128), 1)

    slot_lane = lax.broadcasted_iota(jnp.int32, (SLOTS, 128), 1)
    slot_row = lax.broadcasted_iota(jnp.int32, (SLOTS, 128), 0)
    cosine = trig_ref[0:SLOTS, :]
    sine = trig_ref[SLOTS : 2 * SLOTS, :]
    tile_x = (slot_lane & 15).astype(jnp.float32) * 128.0 - (WIDTH - 1) / 2.0
    set_y = first_y + 8.0 * (slot_lane >> 4).astype(jnp.float32)
    lowest = jnp.minimum(tile_x * cosine, (tile_x + 127.0) * cosine) + set_y * sine + CENTER
    window = ((lowest - 0.25) * (1.0 / 64.0)).astype(jnp.int32) - FIRST_WIN
    where_ref[...] = jnp.clip(window, 0, WINDOWS - 3) * views
    first_bin = (slot_row + FIRST_WIN) * 64 + slot_lane
    halves = jnp.where(slot_lane >= 64, -64, 64)
    bin_ref[...] = (first_bin + 1 + jnp.where((slot_row & 1) == 1, halves, 0)).astype(jnp.float32)
    to_smem = pltpu.make_async_copy(where_ref, where_smem, sem)
    to_smem.start()

    @pl.when(member_ref[0] >= 0)
    def filter_and_tables():
        row = lax.broadcasted_iota(jnp.int32, (views, views), 0)
        col = lax.broadcasted_iota(jnp.int32, (views, views), 1)
        group, which = source_of(row, jnp.full((views, views), member, jnp.int32))
        order = jnp.where(col == group * share + which, 1.0, 0.0).astype(jnp.bfloat16)

        def in_order(low, high):
            part = x_ref[:, :, low:high].reshape(views, high - low)
            return jnp.dot(order, part, preferred_element_type=jnp.float32)

        pieces = [
            in_order(BLOCK * block, BLOCK * block + BLOCK).astype(jnp.bfloat16)
            for block in range(BLOCKS)
        ]
        row = lax.broadcasted_iota(jnp.int32, (views, 128), 0)
        everyone = jnp.full((views, 128), member, jnp.int32)
        group, which = source_of(row, everyone)
        own = lane == residue_of(which, everyone, 8)
        turn = jnp.sum(jnp.where(own, in_order(BINS, BINS + 128), 0.0), axis=1, keepdims=True)
        turn = jnp.broadcast_to(turn, (views, 128)).astype(jnp.int32) + HALF_TURN
        turn_index = (lane + turn) & 127
        turn_near = lane >= turn

        for step in range(2 * BLOCKS - 1):
            delta = (step + 1) // 2 * (1 if step % 2 else -1)
            low, high = max(0, -delta), min(BLOCKS, BLOCKS - delta)
            left = jnp.concatenate(
                [pieces[block] for block in range(low, high)], axis=0
            )
            cols = slice(BLOCK * abs(delta), BLOCK * abs(delta) + BLOCK)
            if delta >= 0:
                left = jnp.concatenate([left, left], axis=1)
                part = jnp.dot(left, ramp_ref[:, cols], preferred_element_type=jnp.float32)
            else:
                part = dot_turned(left, ramp_ref[0:BLOCK, cols]) + dot_turned(left, ramp_ref[BLOCK:, cols])
            rows = slice(views * (low + delta), views * (high + delta))
            if delta == 0:
                filt_ref[rows, :] = part
            else:
                filt_ref[rows, :] += part

        margin = MARGIN // 128
        inner = BINS // 128

        def raw(place):
            half = 128 * (place % 2)
            piece = filt_ref[views * (place // 2) : views * (place // 2) + views, half : half + 128]
            return piece.astype(jnp.bfloat16).astype(jnp.float32)

        largest = jnp.abs(raw(0))
        for place in range(1, inner):
            largest = jnp.maximum(largest, jnp.abs(raw(place)))
        largest = jnp.max(largest, axis=1, keepdims=True)
        largest = jnp.max(largest.reshape(views // SCALE_SET, SCALE_SET, 1), axis=1, keepdims=True)
        largest = jnp.maximum(jnp.broadcast_to(largest, (views // SCALE_SET, SCALE_SET, 128)), 1e-30)
        largest = largest.reshape(views, 128)
        back_ref[...] = largest * (1.0 / (16383.0 * 65536.0))
        scale = 16383.0 / largest
        zero = jnp.zeros((views, 128), jnp.int32)

        def filtered(block):
            place = block - margin
            if place < 0 or place >= inner:
                return zero
            return jnp.floor(raw(place) * scale + 0.5).astype(jnp.int32)

        def turned(piece):
            return pltpu.roll(piece, 127, 1)

        def shifted(block):
            return lane_gather(jnp.where(turn_near, filtered_at(block), filtered_at(block + 1)), turn_index)

        known = {}

        def filtered_at(block):
            if block not in known:
                known[block] = filtered(block)
            return known[block]

        first_block = FIRST_WIN // 2
        piece = shifted(first_block)
        piece_turned = turned(piece)
        before = None
        for block in range(first_block, (FIRST_WIN + WINDOWS) // 2 + 1):
            following = shifted(block + 1)
            following_turned = turned(following)
            step = jnp.where(lane < 127, piece_turned, following_turned) - piece
            word = piece * 65536 + step
            row = (2 * block - FIRST_WIN) * views
            if before is not None:
                word_ref[row - views : row, :] = jnp.where(lane >= 64, before, word)
            if 2 * block < FIRST_WIN + WINDOWS:
                word_ref[row : row + views, :] = word
            before = word
            piece, piece_turned = following, following_turned

    acc_ref[...] = jnp.zeros_like(acc_ref)
    to_smem.wait()

    lane_one = lax.broadcasted_iota(jnp.int32, (8, 128), 1).astype(jnp.float32)
    sub_one = lax.broadcasted_iota(jnp.int32, (8, 128), 0).astype(jnp.float32)
    count = TILES // PARTS
    span = 128 * count
    top = lax.broadcasted_iota(jnp.int32, (8, 128), 0) < 4

    def spread(ref, row):
        return jnp.broadcast_to(ref[pl.ds(row, 1), :], (8, 128))

    member_vec = jnp.full((8, 128), member, jnp.int32)
    is_zero = member_vec == 0
    not_zero = member_vec > 0

    def one_slot(slots, row_set, part, rows_y, straight, mirrored):
        def both(ref, rows):
            if len(rows) == 1:
                return spread(ref, rows[0])
            return jnp.where(top, spread(ref, rows[0]), spread(ref, rows[1]))

        alone = slots[0] == PAIRS
        middle_x = part.astype(jnp.float32) * span + (span // 2 - WIDTH / 2.0 + 0.5)
        first_tile = row_set * TILES + part * count
        cos_v = both(trig_ref, slots)
        base = rows_y * both(trig_ref, [SLOTS + slot for slot in slots]) + CENTER
        stride = cos_v * 128.0
        middle = (lane_one + middle_x) * cos_v + base
        middle_low = jnp.minimum(middle_x * cos_v, (middle_x + 127.0) * cos_v) + base

        def value_of(words, index, along):
            word = lane_gather(words, index)
            return word.astype(jnp.float32) + along * (word << 16).astype(jnp.float32)

        for direction in (1, -1):
            place, place_low = middle, middle_low
            tiles = range(count // 2, count) if direction == 1 else range(count // 2 - 1, -1, -1)
            for tile in tiles:
                if direction == 1 and tile > count // 2:
                    place, place_low = place + stride, place_low + stride
                elif direction == -1:
                    place, place_low = place - stride, place_low - stride
                starts = [where_smem[slot, first_tile + tile] for slot in slots]
                pick = both(bin_ref, [start >> 6 for start in starts]) > place_low
                lower = place.astype(jnp.int32)
                index = lower & 127
                along = place - lower.astype(jnp.float32)

                def words_of(lines):
                    near = [start + line for start, line in zip(starts, lines)]
                    far = [start + (line + 2 * views) for start, line in zip(starts, lines)]
                    return jnp.where(pick, both(word_ref, near), both(word_ref, far))

                if alone:
                    words = words_of([views - 1 for slot in slots])
                    words = jnp.where(is_zero if len(slots) == 1 else top & is_zero, words, 0)
                else:
                    words = words_of(slots)
                    other = words_of([PAIRS + slot for slot in slots])
                    if slots[-1] == PAIRS - 1:
                        other = jnp.where(not_zero if len(slots) == 1 else top | not_zero, other, 0)
                    value = value_of(other, index, along)
                    mirrored[tile] = value if mirrored[tile] is None else mirrored[tile] + value
                value = value_of(words, index, along)
                straight[tile] = value if straight[tile] is None else straight[tile] + value

    def add_up(side, block, line, totals):
        back = spread(back_ref, line)
        for tile in range(count):
            acc_ref[side, block, :, 128 * tile : 128 * tile + 128] += totals[tile] * back

    def all_slots(row_set, part, block, rows_y, slot_sets):
        for first, group in slot_sets:
            straight, mirrored = [None] * count, [None] * count
            for slots in group:
                one_slot(slots, row_set, part, rows_y, straight, mirrored)
            if first == PAIRS:
                add_up(0, block, views - SCALE_SET, straight)
            else:
                add_up(0, block, first, straight)
                add_up(1, block, PAIRS + first, mirrored)

    singles = [
        (first, [(first + item,) for item in range(SCALE_SET)])
        for first in range(0, PAIRS, SCALE_SET)
    ]
    doubles = [
        (first, [(first + item, first + item + 4) for item in range(SCALE_SET // 2)])
        for first in range(0, PAIRS, SCALE_SET)
    ]

    def steps(block, carry):
        row_set = block // PARTS
        rows_y = sub_one + (first_y + 8.0 * row_set.astype(jnp.float32))
        all_slots(row_set, block % PARTS, block, rows_y, singles + [(PAIRS, [(PAIRS,)])])
        return carry

    lax.fori_loop(0, 2 * PARTS, steps, 0)

    def paired_steps(part, carry):
        rows_y = jnp.where(top, sub_one, sub_one - 4.0) + (first_y + 16.0)
        all_slots(2, part, 2 * PARTS + part, rows_y, doubles + [(PAIRS, [(PAIRS, PAIRS)])])
        return carry

    lax.fori_loop(0, PARTS, paired_steps, 0)

    back_index = 127 - lax.broadcasted_iota(jnp.int32, (8, 128), 1)
    for row_set in range(ROW_SETS):
        for tile in range(TILES):
            block, spot = row_set * PARTS + tile // count, tile % count
            turn_tile = TILES - 1 - tile
            other = acc_ref[
                1,
                row_set * PARTS + turn_tile // count,
                :,
                128 * (turn_tile % count) : 128 * (turn_tile % count) + 128,
            ]
            acc_ref[0, block, :, 128 * spot : 128 * spot + 128] += lane_gather(other, back_index)

    def rows_of(row_set, low, high):
        return jnp.concatenate(
            [acc_ref[0, row_set * PARTS + part, low:high, :] for part in range(PARTS)], axis=1
        )

    for member in range(GROUP):
        lower = rows_of(member // 2, 0, 8)
        if member == 1:
            lower = jnp.concatenate([rows_of(0, 4, 8), rows_of(1, 0, 4)], axis=0)
        elif member == 3:
            lower = jnp.concatenate([rows_of(1, 4, 8), rows_of(2, 0, 4) + rows_of(2, 4, 8)], axis=0)
        out_ref[member] = lower.astype(jnp.bfloat16)


def backproject(first_y, member, lines, trig, ramp):
    views = lines.shape[0] * lines.shape[1]
    rows = WINDOWS * views
    vmem = pl.BlockSpec(memory_space=pltpu.VMEM)
    return pl.pallas_call(
        backproject_kernel,
        out_shape=jax.ShapeDtypeStruct((GROUP, 8, WIDTH), jnp.bfloat16),
        in_specs=[pl.BlockSpec(memory_space=pltpu.SMEM)] * 2 + [vmem] * 3,
        out_specs=vmem,
        scratch_shapes=[
            pltpu.VMEM((BLOCKS * views, BLOCK), jnp.float32),
            pltpu.VMEM((rows, 128), jnp.int32),
            pltpu.VMEM((SLOTS, 128), jnp.float32),
            pltpu.VMEM((views, 128), jnp.float32),
            pltpu.VMEM((SLOTS, 128), jnp.int32),
            pltpu.VMEM((2, ROW_SETS * PARTS, 8, WIDTH // PARTS), jnp.float32),
            pltpu.SMEM((SLOTS, 128), jnp.int32),
            pltpu.SemaphoreType.DMA(()),
        ],
        compiler_params=pltpu.CompilerParams(vmem_limit_bytes=16 * 2**20),
        cost_estimate=pl.CostEstimate(flops=1_000_000_000, bytes_accessed=6_000_000, transcendentals=0),
        name="backproject",
    )(first_y, member, lines, trig, ramp)


def layers_kernel(
    scale,
    image_rows,
    row_ref,
    parts_ref,
    first_ref,
    bias_one_ref,
    second_ref,
    bias_two_ref,
    out_ref,
    image_ref,
    stack_ref,
):
    row_base = row_ref[0]
    image = parts_ref[0].astype(jnp.float32)
    for member in range(1, GROUP):
        image = image + parts_ref[member].astype(jnp.float32)
    image = (image * scale).astype(jnp.bfloat16).astype(jnp.float32)
    row = lax.broadcasted_iota(jnp.int32, image.shape, 0) + (row_base - 2)
    image = jnp.where((row >= 0) & (row < image_rows), image, 0.0)
    column = lax.broadcasted_iota(jnp.int32, image.shape, 1)
    left = jnp.where(column == 0, 0.0, pltpu.roll(image, 1, 1))
    right = jnp.where(column == WIDTH - 1, 0.0, pltpu.roll(image, WIDTH - 1, 1))
    three = jnp.concatenate([left, image, right], axis=0).astype(jnp.bfloat16)
    image_ref[...] = jnp.concatenate([three, three, three], axis=0)

    weights = first_ref[...]
    count = CHAN * (ROW_DEV + 2)
    for tile in range(0, WIDTH, 256):
        hidden = jnp.dot(weights, image_ref[:, tile : tile + 256], preferred_element_type=jnp.float32)
        hidden = jnp.maximum(hidden + bias_one_ref[...], 0.0)
        top = jnp.where(row_base > 0, hidden[0:CHAN], 0.0)
        bottom = jnp.where(row_base + ROW_DEV < image_rows, hidden[count - CHAN : count], 0.0)
        hidden = jnp.concatenate([top, hidden[CHAN : count - CHAN], bottom], axis=0)
        stack_ref[:, tile : tile + 256] = hidden

    middle_rows = stack_ref[...]
    column = lax.broadcasted_iota(jnp.int32, middle_rows.shape, 1)
    before = jnp.where(column == 0, 0.0, pltpu.roll(middle_rows, 1, 1)).astype(jnp.bfloat16)
    after = jnp.where(column == WIDTH - 1, 0.0, pltpu.roll(middle_rows, WIDTH - 1, 1)).astype(jnp.bfloat16)
    mixed = jnp.dot(second_ref[0], before, preferred_element_type=jnp.float32)
    mixed = mixed + jnp.dot(second_ref[1], middle_rows.astype(jnp.bfloat16), preferred_element_type=jnp.float32)
    mixed = mixed + jnp.dot(second_ref[2], after, preferred_element_type=jnp.float32)
    mixed = jnp.maximum(mixed + bias_two_ref[...], 0.0)
    out_ref[...] = mixed.reshape(CHAN, ROW_DEV, WIDTH).astype(jnp.bfloat16)[None]


def layers(row_base, parts, first, bias_one, second, bias_two, scale, image_rows):
    vmem = pl.BlockSpec(memory_space=pltpu.VMEM)

    def body(*refs):
        layers_kernel(scale, image_rows, *refs)

    return pl.pallas_call(
        body,
        out_shape=jax.ShapeDtypeStruct((1, CHAN, ROW_DEV, WIDTH), jnp.bfloat16),
        in_specs=[pl.BlockSpec(memory_space=pltpu.SMEM)] + [vmem] * 5,
        out_specs=vmem,
        scratch_shapes=[
            pltpu.VMEM((72, WIDTH), jnp.bfloat16),
            pltpu.VMEM((CHAN * (ROW_DEV + 2), WIDTH), jnp.float32),
        ],
        compiler_params=pltpu.CompilerParams(vmem_limit_bytes=16 * 2**20),
        cost_estimate=pl.CostEstimate(flops=500_000_000, bytes_accessed=1_000_000, transcendentals=0),
        name="layers",
    )(row_base, parts, first, bias_one, second, bias_two)


def local(sinogram, view_shift, conv_one, bias_one, conv_two, bias_two):
    sheets, view_count, detector = sinogram.shape
    row_groups = lax.axis_size("rows")
    view_groups = lax.axis_size("views")
    views_total = view_count * view_groups
    image_rows = ROW_DEV * row_groups
    share = view_count // GROUP
    row_index = lax.axis_index("rows")
    member = row_index % GROUP

    second_row = jnp.where(member == 0, view_count // 2, view_count - member)
    mine = jnp.concatenate(
        [
            lax.dynamic_slice_in_dim(sinogram, member, 1, 1),
            lax.dynamic_slice_in_dim(sinogram, second_row, 1, 1),
        ],
        axis=1,
    )
    shift = jnp.pad(view_shift.astype(jnp.bfloat16), (0, 128 - view_count))
    sent = jnp.concatenate([mine, jnp.broadcast_to(shift, (sheets, share, 128))], axis=2)
    lines = lax.all_to_all(sent, "views", 0, 0, tiled=True)

    member_one = member.astype(jnp.int32).reshape(1)
    ramp, trig = prepare(member_one, views_total, view_count)
    first_row = (row_index - member) * ROW_DEV - 2
    first_y = first_row.astype(jnp.float32) - (image_rows - 1) / 2.0

    partial_rows = backproject(first_y.reshape(1), member_one, lines, trig, ramp)
    groups = [[GROUP * base + item for item in range(GROUP)] for base in range(row_groups // GROUP)]
    parts = lax.all_to_all(partial_rows, "rows", 0, 0, tiled=True, axis_index_groups=groups)

    first, wide_one, second, wide_two = spread_weights(
        partial_rows, conv_one, bias_one[None], conv_two, bias_two[None]
    )
    row_base = (row_index * ROW_DEV).astype(jnp.int32).reshape(1)
    return layers(
        row_base,
        parts,
        first,
        wide_one,
        second,
        wide_two,
        math.pi / views_total,
        image_rows,
    )


def solution(mesh):
    return jax.shard_map(
        local,
        mesh=mesh,
        in_specs=(P(None, "views", None), P("views"), P(), P(), P(), P()),
        out_specs=P("views", None, "rows", None),
        check_vma=False,
    )
```

```python
import math

import jax
import jax.numpy as jnp
from jax import lax
from jax.experimental import pallas as pl
from jax.experimental.pallas import tpu as pltpu
from jax.sharding import PartitionSpec as P

BINS = 2048
WIDTH = 2048
MARGIN = 384
CHAN = 32
ROW_DEV = 4
GROUP = 4
BLOCK = 256
BLOCKS = BINS // BLOCK
FIRST_WIN = 4
WINDOWS = 36
HALF_TURN = 64
PAIRS = 32
PACK_STEPS = 2
PACK_LIMIT = 66_500_000
SLOTS = 40
CENTER = (BINS - 1) / 2.0 + MARGIN - HALF_TURN
TILES = WIDTH // 128
ROW_SETS = 3
RAMP_COLS = BLOCKS * BLOCK
SCALE_SET = 8
PARTS = 2


def selection(shape, test):
    row = lax.broadcasted_iota(jnp.int32, shape, 0)
    col = lax.broadcasted_iota(jnp.int32, shape, 1)
    return jnp.where(test(row, col), 1.0, 0.0)


def exact_dot(left, right, contract=(1, 0)):
    return lax.dot_general(
        left,
        right,
        (((contract[0],), (contract[1],)), ((), ())),
        precision=lax.Precision.HIGHEST,
        preferred_element_type=jnp.float32,
    )


def column_of(picker, row):
    return jnp.sum(picker * row, axis=1, keepdims=True)


def source_of(row, member):
    slot = row & (PAIRS - 1)
    mirror = row >> 5
    turned = jnp.where(mirror == 1, PAIRS - 1 - slot, slot)
    zero_even = jnp.where(mirror == 1, PAIRS + 15 - slot, slot - 15)
    zero_last = jnp.where(mirror == 1, PAIRS // 2, 0)
    zero_group = jnp.where(slot == PAIRS - 1, zero_last, zero_even)
    zero_group = jnp.where(slot < PAIRS // 2, turned, zero_group)
    zero_which = jnp.where(slot < PAIRS // 2, 1, 0)
    group = jnp.where(member == 0, zero_group, turned)
    which = jnp.where(member == 0, zero_which, mirror)
    return group, which


def residue_of(which, member, view_count):
    return jnp.where(
        which == 0, member, jnp.where(member == 0, view_count // 2, view_count - member)
    )


def pack_kernel(member_ref, shift_ref, x_ref, out_ref):
    sheets, views, width = x_ref.shape
    share = out_ref.shape[1]
    row = lax.broadcasted_iota(jnp.int32, (sheets * share, sheets * views), 0)
    col = lax.broadcasted_iota(jnp.int32, (sheets * share, sheets * views), 1)
    member = jnp.full(row.shape, member_ref[0], jnp.int32)
    wanted = (row >> 1) * views + residue_of(row & 1, member, views)
    order = jnp.where(col == wanted, 1.0, 0.0).astype(jnp.bfloat16)
    lines = x_ref[...].reshape(sheets * views, width)
    picked = jnp.dot(order, lines, preferred_element_type=jnp.float32).astype(jnp.bfloat16)
    start = pl.multiple_of(pl.program_id(0) * width, width)
    out_ref[:, :, pl.ds(start, width)] = picked.reshape(sheets, share, width)

    @pl.when(pl.program_id(0) == 0)
    def shifts_of_views():
        lane = lax.broadcasted_iota(jnp.int32, (1, share, 128), 2)
        shifts = jnp.zeros((1, share, 128), jnp.float32)
        for view in range(views):
            shifts = jnp.where(lane == view, shift_ref[view].astype(jnp.float32), shifts)
        shifts = jnp.broadcast_to(shifts.astype(jnp.bfloat16), (sheets, share, 128))
        out_ref[:, :, BINS : BINS + 128] = shifts


def pack(member, view_shift, sinogram, share):
    sheets, views, bins = sinogram.shape
    smem = pl.BlockSpec(memory_space=pltpu.SMEM)
    width = bins // PACK_STEPS
    return pl.pallas_call(
        pack_kernel,
        grid=(PACK_STEPS,),
        out_shape=jax.ShapeDtypeStruct((sheets, share, bins + 128), jnp.bfloat16),
        in_specs=[smem, smem, pl.BlockSpec((sheets, views, width), lambda step: (0, 0, step))],
        out_specs=pl.BlockSpec((sheets, share, bins + 128), lambda step: (0, 0, 0)),
        compiler_params=pltpu.CompilerParams(vmem_limit_bytes=PACK_LIMIT),
        cost_estimate=pl.CostEstimate(flops=70_000_000, bytes_accessed=1_500_000, transcendentals=0),
        name="pack",
    )(member, view_shift, sinogram)


def prepare_kernel(
    views_total,
    view_count,
    member_ref,
    table_ref,
    trig_ref,
):
    width = BLOCKS * BLOCK

    for turn in range(8):
        row = lax.broadcasted_iota(jnp.int32, (16, width + 128), 0)
        col = lax.broadcasted_iota(jnp.int32, (16, width + 128), 1)
        offset = col - row - (128 + 16 * turn)
        place = offset.astype(jnp.float32)
        guarded = jnp.maximum(place * place, 1.0)
        odd = (offset & 1) == 1
        values = jnp.where(odd, (-1.0 / (math.pi * math.pi)) / guarded, 0.0)
        values = jnp.where(offset == 0, 0.25, values)
        high = values.astype(jnp.bfloat16)
        low = (values - high.astype(jnp.float32)).astype(jnp.bfloat16)
        for half in range(2):
            start = 16 * turn + 128 * half
            cols = slice(128 - 128 * half, 128 - 128 * half + width)
            table_ref[start : start + 16, :] = high[:, cols]
            table_ref[BLOCK + start : BLOCK + start + 16, :] = low[:, cols]

    slot = lax.broadcasted_iota(jnp.int32, (SLOTS, 128), 0)
    member = jnp.full((SLOTS, 128), member_ref[0], jnp.int32)
    group, which = source_of(slot & (PAIRS - 1), member)
    view = group * view_count + residue_of(which, member, view_count)
    view = jnp.where(slot < PAIRS, view, views_total // 2)
    angle = view.astype(jnp.float32) * (math.pi / views_total)
    trig_ref[0:SLOTS, :] = jnp.cos(angle)
    trig_ref[SLOTS : 2 * SLOTS, :] = jnp.sin(angle)


def weights_kernel(
    after_ref,
    conv_one_ref,
    bias_one_ref,
    conv_two_ref,
    bias_two_ref,
    first_ref,
    wide_one_ref,
    second_ref,
    wide_two_ref,
):
    del after_ref
    rows_one = CHAN * (ROW_DEV + 2)
    picker = selection((rows_one, CHAN), lambda row, col: (row & (CHAN - 1)) == col)
    wide_one_ref[...] = column_of(picker, bias_one_ref[...])
    taps = exact_dot(picker, conv_one_ref[...], (1, 1))
    weights = jnp.zeros((rows_one, 24), jnp.float32)
    for item in range(3):
        moved = exact_dot(taps, selection((9, 24), lambda row, col: row == 3 * item + (col >> 3)))
        keep = selection((rows_one, 24), lambda row, col: (col & 7) == (row >> 5) + item)
        weights = weights + moved * keep
    high = weights.astype(jnp.bfloat16)
    rest = weights - high.astype(jnp.float32)
    middle = rest.astype(jnp.bfloat16)
    low = (rest - middle.astype(jnp.float32)).astype(jnp.bfloat16)
    first_ref[...] = jnp.concatenate([high, middle, low], axis=1)

    rows_two = CHAN * ROW_DEV
    picker = selection((rows_two, CHAN), lambda row, col: (row >> 2) == col)
    wide_two_ref[...] = column_of(picker, bias_two_ref[...])
    spread = jnp.dot(
        picker.astype(jnp.bfloat16), conv_two_ref[...], preferred_element_type=jnp.float32
    ).astype(jnp.bfloat16)
    cols_two = CHAN * (ROW_DEV + 2)
    for tap in range(3):
        block = jnp.zeros((rows_two, cols_two), jnp.float32)
        for item in range(3):
            source = spread[:, (3 * item + tap) * CHAN : (3 * item + tap + 1) * CHAN]
            place = selection((CHAN, cols_two), lambda row, col: (col & (CHAN - 1)) == row)
            moved = jnp.dot(source, place.astype(jnp.bfloat16), preferred_element_type=jnp.float32)
            keep = selection((rows_two, cols_two), lambda row, col: (col >> 5) == (row & 3) + item)
            block = block + moved * keep
        second_ref[tap] = block.astype(jnp.bfloat16)


def prepare(member, views_total, view_count):
    vmem = pl.BlockSpec(memory_space=pltpu.VMEM)

    def body(*refs):
        prepare_kernel(views_total, view_count, *refs)

    return pl.pallas_call(
        body,
        out_shape=(
            jax.ShapeDtypeStruct((2 * BLOCK, BLOCKS * BLOCK), jnp.bfloat16),
            jax.ShapeDtypeStruct((2 * SLOTS, 128), jnp.float32),
        ),
        in_specs=[pl.BlockSpec(memory_space=pltpu.SMEM)],
        out_specs=(vmem,) * 2,
        compiler_params=pltpu.CompilerParams(vmem_limit_bytes=8 * 2**20),
        cost_estimate=pl.CostEstimate(flops=20_000_000, bytes_accessed=4_000_000, transcendentals=0),
        name="prepare",
    )(member)


def spread_weights(after, conv_one, bias_one, conv_two, bias_two):
    vmem = pl.BlockSpec(memory_space=pltpu.VMEM)
    rows_one, rows_two = CHAN * (ROW_DEV + 2), CHAN * ROW_DEV
    return pl.pallas_call(
        weights_kernel,
        out_shape=(
            jax.ShapeDtypeStruct((rows_one, 72), jnp.bfloat16),
            jax.ShapeDtypeStruct((rows_one, 1), jnp.float32),
            jax.ShapeDtypeStruct((3, rows_two, rows_one), jnp.bfloat16),
            jax.ShapeDtypeStruct((rows_two, 1), jnp.float32),
        ),
        in_specs=[pl.BlockSpec(memory_space=pl.ANY)] + [vmem] * 4,
        out_specs=(vmem,) * 4,
        compiler_params=pltpu.CompilerParams(vmem_limit_bytes=8 * 2**20),
        cost_estimate=pl.CostEstimate(flops=20_000_000, bytes_accessed=1_000_000, transcendentals=0),
        name="weights",
    )(after, conv_one, bias_one, conv_two, bias_two)


def dot_turned(left, right):
    return lax.dot_general(left, right, (((1,), (1,)), ((), ())), preferred_element_type=jnp.float32)


def lane_gather(words, index):
    dims = lax.GatherDimensionNumbers(
        offset_dims=(),
        collapsed_slice_dims=(1,),
        start_index_map=(1,),
        operand_batching_dims=(0,),
        start_indices_batching_dims=(0,),
    )
    return lax.gather(
        words, index[:, :, None], dims, (1, 1), mode=lax.GatherScatterMode.PROMISE_IN_BOUNDS
    )


def backproject_kernel(
    first_ref,
    member_ref,
    x_ref,
    trig_ref,
    ramp_ref,
    out_ref,
    filt_ref,
    word_ref,
    bin_ref,
    back_ref,
    where_ref,
    acc_ref,
    where_smem,
    sem,
):
    share = x_ref.shape[1]
    views = x_ref.shape[0] * share
    first_y = first_ref[0]
    member = member_ref[0]
    lane = lax.broadcasted_iota(jnp.int32, (views, 128), 1)

    slot_lane = lax.broadcasted_iota(jnp.int32, (SLOTS, 128), 1)
    slot_row = lax.broadcasted_iota(jnp.int32, (SLOTS, 128), 0)
    cosine = trig_ref[0:SLOTS, :]
    sine = trig_ref[SLOTS : 2 * SLOTS, :]
    tile_x = (slot_lane & 15).astype(jnp.float32) * 128.0 - (WIDTH - 1) / 2.0
    set_y = first_y + 8.0 * (slot_lane >> 4).astype(jnp.float32)
    lowest = jnp.minimum(tile_x * cosine, (tile_x + 127.0) * cosine) + set_y * sine + CENTER
    window = ((lowest - 0.25) * (1.0 / 64.0)).astype(jnp.int32) - FIRST_WIN
    where_ref[...] = jnp.clip(window, 0, WINDOWS - 3) * views
    first_bin = (slot_row + FIRST_WIN) * 64 + slot_lane
    halves = jnp.where(slot_lane >= 64, -64, 64)
    bin_ref[...] = (first_bin + 1 + jnp.where((slot_row & 1) == 1, halves, 0)).astype(jnp.float32)
    to_smem = pltpu.make_async_copy(where_ref, where_smem, sem)
    to_smem.start()

    @pl.when(member_ref[0] >= 0)
    def filter_and_tables():
        row = lax.broadcasted_iota(jnp.int32, (views, views), 0)
        col = lax.broadcasted_iota(jnp.int32, (views, views), 1)
        group, which = source_of(row, jnp.full((views, views), member, jnp.int32))
        order = jnp.where(col == group * share + which, 1.0, 0.0).astype(jnp.bfloat16)

        def in_order(low, high):
            part = x_ref[:, :, low:high].reshape(views, high - low)
            return jnp.dot(order, part, preferred_element_type=jnp.float32)

        pieces = [
            in_order(BLOCK * block, BLOCK * block + BLOCK).astype(jnp.bfloat16)
            for block in range(BLOCKS)
        ]
        row = lax.broadcasted_iota(jnp.int32, (views, 128), 0)
        everyone = jnp.full((views, 128), member, jnp.int32)
        group, which = source_of(row, everyone)
        own = lane == residue_of(which, everyone, 8)
        turn = jnp.sum(jnp.where(own, in_order(BINS, BINS + 128), 0.0), axis=1, keepdims=True)
        turn = jnp.broadcast_to(turn, (views, 128)).astype(jnp.int32) + HALF_TURN
        turn_index = (lane + turn) & 127
        turn_near = lane >= turn

        for step in range(2 * BLOCKS - 1):
            delta = (step + 1) // 2 * (1 if step % 2 else -1)
            low, high = max(0, -delta), min(BLOCKS, BLOCKS - delta)
            left = jnp.concatenate(
                [pieces[block] for block in range(low, high)], axis=0
            )
            cols = slice(BLOCK * abs(delta), BLOCK * abs(delta) + BLOCK)
            if delta >= 0:
                left = jnp.concatenate([left, left], axis=1)
                part = jnp.dot(left, ramp_ref[:, cols], preferred_element_type=jnp.float32)
            else:
                part = dot_turned(left, ramp_ref[0:BLOCK, cols]) + dot_turned(left, ramp_ref[BLOCK:, cols])
            rows = slice(views * (low + delta), views * (high + delta))
            if delta == 0:
                filt_ref[rows, :] = part
            else:
                filt_ref[rows, :] += part

        margin = MARGIN // 128
        inner = BINS // 128

        def raw(place):
            half = 128 * (place % 2)
            piece = filt_ref[views * (place // 2) : views * (place // 2) + views, half : half + 128]
            return piece.astype(jnp.bfloat16).astype(jnp.float32)

        largest = jnp.abs(raw(0))
        for place in range(1, inner):
            largest = jnp.maximum(largest, jnp.abs(raw(place)))
        largest = jnp.max(largest, axis=1, keepdims=True)
        largest = jnp.max(largest.reshape(views // SCALE_SET, SCALE_SET, 1), axis=1, keepdims=True)
        largest = jnp.maximum(jnp.broadcast_to(largest, (views // SCALE_SET, SCALE_SET, 128)), 1e-30)
        largest = largest.reshape(views, 128)
        back_ref[...] = largest * (1.0 / (16383.0 * 65536.0))
        scale = 16383.0 / largest
        zero = jnp.zeros((views, 128), jnp.int32)

        def filtered(block):
            place = block - margin
            if place < 0 or place >= inner:
                return zero
            return jnp.floor(raw(place) * scale + 0.5).astype(jnp.int32)

        def turned(piece):
            return pltpu.roll(piece, 127, 1)

        def shifted(block):
            return lane_gather(jnp.where(turn_near, filtered_at(block), filtered_at(block + 1)), turn_index)

        known = {}

        def filtered_at(block):
            if block not in known:
                known[block] = filtered(block)
            return known[block]

        first_block = FIRST_WIN // 2
        piece = shifted(first_block)
        piece_turned = turned(piece)
        before = None
        for block in range(first_block, (FIRST_WIN + WINDOWS) // 2 + 1):
            following = shifted(block + 1)
            following_turned = turned(following)
            step = jnp.where(lane < 127, piece_turned, following_turned) - piece
            word = piece * 65536 + step
            row = (2 * block - FIRST_WIN) * views
            if before is not None:
                word_ref[row - views : row, :] = jnp.where(lane >= 64, before, word)
            if 2 * block < FIRST_WIN + WINDOWS:
                word_ref[row : row + views, :] = word
            before = word
            piece, piece_turned = following, following_turned

    acc_ref[...] = jnp.zeros_like(acc_ref)
    to_smem.wait()

    lane_one = lax.broadcasted_iota(jnp.int32, (8, 128), 1).astype(jnp.float32)
    sub_one = lax.broadcasted_iota(jnp.int32, (8, 128), 0).astype(jnp.float32)
    count = TILES // PARTS
    span = 128 * count
    top = lax.broadcasted_iota(jnp.int32, (8, 128), 0) < 4

    def spread(ref, row):
        return jnp.broadcast_to(ref[pl.ds(row, 1), :], (8, 128))

    member_vec = jnp.full((8, 128), member, jnp.int32)
    is_zero = member_vec == 0
    not_zero = member_vec > 0

    def one_slot(slots, row_set, part, rows_y, straight, mirrored):
        def both(ref, rows):
            if len(rows) == 1:
                return spread(ref, rows[0])
            return jnp.where(top, spread(ref, rows[0]), spread(ref, rows[1]))

        alone = slots[0] == PAIRS
        middle_x = part.astype(jnp.float32) * span + (span // 2 - WIDTH / 2.0 + 0.5)
        first_tile = row_set * TILES + part * count
        cos_v = both(trig_ref, slots)
        base = rows_y * both(trig_ref, [SLOTS + slot for slot in slots]) + CENTER
        stride = cos_v * 128.0
        middle = (lane_one + middle_x) * cos_v + base
        middle_low = jnp.minimum(middle_x * cos_v, (middle_x + 127.0) * cos_v) + base

        def value_of(words, index, along):
            word = lane_gather(words, index)
            return word.astype(jnp.float32) + along * (word << 16).astype(jnp.float32)

        for direction in (1, -1):
            place, place_low = middle, middle_low
            tiles = range(count // 2, count) if direction == 1 else range(count // 2 - 1, -1, -1)
            for tile in tiles:
                if direction == 1 and tile > count // 2:
                    place, place_low = place + stride, place_low + stride
                elif direction == -1:
                    place, place_low = place - stride, place_low - stride
                starts = [where_smem[slot, first_tile + tile] for slot in slots]
                pick = both(bin_ref, [start >> 6 for start in starts]) > place_low
                lower = place.astype(jnp.int32)
                index = lower & 127
                along = place - lower.astype(jnp.float32)

                def words_of(lines):
                    near = [start + line for start, line in zip(starts, lines)]
                    far = [start + (line + 2 * views) for start, line in zip(starts, lines)]
                    return jnp.where(pick, both(word_ref, near), both(word_ref, far))

                if alone:
                    words = words_of([views - 1 for slot in slots])
                    words = jnp.where(is_zero if len(slots) == 1 else top & is_zero, words, 0)
                else:
                    words = words_of(slots)
                    other = words_of([PAIRS + slot for slot in slots])
                    if slots[-1] == PAIRS - 1:
                        other = jnp.where(not_zero if len(slots) == 1 else top | not_zero, other, 0)
                    value = value_of(other, index, along)
                    mirrored[tile] = value if mirrored[tile] is None else mirrored[tile] + value
                value = value_of(words, index, along)
                straight[tile] = value if straight[tile] is None else straight[tile] + value

    def add_up(side, block, line, totals):
        back = spread(back_ref, line)
        for tile in range(count):
            acc_ref[side, block, :, 128 * tile : 128 * tile + 128] += totals[tile] * back

    def all_slots(row_set, part, block, rows_y, slot_sets):
        for first, group in slot_sets:
            straight, mirrored = [None] * count, [None] * count
            for slots in group:
                one_slot(slots, row_set, part, rows_y, straight, mirrored)
            if first == PAIRS:
                add_up(0, block, views - SCALE_SET, straight)
            else:
                add_up(0, block, first, straight)
                add_up(1, block, PAIRS + first, mirrored)

    singles = [
        (first, [(first + item,) for item in range(SCALE_SET)])
        for first in range(0, PAIRS, SCALE_SET)
    ]
    doubles = [
        (first, [(first + item, first + item + 4) for item in range(SCALE_SET // 2)])
        for first in range(0, PAIRS, SCALE_SET)
    ]

    def steps(block, carry):
        row_set = block // PARTS
        rows_y = sub_one + (first_y + 8.0 * row_set.astype(jnp.float32))
        all_slots(row_set, block % PARTS, block, rows_y, singles + [(PAIRS, [(PAIRS,)])])
        return carry

    lax.fori_loop(0, 2 * PARTS, steps, 0)

    def paired_steps(part, carry):
        rows_y = jnp.where(top, sub_one, sub_one - 4.0) + (first_y + 16.0)
        all_slots(2, part, 2 * PARTS + part, rows_y, doubles + [(PAIRS, [(PAIRS, PAIRS)])])
        return carry

    lax.fori_loop(0, PARTS, paired_steps, 0)

    back_index = 127 - lax.broadcasted_iota(jnp.int32, (8, 128), 1)
    for row_set in range(ROW_SETS):
        for tile in range(TILES):
            block, spot = row_set * PARTS + tile // count, tile % count
            turn_tile = TILES - 1 - tile
            other = acc_ref[
                1,
                row_set * PARTS + turn_tile // count,
                :,
                128 * (turn_tile % count) : 128 * (turn_tile % count) + 128,
            ]
            acc_ref[0, block, :, 128 * spot : 128 * spot + 128] += lane_gather(other, back_index)

    def rows_of(row_set, low, high):
        return jnp.concatenate(
            [acc_ref[0, row_set * PARTS + part, low:high, :] for part in range(PARTS)], axis=1
        )

    for member in range(GROUP):
        lower = rows_of(member // 2, 0, 8)
        if member == 1:
            lower = jnp.concatenate([rows_of(0, 4, 8), rows_of(1, 0, 4)], axis=0)
        elif member == 3:
            lower = jnp.concatenate([rows_of(1, 4, 8), rows_of(2, 0, 4) + rows_of(2, 4, 8)], axis=0)
        out_ref[member] = lower.astype(jnp.bfloat16)


def backproject(first_y, member, lines, trig, ramp):
    views = lines.shape[0] * lines.shape[1]
    rows = WINDOWS * views
    vmem = pl.BlockSpec(memory_space=pltpu.VMEM)
    return pl.pallas_call(
        backproject_kernel,
        out_shape=jax.ShapeDtypeStruct((GROUP, 8, WIDTH), jnp.bfloat16),
        in_specs=[pl.BlockSpec(memory_space=pltpu.SMEM)] * 2 + [vmem] * 3,
        out_specs=vmem,
        scratch_shapes=[
            pltpu.VMEM((BLOCKS * views, BLOCK), jnp.float32),
            pltpu.VMEM((rows, 128), jnp.int32),
            pltpu.VMEM((SLOTS, 128), jnp.float32),
            pltpu.VMEM((views, 128), jnp.float32),
            pltpu.VMEM((SLOTS, 128), jnp.int32),
            pltpu.VMEM((2, ROW_SETS * PARTS, 8, WIDTH // PARTS), jnp.float32),
            pltpu.SMEM((SLOTS, 128), jnp.int32),
            pltpu.SemaphoreType.DMA(()),
        ],
        compiler_params=pltpu.CompilerParams(vmem_limit_bytes=16 * 2**20),
        cost_estimate=pl.CostEstimate(flops=1_000_000_000, bytes_accessed=6_000_000, transcendentals=0),
        name="backproject",
    )(first_y, member, lines, trig, ramp)


def layers_kernel(
    scale,
    image_rows,
    row_ref,
    parts_ref,
    first_ref,
    bias_one_ref,
    second_ref,
    bias_two_ref,
    out_ref,
    image_ref,
    stack_ref,
):
    row_base = row_ref[0]
    image = parts_ref[0].astype(jnp.float32)
    for member in range(1, GROUP):
        image = image + parts_ref[member].astype(jnp.float32)
    image = (image * scale).astype(jnp.bfloat16).astype(jnp.float32)
    row = lax.broadcasted_iota(jnp.int32, image.shape, 0) + (row_base - 2)
    image = jnp.where((row >= 0) & (row < image_rows), image, 0.0)
    column = lax.broadcasted_iota(jnp.int32, image.shape, 1)
    left = jnp.where(column == 0, 0.0, pltpu.roll(image, 1, 1))
    right = jnp.where(column == WIDTH - 1, 0.0, pltpu.roll(image, WIDTH - 1, 1))
    three = jnp.concatenate([left, image, right], axis=0).astype(jnp.bfloat16)
    image_ref[...] = jnp.concatenate([three, three, three], axis=0)

    weights = first_ref[...]
    count = CHAN * (ROW_DEV + 2)
    for tile in range(0, WIDTH, 256):
        hidden = jnp.dot(weights, image_ref[:, tile : tile + 256], preferred_element_type=jnp.float32)
        hidden = jnp.maximum(hidden + bias_one_ref[...], 0.0)
        top = jnp.where(row_base > 0, hidden[0:CHAN], 0.0)
        bottom = jnp.where(row_base + ROW_DEV < image_rows, hidden[count - CHAN : count], 0.0)
        hidden = jnp.concatenate([top, hidden[CHAN : count - CHAN], bottom], axis=0)
        stack_ref[:, tile : tile + 256] = hidden

    middle_rows = stack_ref[...]
    column = lax.broadcasted_iota(jnp.int32, middle_rows.shape, 1)
    before = jnp.where(column == 0, 0.0, pltpu.roll(middle_rows, 1, 1)).astype(jnp.bfloat16)
    after = jnp.where(column == WIDTH - 1, 0.0, pltpu.roll(middle_rows, WIDTH - 1, 1)).astype(jnp.bfloat16)
    mixed = jnp.dot(second_ref[0], before, preferred_element_type=jnp.float32)
    mixed = mixed + jnp.dot(second_ref[1], middle_rows.astype(jnp.bfloat16), preferred_element_type=jnp.float32)
    mixed = mixed + jnp.dot(second_ref[2], after, preferred_element_type=jnp.float32)
    mixed = jnp.maximum(mixed + bias_two_ref[...], 0.0)
    out_ref[...] = mixed.reshape(CHAN, ROW_DEV, WIDTH).astype(jnp.bfloat16)[None]


def layers(row_base, parts, first, bias_one, second, bias_two, scale, image_rows):
    vmem = pl.BlockSpec(memory_space=pltpu.VMEM)

    def body(*refs):
        layers_kernel(scale, image_rows, *refs)

    return pl.pallas_call(
        body,
        out_shape=jax.ShapeDtypeStruct((1, CHAN, ROW_DEV, WIDTH), jnp.bfloat16),
        in_specs=[pl.BlockSpec(memory_space=pltpu.SMEM)] + [vmem] * 5,
        out_specs=vmem,
        scratch_shapes=[
            pltpu.VMEM((72, WIDTH), jnp.bfloat16),
            pltpu.VMEM((CHAN * (ROW_DEV + 2), WIDTH), jnp.float32),
        ],
        compiler_params=pltpu.CompilerParams(vmem_limit_bytes=16 * 2**20),
        cost_estimate=pl.CostEstimate(flops=500_000_000, bytes_accessed=1_000_000, transcendentals=0),
        name="layers",
    )(row_base, parts, first, bias_one, second, bias_two)


def local(sinogram, view_shift, conv_one, bias_one, conv_two, bias_two):
    sheets, view_count, detector = sinogram.shape
    row_groups = lax.axis_size("rows")
    view_groups = lax.axis_size("views")
    views_total = view_count * view_groups
    image_rows = ROW_DEV * row_groups
    share = view_count // GROUP
    row_index = lax.axis_index("rows")
    member = row_index % GROUP

    member_one = member.astype(jnp.int32).reshape(1)
    sent = pack(member_one, view_shift, sinogram, share)
    lines = lax.all_to_all(sent, "views", 0, 0, tiled=True)

    ramp, trig = prepare(member_one, views_total, view_count)
    first_row = (row_index - member) * ROW_DEV - 2
    first_y = first_row.astype(jnp.float32) - (image_rows - 1) / 2.0

    partial_rows = backproject(first_y.reshape(1), member_one, lines, trig, ramp)
    groups = [[GROUP * base + item for item in range(GROUP)] for base in range(row_groups // GROUP)]
    parts = lax.all_to_all(partial_rows, "rows", 0, 0, tiled=True, axis_index_groups=groups)

    first, wide_one, second, wide_two = spread_weights(
        partial_rows, conv_one, bias_one[None], conv_two, bias_two[None]
    )
    row_base = (row_index * ROW_DEV).astype(jnp.int32).reshape(1)
    return layers(
        row_base,
        parts,
        first,
        wide_one,
        second,
        wide_two,
        math.pi / views_total,
        image_rows,
    )


def solution(mesh):
    return jax.shard_map(
        local,
        mesh=mesh,
        in_specs=(P(None, "views", None), P("views"), P(), P(), P(), P()),
        out_specs=P("views", None, "rows", None),
        check_vma=False,
    )
```

```python
import math

import jax
import jax.numpy as jnp
from jax import lax
from jax.experimental import pallas as pl
from jax.experimental.pallas import tpu as pltpu
from jax.sharding import PartitionSpec as P

BINS = 2048
WIDTH = 2048
MARGIN = 384
CHAN = 32
ROW_DEV = 4
GROUP = 4
BLOCK = 256
BLOCKS = BINS // BLOCK
FIRST_WIN = 4
WINDOWS = 36
HALF_TURN = 64
PAIRS = 32
PACK_STEPS = 2
PACK_LIMIT = 66_500_000
SLOTS = 40
CENTER = (BINS - 1) / 2.0 + MARGIN - HALF_TURN
TILES = WIDTH // 128
ROW_SETS = 3
RAMP_COLS = BLOCKS * BLOCK
SCALE_SET = 8
PARTS = 2


def selection(shape, test):
    row = lax.broadcasted_iota(jnp.int32, shape, 0)
    col = lax.broadcasted_iota(jnp.int32, shape, 1)
    return jnp.where(test(row, col), 1.0, 0.0)


def exact_dot(left, right, contract=(1, 0)):
    return lax.dot_general(
        left,
        right,
        (((contract[0],), (contract[1],)), ((), ())),
        precision=lax.Precision.HIGHEST,
        preferred_element_type=jnp.float32,
    )


def column_of(picker, row):
    return jnp.sum(picker * row, axis=1, keepdims=True)


def source_of(row, member):
    slot = row & (PAIRS - 1)
    mirror = row >> 5
    turned = jnp.where(mirror == 1, PAIRS - 1 - slot, slot)
    zero_even = jnp.where(mirror == 1, PAIRS + 15 - slot, slot - 15)
    zero_last = jnp.where(mirror == 1, PAIRS // 2, 0)
    zero_group = jnp.where(slot == PAIRS - 1, zero_last, zero_even)
    zero_group = jnp.where(slot < PAIRS // 2, turned, zero_group)
    zero_which = jnp.where(slot < PAIRS // 2, 1, 0)
    group = jnp.where(member == 0, zero_group, turned)
    which = jnp.where(member == 0, zero_which, mirror)
    return group, which


def residue_of(which, member, view_count):
    return jnp.where(
        which == 0, member, jnp.where(member == 0, view_count // 2, view_count - member)
    )


def own_member():
    return lax.rem(lax.axis_index("rows"), GROUP)


def pack_kernel(shift_ref, x_ref, out_ref):
    sheets, views, width = x_ref.shape
    share = out_ref.shape[1]
    row = lax.broadcasted_iota(jnp.int32, (sheets * share, sheets * views), 0)
    col = lax.broadcasted_iota(jnp.int32, (sheets * share, sheets * views), 1)
    member = jnp.full(row.shape, own_member(), jnp.int32)
    wanted = (row >> 1) * views + residue_of(row & 1, member, views)
    order = jnp.where(col == wanted, 1.0, 0.0).astype(jnp.bfloat16)
    lines = x_ref[...].reshape(sheets * views, width)
    picked = jnp.dot(order, lines, preferred_element_type=jnp.float32).astype(jnp.bfloat16)
    start = pl.multiple_of(pl.program_id(0) * width, width)
    out_ref[:, :, pl.ds(start, width)] = picked.reshape(sheets, share, width)

    @pl.when(pl.program_id(0) == 0)
    def shifts_of_views():
        lane = lax.broadcasted_iota(jnp.int32, (1, share, 128), 2)
        shifts = jnp.zeros((1, share, 128), jnp.float32)
        for view in range(views):
            shifts = jnp.where(lane == view, shift_ref[view].astype(jnp.float32), shifts)
        shifts = jnp.broadcast_to(shifts.astype(jnp.bfloat16), (sheets, share, 128))
        out_ref[:, :, BINS : BINS + 128] = shifts


def pack(view_shift, sinogram, share):
    sheets, views, bins = sinogram.shape
    smem = pl.BlockSpec(memory_space=pltpu.SMEM)
    width = bins // PACK_STEPS
    return pl.pallas_call(
        pack_kernel,
        grid=(PACK_STEPS,),
        out_shape=jax.ShapeDtypeStruct((sheets, share, bins + 128), jnp.bfloat16),
        in_specs=[smem, pl.BlockSpec((sheets, views, width), lambda step: (0, 0, step))],
        out_specs=pl.BlockSpec((sheets, share, bins + 128), lambda step: (0, 0, 0)),
        compiler_params=pltpu.CompilerParams(vmem_limit_bytes=PACK_LIMIT),
        cost_estimate=pl.CostEstimate(flops=70_000_000, bytes_accessed=1_500_000, transcendentals=0),
        name="pack",
    )(view_shift, sinogram)


def prepare_kernel(
    views_total,
    view_count,
    table_ref,
    trig_ref,
):
    width = BLOCKS * BLOCK

    for turn in range(8):
        row = lax.broadcasted_iota(jnp.int32, (16, width + 128), 0)
        col = lax.broadcasted_iota(jnp.int32, (16, width + 128), 1)
        offset = col - row - (128 + 16 * turn)
        place = offset.astype(jnp.float32)
        guarded = jnp.maximum(place * place, 1.0)
        odd = (offset & 1) == 1
        values = jnp.where(odd, (-1.0 / (math.pi * math.pi)) / guarded, 0.0)
        values = jnp.where(offset == 0, 0.25, values)
        high = values.astype(jnp.bfloat16)
        low = (values - high.astype(jnp.float32)).astype(jnp.bfloat16)
        for half in range(2):
            start = 16 * turn + 128 * half
            cols = slice(128 - 128 * half, 128 - 128 * half + width)
            table_ref[start : start + 16, :] = high[:, cols]
            table_ref[BLOCK + start : BLOCK + start + 16, :] = low[:, cols]

    slot = lax.broadcasted_iota(jnp.int32, (SLOTS, 128), 0)
    member = jnp.full((SLOTS, 128), own_member(), jnp.int32)
    group, which = source_of(slot & (PAIRS - 1), member)
    view = group * view_count + residue_of(which, member, view_count)
    view = jnp.where(slot < PAIRS, view, views_total // 2)
    angle = view.astype(jnp.float32) * (math.pi / views_total)
    trig_ref[0:SLOTS, :] = jnp.cos(angle)
    trig_ref[SLOTS : 2 * SLOTS, :] = jnp.sin(angle)


def weights_kernel(
    after_ref,
    conv_one_ref,
    bias_one_ref,
    conv_two_ref,
    bias_two_ref,
    first_ref,
    wide_one_ref,
    second_ref,
    wide_two_ref,
):
    del after_ref
    rows_one = CHAN * (ROW_DEV + 2)
    picker = selection((rows_one, CHAN), lambda row, col: (row & (CHAN - 1)) == col)
    wide_one_ref[...] = column_of(picker, bias_one_ref[...])
    taps = exact_dot(picker, conv_one_ref[...], (1, 1))
    weights = jnp.zeros((rows_one, 24), jnp.float32)
    for item in range(3):
        moved = exact_dot(taps, selection((9, 24), lambda row, col: row == 3 * item + (col >> 3)))
        keep = selection((rows_one, 24), lambda row, col: (col & 7) == (row >> 5) + item)
        weights = weights + moved * keep
    high = weights.astype(jnp.bfloat16)
    rest = weights - high.astype(jnp.float32)
    middle = rest.astype(jnp.bfloat16)
    low = (rest - middle.astype(jnp.float32)).astype(jnp.bfloat16)
    first_ref[...] = jnp.concatenate([high, middle, low], axis=1)

    rows_two = CHAN * ROW_DEV
    picker = selection((rows_two, CHAN), lambda row, col: (row >> 2) == col)
    wide_two_ref[...] = column_of(picker, bias_two_ref[...])
    spread = jnp.dot(
        picker.astype(jnp.bfloat16), conv_two_ref[...], preferred_element_type=jnp.float32
    ).astype(jnp.bfloat16)
    cols_two = CHAN * (ROW_DEV + 2)
    for tap in range(3):
        block = jnp.zeros((rows_two, cols_two), jnp.float32)
        for item in range(3):
            source = spread[:, (3 * item + tap) * CHAN : (3 * item + tap + 1) * CHAN]
            place = selection((CHAN, cols_two), lambda row, col: (col & (CHAN - 1)) == row)
            moved = jnp.dot(source, place.astype(jnp.bfloat16), preferred_element_type=jnp.float32)
            keep = selection((rows_two, cols_two), lambda row, col: (col >> 5) == (row & 3) + item)
            block = block + moved * keep
        second_ref[tap] = block.astype(jnp.bfloat16)


def prepare(views_total, view_count):
    vmem = pl.BlockSpec(memory_space=pltpu.VMEM)

    def body(*refs):
        prepare_kernel(views_total, view_count, *refs)

    return pl.pallas_call(
        body,
        out_shape=(
            jax.ShapeDtypeStruct((2 * BLOCK, BLOCKS * BLOCK), jnp.bfloat16),
            jax.ShapeDtypeStruct((2 * SLOTS, 128), jnp.float32),
        ),
        out_specs=(vmem,) * 2,
        compiler_params=pltpu.CompilerParams(vmem_limit_bytes=8 * 2**20),
        cost_estimate=pl.CostEstimate(flops=20_000_000, bytes_accessed=4_000_000, transcendentals=0),
        name="prepare",
    )()


def spread_weights(after, conv_one, bias_one, conv_two, bias_two):
    vmem = pl.BlockSpec(memory_space=pltpu.VMEM)
    rows_one, rows_two = CHAN * (ROW_DEV + 2), CHAN * ROW_DEV
    return pl.pallas_call(
        weights_kernel,
        out_shape=(
            jax.ShapeDtypeStruct((rows_one, 72), jnp.bfloat16),
            jax.ShapeDtypeStruct((rows_one, 1), jnp.float32),
            jax.ShapeDtypeStruct((3, rows_two, rows_one), jnp.bfloat16),
            jax.ShapeDtypeStruct((rows_two, 1), jnp.float32),
        ),
        in_specs=[pl.BlockSpec(memory_space=pl.ANY)] + [vmem] * 4,
        out_specs=(vmem,) * 4,
        compiler_params=pltpu.CompilerParams(vmem_limit_bytes=8 * 2**20),
        cost_estimate=pl.CostEstimate(flops=20_000_000, bytes_accessed=1_000_000, transcendentals=0),
        name="weights",
    )(after, conv_one, bias_one, conv_two, bias_two)


def dot_turned(left, right):
    return lax.dot_general(left, right, (((1,), (1,)), ((), ())), preferred_element_type=jnp.float32)


def lane_gather(words, index):
    dims = lax.GatherDimensionNumbers(
        offset_dims=(),
        collapsed_slice_dims=(1,),
        start_index_map=(1,),
        operand_batching_dims=(0,),
        start_indices_batching_dims=(0,),
    )
    return lax.gather(
        words, index[:, :, None], dims, (1, 1), mode=lax.GatherScatterMode.PROMISE_IN_BOUNDS
    )


def backproject_kernel(
    image_rows,
    x_ref,
    trig_ref,
    ramp_ref,
    out_ref,
    filt_ref,
    word_ref,
    bin_ref,
    back_ref,
    where_ref,
    acc_ref,
    where_smem,
    sem,
):
    share = x_ref.shape[1]
    views = x_ref.shape[0] * share
    member = own_member()
    first_row = (lax.axis_index("rows") - member) * ROW_DEV - 2
    first_y = first_row.astype(jnp.float32) - (image_rows - 1) / 2.0
    lane = lax.broadcasted_iota(jnp.int32, (views, 128), 1)

    slot_lane = lax.broadcasted_iota(jnp.int32, (SLOTS, 128), 1)
    slot_row = lax.broadcasted_iota(jnp.int32, (SLOTS, 128), 0)
    cosine = trig_ref[0:SLOTS, :]
    sine = trig_ref[SLOTS : 2 * SLOTS, :]
    tile_x = (slot_lane & 15).astype(jnp.float32) * 128.0 - (WIDTH - 1) / 2.0
    set_y = first_y + 8.0 * (slot_lane >> 4).astype(jnp.float32)
    lowest = jnp.minimum(tile_x * cosine, (tile_x + 127.0) * cosine) + set_y * sine + CENTER
    window = ((lowest - 0.25) * (1.0 / 64.0)).astype(jnp.int32) - FIRST_WIN
    where_ref[...] = jnp.clip(window, 0, WINDOWS - 3) * views
    first_bin = (slot_row + FIRST_WIN) * 64 + slot_lane
    halves = jnp.where(slot_lane >= 64, -64, 64)
    bin_ref[...] = (first_bin + 1 + jnp.where((slot_row & 1) == 1, halves, 0)).astype(jnp.float32)
    to_smem = pltpu.make_async_copy(where_ref, where_smem, sem)
    to_smem.start()

    @pl.when(member >= 0)
    def filter_and_tables():
        row = lax.broadcasted_iota(jnp.int32, (views, views), 0)
        col = lax.broadcasted_iota(jnp.int32, (views, views), 1)
        group, which = source_of(row, jnp.full((views, views), member, jnp.int32))
        order = jnp.where(col == group * share + which, 1.0, 0.0).astype(jnp.bfloat16)

        def in_order(low, high):
            part = x_ref[:, :, low:high].reshape(views, high - low)
            return jnp.dot(order, part, preferred_element_type=jnp.float32)

        pieces = [
            in_order(BLOCK * block, BLOCK * block + BLOCK).astype(jnp.bfloat16)
            for block in range(BLOCKS)
        ]
        row = lax.broadcasted_iota(jnp.int32, (views, 128), 0)
        everyone = jnp.full((views, 128), member, jnp.int32)
        group, which = source_of(row, everyone)
        own = lane == residue_of(which, everyone, 8)
        turn = jnp.sum(jnp.where(own, in_order(BINS, BINS + 128), 0.0), axis=1, keepdims=True)
        turn = jnp.broadcast_to(turn, (views, 128)).astype(jnp.int32) + HALF_TURN
        turn_index = (lane + turn) & 127
        turn_near = lane >= turn

        for step in range(2 * BLOCKS - 1):
            delta = (step + 1) // 2 * (1 if step % 2 else -1)
            low, high = max(0, -delta), min(BLOCKS, BLOCKS - delta)
            left = jnp.concatenate(
                [pieces[block] for block in range(low, high)], axis=0
            )
            cols = slice(BLOCK * abs(delta), BLOCK * abs(delta) + BLOCK)
            if delta >= 0:
                left = jnp.concatenate([left, left], axis=1)
                part = jnp.dot(left, ramp_ref[:, cols], preferred_element_type=jnp.float32)
            else:
                part = dot_turned(left, ramp_ref[0:BLOCK, cols]) + dot_turned(left, ramp_ref[BLOCK:, cols])
            rows = slice(views * (low + delta), views * (high + delta))
            if delta == 0:
                filt_ref[rows, :] = part
            else:
                filt_ref[rows, :] += part

        margin = MARGIN // 128
        inner = BINS // 128

        def raw(place):
            half = 128 * (place % 2)
            piece = filt_ref[views * (place // 2) : views * (place // 2) + views, half : half + 128]
            return piece.astype(jnp.bfloat16).astype(jnp.float32)

        largest = jnp.abs(raw(0))
        for place in range(1, inner):
            largest = jnp.maximum(largest, jnp.abs(raw(place)))
        largest = jnp.max(largest, axis=1, keepdims=True)
        largest = jnp.max(largest.reshape(views // SCALE_SET, SCALE_SET, 1), axis=1, keepdims=True)
        largest = jnp.maximum(jnp.broadcast_to(largest, (views // SCALE_SET, SCALE_SET, 128)), 1e-30)
        largest = largest.reshape(views, 128)
        back_ref[...] = largest * (1.0 / (16383.0 * 65536.0))
        scale = 16383.0 / largest
        zero = jnp.zeros((8, 128), jnp.int32)
        lane_row = lax.broadcasted_iota(jnp.int32, (8, 128), 1)

        def group_tables(first):
            here = slice(first, first + 8)
            scale_here, near_here, index_here = scale[here], turn_near[here], turn_index[here]

            def filtered(block):
                place = block - margin
                if place < 0 or place >= inner:
                    return zero
                line = views * (place // 2) + first
                half = 128 * (place % 2)
                piece = filt_ref[line : line + 8, half : half + 128]
                piece = piece.astype(jnp.bfloat16).astype(jnp.float32)
                return jnp.floor(piece * scale_here + 0.5).astype(jnp.int32)

            first_block = FIRST_WIN // 2
            last_block = (FIRST_WIN + WINDOWS) // 2 + 1
            bins = [filtered(block) for block in range(first_block, last_block + 2)]
            pieces = [
                lane_gather(jnp.where(near_here, low, high), index_here)
                for low, high in zip(bins[:-1], bins[1:])
            ]
            rolled = [pltpu.roll(piece, 127, 1) for piece in pieces]
            before = None
            for item in range(last_block - first_block):
                after = jnp.where(lane_row < 127, rolled[item], rolled[item + 1])
                word = pieces[item] * 65536 + (after - pieces[item])
                row = 2 * item * views + first
                if before is not None:
                    word_ref[row - views : row - views + 8, :] = jnp.where(lane_row >= 64, before, word)
                if 2 * item < WINDOWS:
                    word_ref[row : row + 8, :] = word
                before = word

        for first in range(0, views, 8):
            group_tables(first)

    acc_ref[...] = jnp.zeros_like(acc_ref)
    to_smem.wait()

    lane_one = lax.broadcasted_iota(jnp.int32, (8, 128), 1).astype(jnp.float32)
    sub_one = lax.broadcasted_iota(jnp.int32, (8, 128), 0).astype(jnp.float32)
    count = TILES // PARTS
    span = 128 * count
    top = lax.broadcasted_iota(jnp.int32, (8, 128), 0) < 4

    def spread(ref, row):
        return jnp.broadcast_to(ref[pl.ds(row, 1), :], (8, 128))

    member_vec = jnp.full((8, 128), member, jnp.int32)
    is_zero = member_vec == 0
    not_zero = member_vec > 0

    def one_slot(slots, row_set, part, rows_y, straight, mirrored):
        def both(ref, rows):
            if len(rows) == 1:
                return spread(ref, rows[0])
            return jnp.where(top, spread(ref, rows[0]), spread(ref, rows[1]))

        alone = slots[0] == PAIRS
        middle_x = part.astype(jnp.float32) * span + (span // 2 - WIDTH / 2.0 + 0.5)
        first_tile = row_set * TILES + part * count
        cos_v = both(trig_ref, slots)
        base = rows_y * both(trig_ref, [SLOTS + slot for slot in slots]) + CENTER
        stride = cos_v * 128.0
        middle = (lane_one + middle_x) * cos_v + base
        middle_low = jnp.minimum(middle_x * cos_v, (middle_x + 127.0) * cos_v) + base

        def value_of(words, index, along):
            word = lane_gather(words, index)
            return word.astype(jnp.float32) + along * (word << 16).astype(jnp.float32)

        for direction in (1, -1):
            place, place_low = middle, middle_low
            tiles = range(count // 2, count) if direction == 1 else range(count // 2 - 1, -1, -1)
            for tile in tiles:
                if direction == 1 and tile > count // 2:
                    place, place_low = place + stride, place_low + stride
                elif direction == -1:
                    place, place_low = place - stride, place_low - stride
                starts = [where_smem[slot, first_tile + tile] for slot in slots]
                pick = both(bin_ref, [start >> 6 for start in starts]) > place_low
                lower = place.astype(jnp.int32)
                index = lower & 127
                along = place - lower.astype(jnp.float32)

                def words_of(lines):
                    near = [start + line for start, line in zip(starts, lines)]
                    far = [start + (line + 2 * views) for start, line in zip(starts, lines)]
                    return jnp.where(pick, both(word_ref, near), both(word_ref, far))

                if alone:
                    words = words_of([views - 1 for slot in slots])
                    words = jnp.where(is_zero if len(slots) == 1 else top & is_zero, words, 0)
                else:
                    words = words_of(slots)
                    other = words_of([PAIRS + slot for slot in slots])
                    if slots[-1] == PAIRS - 1:
                        other = jnp.where(not_zero if len(slots) == 1 else top | not_zero, other, 0)
                    value = value_of(other, index, along)
                    mirrored[tile] = value if mirrored[tile] is None else mirrored[tile] + value
                value = value_of(words, index, along)
                straight[tile] = value if straight[tile] is None else straight[tile] + value

    def add_up(side, block, line, totals):
        back = spread(back_ref, line)
        for tile in range(count):
            acc_ref[side, block, :, 128 * tile : 128 * tile + 128] += totals[tile] * back

    def all_slots(row_set, part, block, rows_y, slot_sets):
        for first, group in slot_sets:
            straight, mirrored = [None] * count, [None] * count
            for slots in group:
                one_slot(slots, row_set, part, rows_y, straight, mirrored)
            if first == PAIRS:
                add_up(0, block, views - SCALE_SET, straight)
            else:
                add_up(0, block, first, straight)
                add_up(1, block, PAIRS + first, mirrored)

    singles = [
        (first, [(first + item,) for item in range(SCALE_SET)])
        for first in range(0, PAIRS, SCALE_SET)
    ]
    doubles = [
        (first, [(first + item, first + item + 4) for item in range(SCALE_SET // 2)])
        for first in range(0, PAIRS, SCALE_SET)
    ]

    def steps(block, carry):
        row_set = block // PARTS
        rows_y = sub_one + (first_y + 8.0 * row_set.astype(jnp.float32))
        all_slots(row_set, block % PARTS, block, rows_y, singles + [(PAIRS, [(PAIRS,)])])
        return carry

    lax.fori_loop(0, 2 * PARTS, steps, 0)

    def paired_steps(part, carry):
        rows_y = jnp.where(top, sub_one, sub_one - 4.0) + (first_y + 16.0)
        all_slots(2, part, 2 * PARTS + part, rows_y, doubles + [(PAIRS, [(PAIRS, PAIRS)])])
        return carry

    lax.fori_loop(0, PARTS, paired_steps, 0)

    back_index = 127 - lax.broadcasted_iota(jnp.int32, (8, 128), 1)
    for row_set in range(ROW_SETS):
        for tile in range(TILES):
            block, spot = row_set * PARTS + tile // count, tile % count
            turn_tile = TILES - 1 - tile
            other = acc_ref[
                1,
                row_set * PARTS + turn_tile // count,
                :,
                128 * (turn_tile % count) : 128 * (turn_tile % count) + 128,
            ]
            acc_ref[0, block, :, 128 * spot : 128 * spot + 128] += lane_gather(other, back_index)

    def rows_of(row_set, low, high):
        return jnp.concatenate(
            [acc_ref[0, row_set * PARTS + part, low:high, :] for part in range(PARTS)], axis=1
        )

    for member in range(GROUP):
        lower = rows_of(member // 2, 0, 8)
        if member == 1:
            lower = jnp.concatenate([rows_of(0, 4, 8), rows_of(1, 0, 4)], axis=0)
        elif member == 3:
            lower = jnp.concatenate([rows_of(1, 4, 8), rows_of(2, 0, 4) + rows_of(2, 4, 8)], axis=0)
        out_ref[member] = lower.astype(jnp.bfloat16)


def backproject(lines, trig, ramp, image_rows):
    views = lines.shape[0] * lines.shape[1]
    rows = WINDOWS * views
    vmem = pl.BlockSpec(memory_space=pltpu.VMEM)
    def body(*refs):
        backproject_kernel(image_rows, *refs)

    return pl.pallas_call(
        body,
        out_shape=jax.ShapeDtypeStruct((GROUP, 8, WIDTH), jnp.bfloat16),
        in_specs=[vmem] * 3,
        out_specs=vmem,
        scratch_shapes=[
            pltpu.VMEM((BLOCKS * views, BLOCK), jnp.float32),
            pltpu.VMEM((rows, 128), jnp.int32),
            pltpu.VMEM((SLOTS, 128), jnp.float32),
            pltpu.VMEM((views, 128), jnp.float32),
            pltpu.VMEM((SLOTS, 128), jnp.int32),
            pltpu.VMEM((2, ROW_SETS * PARTS, 8, WIDTH // PARTS), jnp.float32),
            pltpu.SMEM((SLOTS, 128), jnp.int32),
            pltpu.SemaphoreType.DMA(()),
        ],
        compiler_params=pltpu.CompilerParams(vmem_limit_bytes=16 * 2**20),
        cost_estimate=pl.CostEstimate(flops=1_000_000_000, bytes_accessed=6_000_000, transcendentals=0),
        name="backproject",
    )(lines, trig, ramp)


def layers_kernel(
    scale,
    image_rows,
    parts_ref,
    first_ref,
    bias_one_ref,
    second_ref,
    bias_two_ref,
    out_ref,
    image_ref,
    stack_ref,
):
    row_base = lax.axis_index("rows") * ROW_DEV
    image = parts_ref[0].astype(jnp.float32)
    for member in range(1, GROUP):
        image = image + parts_ref[member].astype(jnp.float32)
    image = (image * scale).astype(jnp.bfloat16).astype(jnp.float32)
    row = lax.broadcasted_iota(jnp.int32, image.shape, 0) + (row_base - 2)
    image = jnp.where((row >= 0) & (row < image_rows), image, 0.0)
    column = lax.broadcasted_iota(jnp.int32, image.shape, 1)
    left = jnp.where(column == 0, 0.0, pltpu.roll(image, 1, 1))
    right = jnp.where(column == WIDTH - 1, 0.0, pltpu.roll(image, WIDTH - 1, 1))
    three = jnp.concatenate([left, image, right], axis=0).astype(jnp.bfloat16)
    image_ref[...] = jnp.concatenate([three, three, three], axis=0)

    weights = first_ref[...]
    count = CHAN * (ROW_DEV + 2)
    for tile in range(0, WIDTH, 256):
        hidden = jnp.dot(weights, image_ref[:, tile : tile + 256], preferred_element_type=jnp.float32)
        hidden = jnp.maximum(hidden + bias_one_ref[...], 0.0)
        top = jnp.where(row_base > 0, hidden[0:CHAN], 0.0)
        bottom = jnp.where(row_base + ROW_DEV < image_rows, hidden[count - CHAN : count], 0.0)
        hidden = jnp.concatenate([top, hidden[CHAN : count - CHAN], bottom], axis=0)
        stack_ref[:, tile : tile + 256] = hidden

    middle_rows = stack_ref[...]
    column = lax.broadcasted_iota(jnp.int32, middle_rows.shape, 1)
    before = jnp.where(column == 0, 0.0, pltpu.roll(middle_rows, 1, 1)).astype(jnp.bfloat16)
    after = jnp.where(column == WIDTH - 1, 0.0, pltpu.roll(middle_rows, WIDTH - 1, 1)).astype(jnp.bfloat16)
    mixed = jnp.dot(second_ref[0], before, preferred_element_type=jnp.float32)
    mixed = mixed + jnp.dot(second_ref[1], middle_rows.astype(jnp.bfloat16), preferred_element_type=jnp.float32)
    mixed = mixed + jnp.dot(second_ref[2], after, preferred_element_type=jnp.float32)
    mixed = jnp.maximum(mixed + bias_two_ref[...], 0.0)
    out_ref[...] = mixed.reshape(CHAN, ROW_DEV, WIDTH).astype(jnp.bfloat16)[None]


def layers(parts, first, bias_one, second, bias_two, scale, image_rows):
    vmem = pl.BlockSpec(memory_space=pltpu.VMEM)

    def body(*refs):
        layers_kernel(scale, image_rows, *refs)

    return pl.pallas_call(
        body,
        out_shape=jax.ShapeDtypeStruct((1, CHAN, ROW_DEV, WIDTH), jnp.bfloat16),
        in_specs=[vmem] * 5,
        out_specs=vmem,
        scratch_shapes=[
            pltpu.VMEM((72, WIDTH), jnp.bfloat16),
            pltpu.VMEM((CHAN * (ROW_DEV + 2), WIDTH), jnp.float32),
        ],
        compiler_params=pltpu.CompilerParams(vmem_limit_bytes=16 * 2**20),
        cost_estimate=pl.CostEstimate(flops=500_000_000, bytes_accessed=1_000_000, transcendentals=0),
        name="layers",
    )(parts, first, bias_one, second, bias_two)


def local(sinogram, view_shift, conv_one, bias_one, conv_two, bias_two):
    sheets, view_count, detector = sinogram.shape
    row_groups = lax.axis_size("rows")
    view_groups = lax.axis_size("views")
    views_total = view_count * view_groups
    image_rows = ROW_DEV * row_groups
    share = view_count // GROUP
    sent = pack(view_shift, sinogram, share)
    lines = lax.all_to_all(sent, "views", 0, 0, tiled=True)

    ramp, trig = prepare(views_total, view_count)
    partial_rows = backproject(lines, trig, ramp, image_rows)
    groups = [[GROUP * base + item for item in range(GROUP)] for base in range(row_groups // GROUP)]
    parts = lax.all_to_all(partial_rows, "rows", 0, 0, tiled=True, axis_index_groups=groups)

    first, wide_one, second, wide_two = spread_weights(
        partial_rows, conv_one, bias_one[None], conv_two, bias_two[None]
    )
    return layers(
        parts,
        first,
        wide_one,
        second,
        wide_two,
        math.pi / views_total,
        image_rows,
    )


def solution(mesh):
    return jax.shard_map(
        local,
        mesh=mesh,
        in_specs=(P(None, "views", None), P("views"), P(), P(), P(), P()),
        out_specs=P("views", None, "rows", None),
        check_vma=False,
    )
```
